32 devices in a mesh: section: 4 (over x, core), wide: 8 (over z, y).
Axes of the slice: x: 2, y: 2, z: 4, core: 2. Of those that a mesh axis runs over, the one named last changes fastest.
Arguments:
- tokens_in: bfloat16 [2, 2048, 1024], P(None, 'wide', 'section'), may hold values from -6 to 6
- cotangent: bfloat16 [2, 2048, 1024], P(None, 'wide', 'section'), may hold values from -6 to 6
- routes: int32 [2, 2048, 1], P(None, 'wide'), may hold values from 0 to 7; in each aligned block of 256 rows (0 to 255, 256 to 511, ..., all dimensions but the last counted through in order) at most 40 rows name the same one
- seq_lengths: int32 [2], replicated, may hold values from 128 to 256, as said below
- qkv_weight: bfloat16 [1024, 3072], P(('section', 'wide')), may hold values from -0.1875 to 0.1875
- out_weight: bfloat16 [1024, 1024], P(('section', 'wide')), may hold values from -0.75 to 0.75
- attn_gain: bfloat16 [1024], P(('section', 'wide')), may hold values from 0.5 to 1.5
- ffn_in: bfloat16 [1024, 4096], P(('section', 'wide')), may hold values from -0.1875 to 0.1875
- ffn_back: bfloat16 [4096, 1024], P(('section', 'wide')), may hold values from -0.09375 to 0.09375
- ffn_gain: bfloat16 [1024], P(('section', 'wide')), may hold values from 0.5 to 1.5
- centroids: bfloat16 [8, 1024], P('wide', 'section'), may hold values from -0.1875 to 0.1875
- first_gain: bfloat16 [8, 1024], P('wide', 'section'), may hold values from 0.5 to 1.5
- first_in: bfloat16 [8, 1024, 4096], P('wide', 'section'), may hold values from -0.1875 to 0.1875
- first_back: bfloat16 [8, 4096, 1024], P('wide', 'section'), may hold values from -0.09375 to 0.09375
- second_gain: bfloat16 [8, 1024], P('wide', 'section'), may hold values from 0.5 to 1.5
- second_in: bfloat16 [8, 1024, 4096], P('wide', 'section'), may hold values from -0.1875 to 0.1875
- second_back: bfloat16 [8, 4096, 1024], P('wide', 'section'), may hold values from -0.09375 to 0.09375
Outputs:
- block_out: bfloat16 [2, 2048, 1024], P(None, 'wide', 'section')
- tokens_grad: float32 [2, 2048, 1024], P(None, 'wide', 'section')
- qkv_grad: float32 [1024, 3072], P(('section', 'wide'))
- out_grad: float32 [1024, 1024], P(('section', 'wide'))
- attn_gain_grad: float32 [1024], P(('section', 'wide'))
- ffn_in_grad: float32 [1024, 4096], P(('section', 'wide'))
- ffn_back_grad: float32 [4096, 1024], P(('section', 'wide'))
- ffn_gain_grad: float32 [1024], P(('section', 'wide'))
- centroids_grad: float32 [8, 1024], P('wide', 'section')
- first_gain_grad: float32 [8, 1024], P('wide', 'section')
- first_in_grad: float32 [8, 1024, 4096], P('wide', 'section')
- first_back_grad: float32 [8, 4096, 1024], P('wide', 'section')
- second_gain_grad: float32 [8, 1024], P('wide', 'section')
- second_in_grad: float32 [8, 1024, 4096], P('wide', 'section')
- second_back_grad: float32 [8, 4096, 1024], P('wide', 'section')
The draws below stay inside these ranges and needn't reach their ends.
Inputs may be any that keep to these rules, and one draw needn't show every extreme that they name: `routes`: in each micro-batch, at most 40 of one device's 256 rows name the same expert. `seq_lengths`: each micro-batch holds sequences of one length, 128 or 256; a device's 256 rows of a micro-batch are whole sequences in order; both lengths occur.
All inputs are finite; a program needn't handle non-finite values.
Results may differ from the reference program's by a relative error of at most 0.015.
Values may be sent and summed in bfloat16 or wider, within the bound.
A program may use at most 512 MiB of HBM per device.

```python
import math
import jax
import jax.numpy as jnp
import numpy as np
from jax import lax

D = 1024
HEADS = 16
FF = 4096
ROWS = 256
SHORT = 128
MICRO = 2
EXPERTS = 8
CAP = 40
TOK_MB = 2048
N_WIDE = 8


def draw_seq_lengths(key, part):
    order = jax.random.permutation(key, MICRO)
    return jnp.where(order % 2 == 0, SHORT, ROWS).astype(jnp.int32)


def level_of(rng, extent, pieces, least, largest):
    def one(axis_at, parts):
        steps = jax.random.uniform(jax.random.fold_in(jax.random.fold_in(rng, 6), axis_at), (parts,), jnp.float32, least / len(pieces), largest / len(pieces))
        return jnp.repeat(jnp.exp(steps), extent[axis_at] // parts).reshape((-1,) + (1,) * (len(extent) - axis_at - 1))

    level = one(*pieces[0])
    for cut in pieces[1:]:
        level = level * one(*cut)
    return level


def assign_block(rng, own, number, rows, amount, top, limit, lean):
    order = jax.random.permutation(rng, amount)
    crowded, ordinary = portions_of(amount, rows * top, limit, lean, True), portions_of(amount, rows * top, limit, lean, False)
    places = jnp.arange(amount)

    def named(tallies, rotation):
        used = int((tallies > 0).sum())
        fixed = max(1, used // 4)
        passed = fixed + (places - fixed + rotation * (used - fixed)) % max(1, amount - fixed)
        return jnp.zeros((amount,), jnp.int32).at[order[jnp.where(places < fixed, places, passed)]].set(jnp.asarray(tallies, jnp.int32))

    tallies = jnp.where(number % 4 == 0, named(crowded, number // 4), named(ordinary, number - number // 4 - 1))
    mixed = jax.random.permutation(jax.random.fold_in(own, 3), amount)
    donor, receiver = mixed[0:amount // 2 * 2:2], mixed[1:amount // 2 * 2:2]
    room = jnp.minimum(tallies[donor] - 1, limit - tallies[receiver]) // 2
    room = jnp.where((donor == order[0]) | (receiver == order[0]) | (tallies[receiver] == 0), 0, jnp.maximum(room, 0))
    passed = jax.random.randint(jax.random.fold_in(own, 4), (amount // 2,), 0, 1 << 20) % (room + 1)
    tallies = tallies.at[donor].add(-passed).at[receiver].add(passed)
    items = jnp.searchsorted(jnp.cumsum(tallies), jnp.arange(rows * top), side="right").astype(jnp.int32)
    grid = items.reshape(top, rows).T
    grid = grid[jax.random.permutation(jax.random.fold_in(own, 1), rows)]
    rotation = jax.random.randint(jax.random.fold_in(own, 2), (rows, 1), 0, top)
    return jnp.take_along_axis(grid, (jnp.arange(top)[None, :] + rotation) % top, axis=1)


def portions_of(number_of, total, most, lean, full):
    weights = [(1 << 20) // math.isqrt(grade ** lean) + 1 for grade in range(1, number_of + 1)]
    largest = most if full else min(most, max(-(-total // number_of), total * weights[0] // sum(weights)))
    least = 1 if total - largest >= number_of - 1 else 0
    holding, spare = [largest] + [least] * (number_of - 1), total - largest - least * (number_of - 1)
    while spare > 0:
        candidates = [i for i in range(1, number_of) if holding[i] < largest] or [i for i in range(1, number_of) if holding[i] < most]
        pool, left = sum([weights[i] for i in candidates]), spare
        for i in candidates:
            extra = min(most - holding[i], max(1, left * weights[i] // pool), spare)
            holding[i] = holding[i] + extra
            spare = spare - extra
    return np.array(holding)


def gaussian(stream_key, dims, deviation, bound, cuts=(), held_as=jnp.bfloat16):
    gain = level_of(stream_key, dims, cuts, -0.22, 0.18) if cuts else 1.0
    drawn = jax.random.normal(stream_key, dims, jnp.float32) * deviation * gain
    return jnp.minimum(jnp.maximum(drawn, -bound), bound).astype(held_as)


def setup_inputs(seed: int = 0) -> dict:
    key_of = jax.random.split(jax.random.key(seed), 18)
    tokens_in = gaussian(key_of[0], (MICRO, TOK_MB, D), 1.0, 6.0, ((1, 8), (2, 4)))
    cotangent = gaussian(key_of[1], (MICRO, TOK_MB, D), 1.0, 6.0, ((1, 8), (2, 4)))
    routes_keys = jax.random.split(jax.random.fold_in(key_of[2], 1), MICRO * TOK_MB // ROWS)
    routes_turns = jax.random.permutation(jax.random.fold_in(key_of[2], 3), MICRO * TOK_MB // ROWS)
    routes = jax.vmap(lambda own, number: assign_block(jax.random.fold_in(key_of[2], 2), own, number, ROWS, EXPERTS, 1, CAP, 1))(routes_keys, routes_turns).reshape((MICRO, TOK_MB, 1))
    seq_lengths = draw_seq_lengths(jax.random.fold_in(key_of[17], 71), 0)
    qkv_weight = gaussian(key_of[4], (D, 3 * D), D ** -0.5, 0.1875, ((0, 32),))
    out_weight = gaussian(key_of[5], (D, D), (D // 16) ** -0.5, 0.75, ((0, 32),))
    attn_gain = jnp.clip(1.0 + 0.1 * jax.random.normal(key_of[6], (D,), jnp.float32), 0.5, 1.5).astype(jnp.bfloat16)
    ffn_in = gaussian(key_of[7], (D, FF), D ** -0.5, 0.1875, ((0, 32),))
    ffn_back = gaussian(key_of[8], (FF, D), FF ** -0.5, 0.09375, ((0, 32),))
    ffn_gain = jnp.clip(1.0 + 0.1 * jax.random.normal(key_of[9], (D,), jnp.float32), 0.5, 1.5).astype(jnp.bfloat16)
    centroids = gaussian(key_of[10], (EXPERTS, D), D ** -0.5, 0.1875, ((0, 8), (1, 4)))
    first_gain = jnp.clip(1.0 + 0.1 * jax.random.normal(key_of[11], (EXPERTS, D), jnp.float32), 0.5, 1.5).astype(jnp.bfloat16)
    first_in = gaussian(key_of[12], (EXPERTS, D, FF), D ** -0.5, 0.1875, ((0, 8), (1, 4)))
    first_back = gaussian(key_of[13], (EXPERTS, FF, D), FF ** -0.5, 0.09375, ((0, 8), (1, 4)))
    second_gain = jnp.clip(1.0 + 0.1 * jax.random.normal(key_of[14], (EXPERTS, D), jnp.float32), 0.5, 1.5).astype(jnp.bfloat16)
    second_in = gaussian(key_of[15], (EXPERTS, D, FF), D ** -0.5, 0.1875, ((0, 8), (1, 4)))
    second_back = gaussian(key_of[16], (EXPERTS, FF, D), FF ** -0.5, 0.09375, ((0, 8), (1, 4)))
    return dict(tokens_in=tokens_in, cotangent=cotangent, routes=routes, seq_lengths=seq_lengths, qkv_weight=qkv_weight, out_weight=out_weight, attn_gain=attn_gain, ffn_in=ffn_in, ffn_back=ffn_back, ffn_gain=ffn_gain, centroids=centroids, first_gain=first_gain, first_in=first_in, first_back=first_back, second_gain=second_gain, second_in=second_in, second_back=second_back)


@jax.custom_vjp
def low(v):
    return lax.optimization_barrier(v.astype(jnp.bfloat16)).astype(jnp.float32)

@jax.custom_vjp
def low_back(v):
    return v

def low_keep(v):
    return (low(v), None)

def low_pass(kept, grad):
    return (grad,)

def back_keep(v):
    return (v, None)

def back_low(kept, grad):
    return (low(grad),)
low.defvjp(low_keep, low_pass)
low_back.defvjp(back_keep, back_low)

def rounded_both(values_in):
    return low(low_back(values_in))

def matmul_high(left, right):
    return jnp.matmul(left, right, precision=lax.Precision.HIGHEST)

def layer_norm(values_in, gain_vec):
    centred = values_in - lax.optimization_barrier(jnp.mean(values_in, axis=-1, keepdims=True))
    spread_sq = lax.optimization_barrier(jnp.mean(centred * centred, axis=-1, keepdims=True))
    return centred * lax.rsqrt(spread_sq + 1e-05) * gain_vec

def gelu_value(values_in):
    return 0.5 * values_in * (1.0 + lax.erf(values_in * 0.7071067811865476))

def attention_block(block_rows, length, qkv_w, out_w, gain_vec):
    head_size = D // HEADS
    normed = low(layer_norm(block_rows, gain_vec))
    packed = rounded_both(matmul_high(normed, qkv_w))
    queries = packed[:, :D].reshape(ROWS, HEADS, head_size).transpose(1, 0, 2)
    keys_all = packed[:, D:2 * D].reshape(ROWS, HEADS, head_size).transpose(1, 0, 2)
    values_all = packed[:, 2 * D:].reshape(ROWS, HEADS, head_size).transpose(1, 0, 2)
    raw = low_back(jnp.einsum('hqd,hkd->hqk', queries, keys_all, precision=lax.Precision.HIGHEST))
    position = jnp.arange(ROWS, dtype=jnp.int32)
    allowed = (position[:, None] >= position[None, :]) & (position[:, None] // length == position[None, :] // length)
    scores = jnp.where(allowed[None], raw * head_size ** (-0.5), -1e+30)
    attn_probs = jax.nn.softmax(scores, axis=-1)
    mixed_rows = jnp.einsum('hqk,hkd->qhd', low(attn_probs), values_all, precision=lax.Precision.HIGHEST).reshape(ROWS, D)
    mixed_rows = rounded_both(mixed_rows)
    return rounded_both(block_rows + matmul_high(mixed_rows, out_w))

def residual_ffn(rows_in, first_w, second_w, gain_vec):
    normed = low(layer_norm(rows_in, gain_vec))
    before = low_back(matmul_high(normed, first_w))
    return rows_in + matmul_high(low(gelu_value(before)), second_w)

def expert_block(entry_all):
    routed_rows, gain_one, in_one, back_one, gain_two, in_two, back_two, centre = entry_all
    first_rows = rounded_both(residual_ffn(routed_rows, in_one, back_one, gain_one))
    gated_rows = low_back(routed_rows)
    normed = low(layer_norm(first_rows, gain_two))
    before = low_back(matmul_high(normed, in_two))
    branch_out = low_back(matmul_high(low(gelu_value(before)), back_two))
    second_rows = first_rows + branch_out
    gate_vals = jax.nn.sigmoid(lax.optimization_barrier(jnp.sum(gated_rows * centre, axis=-1, keepdims=True)))
    return gated_rows + gate_vals * second_rows

def reference(tokens_in, cotangent, routes, seq_lengths, qkv_weight, out_weight, attn_gain, ffn_in, ffn_back, ffn_gain, centroids, first_gain, first_in, first_back, second_gain, second_in, second_back):
    floats = [array_in.astype(jnp.float32) for array_in in (tokens_in, qkv_weight, out_weight, attn_gain, ffn_in, ffn_back, ffn_gain, centroids, first_gain, first_in, first_back, second_gain, second_in, second_back)]
    route_ids = routes[:, :, 0].reshape(MICRO, N_WIDE, ROWS).astype(jnp.int32)
    choose = (route_ids[..., None] == jnp.arange(EXPERTS, dtype=jnp.int32)).astype(jnp.int32)
    ranking = jnp.cumsum(choose, axis=2) - 1
    slot_table = (route_ids * CAP + lax.optimization_barrier(jnp.sum(ranking * choose, axis=3))).astype(jnp.int32)
    lengths = jnp.repeat(seq_lengths, N_WIDE)

    def forward(tokens, qkv_w, out_w, gain_a, in_w, back_w, gain_f, centre, gain_one, in_one, back_one, gain_two, in_two, back_two):
        blocks = tokens.reshape(MICRO * N_WIDE, ROWS, D)

        def attend_one(entry_pair):
            return attention_block(entry_pair[0], entry_pair[1], qkv_w, out_w, gain_a)

        def dense_one(block_rows):
            return rounded_both(residual_ffn(block_rows, in_w, back_w, gain_f))
        attended = lax.map(jax.checkpoint(attend_one), (blocks, lengths))
        fed = lax.map(jax.checkpoint(dense_one), attended).reshape(MICRO, N_WIDE, ROWS, D)

        def scatter_one(token_rows, slot_idx):
            return jnp.zeros((EXPERTS * CAP, D), jnp.float32).at[slot_idx].set(token_rows)

        def gather_one(rows_all, slot_idx):
            return jnp.take(rows_all, slot_idx, axis=0)
        buffers = jax.vmap(jax.vmap(scatter_one))(fed, slot_table)
        routed = buffers.reshape(MICRO, N_WIDE, EXPERTS, CAP, D).transpose(2, 0, 1, 3, 4).reshape(EXPERTS, MICRO * N_WIDE * CAP, D)
        mixed = lax.map(jax.checkpoint(expert_block), (routed, gain_one, in_one, back_one, gain_two, in_two, back_two, centre))
        back_rows = mixed.reshape(EXPERTS, MICRO, N_WIDE, CAP, D).transpose(1, 2, 0, 3, 4).reshape(MICRO, N_WIDE, EXPERTS * CAP, D)
        result = jax.vmap(jax.vmap(gather_one))(back_rows, slot_table)
        return low(result.reshape(MICRO, N_WIDE * ROWS, D))
    result, pullback = jax.vjp(forward, *floats)
    grads = pullback(cotangent.astype(jnp.float32))
    return (result.astype(jnp.bfloat16), grads[0], grads[1], grads[2], grads[3], grads[4], grads[5], grads[6], grads[7], grads[8], grads[9], grads[10], grads[11], grads[12], grads[13])
```

```python
import jax
import jax.numpy as jnp
from jax import lax
from jax.sharding import PartitionSpec as P

HEAD_SIZE = 64
F32 = jnp.float32
BF16 = jnp.bfloat16


def dot(left, right):
    return jnp.dot(left, right, preferred_element_type=F32)


def dot_nt(left, right):
    return lax.dot_general(left, right, (((1,), (1,)), ((), ())), preferred_element_type=F32)


def dot_tn(left, right):
    return lax.dot_general(left, right, (((0,), (0,)), ((), ())), preferred_element_type=F32)


def gelu_value(v):
    return 0.5 * v * (1.0 + lax.erf(v * 0.7071067811865476))


def gelu_slope(v):
    return (
        0.5 * (1.0 + lax.erf(v * 0.7071067811865476))
        + v * jnp.exp(-0.5 * v * v) * 0.3989422804014327
    )


def unit_norm(v):
    centred = v - jnp.mean(v, axis=-1, keepdims=True)
    scale = lax.rsqrt(jnp.mean(centred * centred, axis=-1, keepdims=True) + 1e-05)
    return centred * scale, scale


def reduce_quarters(part):
    rows, width = part.shape
    return lax.psum_scatter(part.astype(BF16), "section", scatter_dimension=1, tiled=True).astype(F32)


def gather_quarters(quarter):
    return lax.all_gather(quarter, "section", axis=1, tiled=True)


def section_sum(v):
    return lax.psum(v, "section")


def wide_exchange(slots):
    return lax.all_to_all(slots, "wide", split_axis=0, concat_axis=0, tiled=True)


def attention_probs(queries, keys, lengths):
    rows = queries.shape[2]
    raw = jnp.einsum("mhqd,mhkd->mhqk", queries, keys, preferred_element_type=F32)
    pos = jnp.arange(rows, dtype=jnp.int32)
    same = pos[None, :, None] // lengths[:, None, None] == pos[None, None, :] // lengths[:, None, None]
    allowed = (pos[:, None] >= pos[None, :])[None] & same
    scores = jnp.where(allowed[:, None], raw * HEAD_SIZE ** (-0.5), -1e30)
    highest = jnp.max(scores, axis=-1, keepdims=True)
    expo = jnp.exp(scores - highest)
    return expo / jnp.sum(expo, axis=-1, keepdims=True)


def body(
    tokens_in,
    cotangent,
    routes,
    seq_lengths,
    qkv_weight,
    out_weight,
    attn_gain,
    ffn_in,
    ffn_back,
    ffn_gain,
    centroids,
    first_gain,
    first_in,
    first_back,
    second_gain,
    second_in,
    second_back,
):
    sections = lax.axis_size("section")
    wide = lax.axis_size("wide")
    section_id = lax.axis_index("section")
    wide_id = lax.axis_index("wide")
    micro, rows, quarter = tokens_in.shape
    width = quarter * sections
    cap = 5 * rows // (4 * wide)
    tok_rows = micro * rows
    hid = first_back.shape[1]
    small = qkv_weight.shape[0]
    qkv_cols = qkv_weight.shape[1] // sections

    qkv_cut = (
        qkv_weight.reshape(small, 3, sections, quarter).transpose(2, 0, 1, 3).reshape(sections, small, qkv_cols)
    )
    in_cut = ffn_in.reshape(small, sections, hid).transpose(1, 0, 2)
    cut = lax.all_to_all(jnp.concatenate([qkv_cut, in_cut], axis=2), "section", split_axis=0, concat_axis=0, tiled=True)

    def whole_rows(piece):
        got = lax.all_gather(piece, "wide", axis=0, tiled=False)
        return got.transpose(1, 0, 2, 3).reshape(width, piece.shape[2])

    vectors = jnp.concatenate([first_gain[0], second_gain[0], centroids[0], attn_gain, ffn_gain])
    vectors = jnp.pad(vectors, (0, 1024 - vectors.shape[0])).reshape(8, 128)
    vectors = lax.all_gather(vectors, ("section", "wide"), axis=0, tiled=False).reshape(sections, wide, 1024)
    own = lax.dynamic_index_in_dim(vectors, wide_id, axis=1, keepdims=False).astype(F32)
    gain_first = own[:, :quarter].reshape(1, width)
    gain_second = own[:, quarter : 2 * quarter].reshape(1, width)
    centre = own[:, 2 * quarter : 3 * quarter].reshape(1, width)
    gain_attn = vectors[:, :, 3 * quarter : 3 * quarter + small].reshape(1, width).astype(F32)
    gain_ffn = vectors[:, :, 3 * quarter + small : 3 * quarter + 2 * small].reshape(1, width).astype(F32)
    own_quarter = lambda v: lax.dynamic_slice_in_dim(v, section_id * quarter, quarter, axis=1)

    tokens_q = tokens_in.reshape(tok_rows, quarter)
    tokens = gather_quarters(tokens_q)
    qkv_w = whole_rows(cut[:, :, :qkv_cols])
    out_w = lax.all_gather(out_weight, "wide", axis=0, tiled=True)
    in_w = whole_rows(cut[:, :, qkv_cols:])
    back_w = lax.all_gather(ffn_back, "wide", axis=0, tiled=True)

    def slice_in(weight):
        pieces = weight[0].reshape(quarter, sections, hid).transpose(1, 0, 2)
        return lax.all_to_all(pieces, "section", split_axis=0, concat_axis=0, tiled=True).reshape(width, hid)

    first_w = slice_in(first_in)
    second_w = slice_in(second_in)
    first_b = first_back[0]
    second_b = second_back[0]

    experts = jnp.arange(wide, dtype=jnp.int32)
    choose = (routes == experts).astype(jnp.int32)
    upto = (jnp.arange(rows)[:, None] >= jnp.arange(rows)[None, :]).astype(BF16)
    ranking = jnp.einsum("rk,mke->mre", upto, choose.astype(BF16), preferred_element_type=F32).astype(jnp.int32) - 1
    slot_of = routes[:, :, 0] * cap + jnp.sum(ranking * choose, axis=2)
    onehot = (jnp.arange(wide * cap, dtype=jnp.int32)[None, :, None] == slot_of[:, None, :]).astype(BF16)

    def to_experts(rows_q):
        packed = jnp.einsum("msr,mrd->msd", onehot, rows_q.reshape(micro, rows, quarter), preferred_element_type=F32)
        packed = packed.astype(BF16).reshape(micro, wide, cap, quarter).transpose(1, 0, 2, 3)
        return wide_exchange(packed.reshape(wide, micro * cap, quarter)).reshape(wide * micro * cap, quarter)

    def to_tokens(slots_q):
        back = wide_exchange(slots_q.reshape(wide, micro * cap, quarter))
        back = back.reshape(wide, micro, cap, quarter).transpose(1, 0, 2, 3).reshape(micro, wide * cap, quarter)
        got = jnp.einsum("msr,msd->mrd", onehot, back, preferred_element_type=F32)
        return got.astype(BF16).reshape(tok_rows, quarter)

    unit_a, scale_a = unit_norm(tokens.astype(F32))
    normed_a = (unit_a * gain_attn).astype(BF16)
    packed = dot(normed_a, qkv_w).astype(BF16)
    heads = quarter // HEAD_SIZE

    def by_head(v):
        return v.reshape(micro, rows, heads, HEAD_SIZE).transpose(0, 2, 1, 3)

    def from_head(v):
        return v.transpose(0, 2, 1, 3).reshape(tok_rows, quarter)

    queries, keys, values = (by_head(packed[:, i * quarter : (i + 1) * quarter]) for i in range(3))
    probs = attention_probs(queries, keys, seq_lengths)
    probs_b = probs.astype(BF16)
    mixed = from_head(
        jnp.einsum("mhqk,mhkd->mhqd", probs_b, values, preferred_element_type=F32).astype(BF16)
    )
    attended_q = (tokens_q.astype(F32) + reduce_quarters(dot(mixed, out_w))).astype(BF16)
    attended = gather_quarters(attended_q)

    def branch(v, w_in, w_back, gain):
        unit, scale = unit_norm(v.astype(F32))
        normed = (unit * gain).astype(BF16)
        pre = dot(normed, w_in)
        hidden = gelu_value(pre).astype(BF16)
        return (normed, unit, scale, pre, hidden), dot(hidden, w_back)

    def branch_back(grad, saved, w_in, w_back, gain):
        normed, unit, scale, pre, hidden = saved
        d_back = dot_tn(hidden, grad)
        d_pre = (dot_nt(grad, w_back) * gelu_slope(pre)).astype(BF16)
        d_in = dot_tn(normed, d_pre)
        return d_in, d_back, norm_back(dot_nt(d_pre, w_in), unit, scale, gain)

    def norm_back(d_part, unit, scale, gain):
        d_unit = d_part * gain
        sums = section_sum(
            jnp.stack([jnp.sum(d_unit, axis=1), jnp.sum(d_unit * unit, axis=1)])
        ) / width
        d_q = reduce_quarters(d_part)
        unit_q = own_quarter(unit)
        d_rows = scale * (d_q * own_quarter(gain) - sums[0][:, None] - unit_q * sums[1][:, None])
        return d_rows, jnp.sum(d_q * unit_q, axis=0)

    saved_d, part = branch(attended, in_w, back_w, gain_ffn)
    fed_q = (attended_q.astype(F32) + reduce_quarters(part)).astype(BF16)
    routed_q = to_experts(fed_q)
    routed = gather_quarters(routed_q)
    d_mixed_q = to_experts(cotangent.reshape(tok_rows, quarter))
    d_mixed = gather_quarters(d_mixed_q).astype(F32)
    saved_1, part = branch(routed, first_w, first_b, gain_first)
    first_q = (routed_q.astype(F32) + reduce_quarters(part)).astype(BF16)
    first = gather_quarters(first_q)
    saved_2, part = branch(first, second_w, second_b, gain_second)
    gate = jax.nn.sigmoid(jnp.sum(routed.astype(F32) * centre, axis=-1, keepdims=True))
    second_q = first_q.astype(F32) + reduce_quarters(part)
    mixed_q = routed_q.astype(F32) + gate * second_q
    block_out = to_tokens(mixed_q.astype(BF16)).reshape(micro, rows, quarter)

    d_second = gate * d_mixed
    d_second_q = gate * d_mixed_q.astype(F32)
    d_logit = section_sum(jnp.sum(d_mixed_q.astype(F32) * second_q, axis=-1))[:, None] * gate * (1.0 - gate)
    centroids_grad = jnp.sum(d_logit * routed_q.astype(F32), axis=0)[None]
    d_gated_q = (d_mixed_q.astype(F32) + d_logit * own_quarter(centre)).astype(BF16)
    d_second_in, d_second_back, (norm_q, second_gain_grad) = branch_back(
        d_second.astype(BF16), saved_2, second_w, second_b, gain_second
    )
    d_first_q = (d_second_q + norm_q).astype(BF16)
    d_first_in, d_first_back, (norm_q, first_gain_grad) = branch_back(
        gather_quarters(d_first_q), saved_1, first_w, first_b, gain_first
    )
    d_routed_q = (d_first_q.astype(F32) + norm_q + d_gated_q.astype(F32)).astype(BF16)
    d_fed_q = to_tokens(d_routed_q)
    d_in, d_back, (norm_q, d_gain_ffn) = branch_back(gather_quarters(d_fed_q), saved_d, in_w, back_w, gain_ffn)
    d_attended_q = (d_fed_q.astype(F32) + norm_q).astype(BF16)
    d_attended = gather_quarters(d_attended_q)
    d_out = dot_tn(mixed, d_attended)
    d_mix = by_head(dot_nt(d_attended, out_w).astype(BF16))
    d_probs = jnp.einsum("mhqd,mhkd->mhqk", d_mix, values, preferred_element_type=F32)
    delta = jnp.sum(probs * d_probs, axis=-1, keepdims=True)
    d_scores = (probs * (d_probs - delta) * HEAD_SIZE ** (-0.5)).astype(BF16)
    d_queries = jnp.einsum("mhqk,mhkd->mhqd", d_scores, keys, preferred_element_type=F32)
    d_keys = jnp.einsum("mhqk,mhqd->mhkd", d_scores, queries, preferred_element_type=F32)
    d_values = jnp.einsum("mhqk,mhqd->mhkd", probs_b, d_mix, preferred_element_type=F32)
    d_packed = jnp.concatenate([from_head(v) for v in (d_queries, d_keys, d_values)], axis=1).astype(BF16)
    d_qkv = dot_tn(normed_a, d_packed)
    norm_q, d_gain_attn = norm_back(dot_nt(d_packed, qkv_w), unit_a, scale_a, gain_attn)
    tokens_grad = (d_attended_q.astype(F32) + norm_q).reshape(micro, rows, quarter)

    def own_in(grad):
        pieces = grad.astype(BF16).reshape(sections, quarter, hid)
        got = lax.all_to_all(pieces, "section", split_axis=0, concat_axis=0, tiled=True)
        return got.transpose(1, 0, 2).reshape(1, quarter, sections * hid).astype(F32)

    def sum_rows(grad):
        pieces = grad.astype(BF16).reshape(sections, wide, small, grad.shape[1]).transpose(1, 0, 2, 3)
        return lax.psum_scatter(pieces, "wide", scatter_dimension=0, tiled=True)[0]

    d_cut = jnp.concatenate([sum_rows(d_qkv), sum_rows(d_in)], axis=2)
    d_cut = lax.all_to_all(d_cut, "section", split_axis=0, concat_axis=0, tiled=True).astype(F32)
    qkv_grad = d_cut[:, :, :qkv_cols].reshape(sections, small, 3, quarter).transpose(1, 2, 0, 3)
    qkv_grad = qkv_grad.reshape(small, 3 * width)
    ffn_in_grad = d_cut[:, :, qkv_cols:].transpose(1, 0, 2).reshape(small, sections * hid)
    out_grad = lax.psum_scatter(d_out.astype(BF16), "wide", scatter_dimension=0, tiled=True).astype(F32)
    ffn_back_grad = lax.psum_scatter(d_back.astype(BF16), "wide", scatter_dimension=0, tiled=True).astype(F32)
    d_gains = jnp.stack([d_gain_attn.reshape(wide, small), d_gain_ffn.reshape(wide, small)], axis=1)
    d_gains = jnp.sum(lax.all_to_all(d_gains, "wide", split_axis=0, concat_axis=0, tiled=True), axis=0)
    return (
        block_out,
        tokens_grad,
        qkv_grad,
        out_grad,
        d_gains[0],
        ffn_in_grad,
        ffn_back_grad,
        d_gains[1],
        centroids_grad,
        first_gain_grad[None],
        own_in(d_first_in),
        d_first_back[None],
        second_gain_grad[None],
        own_in(d_second_in),
        d_second_back[None],
    )


def solution(mesh):
    dense = P(("section", "wide"), None)
    dense_gain = P(("section", "wide"))
    tokens = P(None, "wide", "section")
    gain = P("wide", "section")
    expert = P("wide", "section", None)
    in_specs = (
        (tokens, tokens, P(None, "wide", None), P(), dense, dense, dense_gain, dense, dense, dense_gain)
        + (gain, gain, expert, expert, gain, expert, expert)
    )
    out_specs = (
        (tokens, tokens, dense, dense, dense_gain, dense, dense, dense_gain)
        + (gain, gain, expert, expert, gain, expert, expert)
    )
    return jax.shard_map(body, mesh=mesh, in_specs=in_specs, out_specs=out_specs, check_vma=False)
```

```python
import functools

import jax
import jax.numpy as jnp
from jax import lax
from jax.experimental import pallas as pl
from jax.experimental.pallas import tpu as pltpu
from jax.sharding import PartitionSpec as P

HEAD_SIZE = 64
F32 = jnp.float32
BF16 = jnp.bfloat16

MESH = pl.DeviceIdType.MESH
ANY = pl.BlockSpec(memory_space=pl.ANY)
VM = pl.BlockSpec(memory_space=pltpu.VMEM)
DMA = pltpu.SemaphoreType.DMA
VMEM_BYTES = 60 * 1024 * 1024
QUARTER = 256


def section_places():
    me = lax.axis_index("section")
    return me, me + 1 - 2 * lax.rem(me, 2), me + 2 - 4 * lax.div(me, 2)


def greet(peers):
    barrier = pltpu.get_barrier_semaphore()
    for peer in peers:
        pl.semaphore_signal(barrier, inc=1, device_id=peer, device_id_type=MESH)
    pl.semaphore_wait(barrier, len(peers))


def push(src, dst, send, recv, peer):
    return pltpu.make_async_remote_copy(
        src_ref=src, dst_ref=dst, send_sem=send, recv_sem=recv, device_id=peer, device_id_type=MESH
    )


def columns(which):
    return pl.ds(pl.multiple_of(which * QUARTER, QUARTER), QUARTER)


def call(kernel, out_shape, in_specs, out_specs, scratch, collective_id, *operands):
    return pl.pallas_call(
        kernel,
        out_shape=out_shape,
        in_specs=in_specs,
        out_specs=out_specs,
        scratch_shapes=scratch,
        compiler_params=pltpu.CompilerParams(
            collective_id=collective_id, has_side_effects=True, vmem_limit_bytes=VMEM_BYTES
        ),
    )(*operands)


def reduce_kernel(chunks, with_stats, *refs):
    if with_stats:
        part, stats, out, stats_out = refs[:4]
        first_in, far, far_in, s1, r1, s2, r2, st_in, st_mid, st_far, st_s, st_r = refs[4:]
    else:
        part, out, first_in, far, far_in, s1, r1, s2, r2 = refs
    me, beside, across = section_places()
    core, side = lax.rem(me, 2), lax.div(me, 2)
    greet([{"section": beside}, {"section": across}])
    rows = part.shape[0] // chunks
    beside_core = 1 - core
    sends = []
    if with_stats:
        st = push(stats, st_in, st_s.at[0], st_r.at[0], {"section": beside})
        st.start()
    for k in range(chunks):
        for which, half in ((1, 1 - side), (0, side)):
            at = pl.ds(k * rows, rows)
            c = push(
                part.at[at, columns(2 * half + beside_core)],
                first_in.at[which, at],
                s1.at[which, k],
                r1.at[which, k],
                {"section": beside},
            )
            c.start()
            sends.append(c)
    if with_stats:
        st.wait()
        st_mid[...] = stats[...] + st_in[...]
        st2 = push(st_mid, st_far, st_s.at[1], st_r.at[1], {"section": across})
        st2.start()
    crossing = []
    for k in range(chunks):
        at = pl.ds(k * rows, rows)
        sends[2 * k].wait()
        far[at] = (part[at, columns(2 * (1 - side) + core)].astype(F32) + first_in[1, at].astype(F32)).astype(BF16)
        c = push(far.at[at], far_in.at[at], s2.at[k], r2.at[k], {"section": across})
        c.start()
        crossing.append(c)
    for k in range(chunks):
        at = pl.ds(k * rows, rows)
        sends[2 * k + 1].wait()
        near = part[at, columns(me)].astype(F32) + first_in[0, at].astype(F32)
        crossing[k].wait()
        out[at] = near + far_in[at].astype(F32)
    if with_stats:
        st2.wait()
        stats_out[...] = st_mid[...] + st_far[...]


def reduce_call(part, stats, collective_id, chunks=4):
    rows, _ = part.shape
    scratch = [
        pltpu.VMEM((2, rows, QUARTER), BF16),
        pltpu.VMEM((rows, QUARTER), BF16),
        pltpu.VMEM((rows, QUARTER), BF16),
        DMA((2, chunks)),
        DMA((2, chunks)),
        DMA((chunks,)),
        DMA((chunks,)),
    ]
    out = jax.ShapeDtypeStruct((rows, QUARTER), F32)
    if stats is None:
        return call(
            functools.partial(reduce_kernel, chunks, False), out, [VM], VM, scratch, collective_id, part
        )
    st = pltpu.VMEM(stats.shape, F32)
    return call(
        functools.partial(reduce_kernel, chunks, True),
        (out, jax.ShapeDtypeStruct(stats.shape, F32)),
        [VM, VM],
        (VM, VM),
        scratch + [st, st, st, DMA((2,)), DMA((2,))],
        collective_id,
        part,
        stats,
    )


def gather_kernel(chunks, q, out, s, r):
    me, beside, across = section_places()
    greet([{"section": beside}, {"section": across}])
    rows = q.shape[0] // chunks
    copies = []
    for k in range(chunks):
        at = pl.ds(k * rows, rows)
        for kind, to in ((0, across), (1, beside)):
            c = push(q.at[at], out.at[at, columns(me)], s.at[kind, k], r.at[kind, k], {"section": to})
            c.start()
            copies.append(c)
    out[:, columns(me)] = q[...]
    for k in range(chunks):
        at = pl.ds(k * rows, rows)
        copies[2 * k].wait()
        here = out.at[at, columns(across)]
        c = push(here, here, s.at[2, k], r.at[2, k], {"section": beside})
        c.start()
        copies.append(c)
    for k in range(chunks):
        copies[2 * k + 1].wait()
        copies[2 * chunks + k].wait()


def gather_call(q, collective_id, chunks=4):
    rows = q.shape[0]
    return call(
        functools.partial(gather_kernel, chunks),
        jax.ShapeDtypeStruct((rows, 4 * QUARTER), BF16),
        [VM],
        VM,
        [DMA((3, chunks)), DMA((3, chunks))],
        collective_id,
        q,
    )


def exchange_kernel(spread, src, out, s, r):
    me, beside, across = section_places()
    w = lax.axis_index("wide")
    count = src.shape[0]
    peers = [{"wide": lax.rem(w + j, count)} for j in range(1, count)]
    greet(peers + ([{"section": beside}, {"section": across}] if spread else []))

    def place(which, block):
        return out.at[block, :, columns(which)] if spread else out.at[block]

    def wide_copy(to):
        return push(src.at[to], place(me, w), s.at[0, to], r.at[0, w], {"wide": to})

    def arrival(frm):
        return push(src.at[frm], place(me, frm), s.at[0, frm], r.at[0, frm], {"wide": frm})

    def spread_copy(kind, block, to):
        here = place(across, block) if kind == 3 else place(me, block)
        return push(here, here, s.at[kind, block], r.at[kind, block], {"section": to})

    for j in range(1, count):
        wide_copy(lax.rem(w + j, count)).start()
    if spread:
        out[w, :, columns(me)] = src[w]
    else:
        out[w] = src[w]
    for j in range(count):
        block = lax.rem(w + j, count)
        if j:
            arrival(block).wait_recv()
        if spread:
            spread_copy(1, block, across).start()
            spread_copy(2, block, beside).start()
    if spread:
        for j in range(count):
            block = lax.rem(w + j, count)
            spread_copy(1, block, across).wait_recv()
            spread_copy(3, block, beside).start()
        for j in range(count):
            block = lax.rem(w + j, count)
            spread_copy(1, block, across).wait_send()
            spread_copy(2, block, beside).wait()
            spread_copy(3, block, beside).wait()
    for j in range(1, count):
        wide_copy(lax.rem(w + j, count)).wait_send()


def exchange_call(slots, spread, collective_id):
    count, n, quarter = slots.shape
    return call(
        functools.partial(exchange_kernel, spread),
        jax.ShapeDtypeStruct((count, n, 4 * quarter if spread else quarter), BF16),
        [VM],
        VM,
        [DMA((4, count)), DMA((4, count))],
        collective_id,
        slots,
    )


def weights_kernel(qkv, inn, vec, outw, backw, first, second, tok, *refs):
    o_qkv, o_in, o_vec, o_out, o_back, o_first, o_second, o_tok = refs[:8]
    st_qkv, st_in, st_vec, loc, cut_s, cut_r, tok_s, tok_r, line_s, line_r, exp_s, exp_r = refs[8:]
    me, beside, across = section_places()
    w = lax.axis_index("wide")
    length = lax.axis_size("wide") // 2
    a, b = lax.div(w, 2), lax.rem(w, 2)
    other = 1 - b
    diagonal = beside + across - me
    peers = [beside, across, diagonal]
    barrier = pltpu.get_barrier_semaphore()
    for p in peers:
        pl.semaphore_signal(barrier, inc=1, device_id={"section": p}, device_id_type=MESH)
    pl.semaphore_signal(barrier, inc=1, device_id={"wide": 2 * a + other}, device_id_type=MESH)

    @pl.when(a > 0)
    def _():
        pl.semaphore_signal(barrier, inc=1, device_id={"wide": w - 2}, device_id_type=MESH)

    @pl.when(a < length - 1)
    def _():
        pl.semaphore_signal(barrier, inc=1, device_id={"wide": w + 2}, device_id_type=MESH)

    pl.semaphore_wait(barrier, 4 + jnp.minimum(a, 1) + jnp.minimum(length - 1 - a, 1))

    cuts = ((qkv, st_qkv), (inn, st_in), (vec, st_vec))
    sent, locals_ = [], []
    for i, (src, stage) in enumerate(cuts):
        for k, p in enumerate(peers):
            c = push(src.at[p] if i < 2 else src, stage.at[me], cut_s.at[i, k], cut_r.at[i, k], {"section": p})
            c.start()
            sent.append(c)
        c = pltpu.make_async_copy(src.at[me] if i < 2 else src, stage.at[me], loc.at[i])
        c.start()
        locals_.append(c)
    tok_c = [
        push(tok, o_tok.at[:, columns(me)], tok_s.at[k], tok_r.at[k], {"section": p})
        for k, p in enumerate((across, beside))
    ]
    for c in tok_c:
        c.start()
    own_tok = pltpu.make_async_copy(tok, o_tok.at[:, columns(me)], loc.at[3])
    own_tok.start()
    late = [own_tok]
    for i, (src, dst) in enumerate(((first, o_first), (second, o_second))):
        c = pltpu.make_async_copy(src.at[me], dst.at[me], loc.at[4 + i])
        c.start()
        late.append(c)
    exp_c = []
    for i, (src, dst) in enumerate(((first, o_first), (second, o_second))):
        for k, p in enumerate((across, diagonal, beside)):
            c = push(src.at[p], dst.at[me], exp_s.at[i, k], exp_r.at[i, k], {"section": p})
            c.start()
            exp_c.append(c)

    lines = (
        (st_qkv, o_qkv, True),
        (outw, o_out, False),
        (st_in, o_in, True),
        (backw, o_back, False),
        (st_vec, o_vec, False),
    )
    staged = {0: 0, 2: 1, 4: 2}

    def item(i, which, kind, to, own=False):
        src, dst, _ = lines[i]
        return push(
            src if own else dst.at[which], dst.at[which], line_s.at[kind, i, which], line_r.at[i, which], {"wide": to}
        )

    up, down, pair = 0, 1, 2

    def along(i, which, kind, own, act):
        if kind == pair:
            act(item(i, which, pair, 2 * a + other, own))
            return

        @pl.when((a < length - 1) if kind == up else (a > 0))
        def _():
            act(item(i, which, kind, w + 2 if kind == up else w - 2, own))

    def start(c):
        c.start()

    def done(c):
        c.wait_send()

    for i, (src, dst, _) in enumerate(lines):
        if i in staged:
            j = staged[i]
            for k in range(3):
                sent[3 * j + k].wait_recv()
            locals_[j].wait()
        for kind in (up, down, pair):
            along(i, w, kind, True, start)
        c = pltpu.make_async_copy(src, dst.at[w], loc.at[6 + i])
        c.start()
        late.append(c)
    tok_c[0].wait_recv()
    spot = o_tok.at[:, columns(across)]
    tok_fwd = push(spot, spot, tok_s.at[2], tok_r.at[2], {"section": beside})
    tok_fwd.start()

    mate = 2 * a + other

    def arrived(i, which):
        item(i, which, pair, mate).wait_recv()

    for i in range(len(lines)):
        if not lines[i][2]:
            arrived(i, mate)
            for kind in (up, down):
                along(i, mate, kind, False, start)

    def step(t, carry):
        for i in range(len(lines)):
            for kind, there, ok in ((up, a - t, a - t >= 0), (down, a + t, a + t < length)):

                @pl.when(ok)
                def _():
                    arrived(i, 2 * there + b)
                    along(i, 2 * there + b, kind, False, start)
                    if lines[i][2]:
                        along(i, 2 * there + b, pair, False, start)
                    else:
                        arrived(i, 2 * there + other)
                        along(i, 2 * there + other, kind, False, start)

        return carry

    lax.fori_loop(1, length, step, 0)
    for i in range(len(lines)):
        if lines[i][2]:
            lax.fori_loop(0, length, lambda there, carry: (arrived(i, 2 * there + other), carry)[1], 0)
        for kind in (up, down, pair):
            along(i, w, kind, True, done)
        if not lines[i][2]:
            for kind in (up, down):
                along(i, mate, kind, False, done)

    def finish(t, carry):
        for i in range(len(lines)):
            for kind, there, ok in ((up, a - t, a - t >= 0), (down, a + t, a + t < length)):

                @pl.when(ok)
                def _():
                    along(i, 2 * there + b, kind, False, done)
                    if lines[i][2]:
                        along(i, 2 * there + b, pair, False, done)
                    else:
                        along(i, 2 * there + other, kind, False, done)

        return carry

    lax.fori_loop(1, length, finish, 0)
    for c in sent:
        c.wait_send()
    tok_c[0].wait_send()
    tok_c[1].wait()
    tok_fwd.wait()
    for c in exp_c:
        c.wait()
    for c in late:
        c.wait()


def weights_call(qkv, inn, vec, outw, backw, first, second, tok, wide, collective_id):
    outs = [
        ((wide, *qkv.shape), BF16),
        ((wide, *inn.shape), BF16),
        ((wide, 4, *vec.shape), F32),
        ((wide, *outw.shape), BF16),
        ((wide, *backw.shape), BF16),
        (first.shape, BF16),
        (second.shape, BF16),
        ((tok.shape[0], 4 * QUARTER), BF16),
    ]
    return call(
        weights_kernel,
        tuple(jax.ShapeDtypeStruct(*o) for o in outs),
        [ANY] * 8,
        tuple([ANY] * 8),
        [
            pltpu.VMEM(qkv.shape, BF16),
            pltpu.VMEM(inn.shape, BF16),
            pltpu.VMEM((4, *vec.shape), F32),
            DMA((11,)),
            DMA((3, 3)),
            DMA((3, 3)),
            DMA((3,)),
            DMA((3,)),
            DMA((3, 5, wide)),
            DMA((5, wide)),
            DMA((2, 3)),
            DMA((2, 3)),
        ],
        collective_id,
        qkv,
        inn,
        vec,
        outw,
        backw,
        first,
        second,
        tok,
    )


GROUP = 32


def add_rows(dst, left, right):
    rows = dst.shape[0]
    step = min(rows, GROUP)

    def one(j, carry):
        at = pl.ds(pl.multiple_of(j * step, step), step)
        dst[at] = (left[at].astype(F32) + right[at].astype(F32)).astype(dst.dtype)
        return carry

    lax.fori_loop(0, rows // step, one, 0)


def gradients_kernel(*refs):
    count = 5
    src = refs[:count]
    first, second = refs[count : count + 2]
    o_qkv, o_in, o_out, o_back, o_gain, o_first, o_second = refs[7:14]
    acc = refs[14:19]
    line_in = refs[19:24]
    pair_in = refs[24:29]
    (st_qkv, st_in, loc, exp_s, exp_r, cut_s, cut_r, pair_s, pair_r, line_s, line_r) = refs[29:]
    me, beside, across = section_places()
    diagonal = beside + across - me
    w = lax.axis_index("wide")
    length = lax.axis_size("wide") // 2
    a, b = lax.div(w, 2), lax.rem(w, 2)
    other = 1 - b
    mate = {"wide": 2 * a + other}
    peers = [beside, across, diagonal]
    barrier = pltpu.get_barrier_semaphore()
    for p in peers:
        pl.semaphore_signal(barrier, inc=1, device_id={"section": p}, device_id_type=MESH)
    pl.semaphore_signal(barrier, inc=1, device_id=mate, device_id_type=MESH)

    @pl.when(a > 0)
    def _():
        pl.semaphore_signal(barrier, inc=1, device_id={"wide": w - 2}, device_id_type=MESH)

    @pl.when(a < length - 1)
    def _():
        pl.semaphore_signal(barrier, inc=1, device_id={"wide": w + 2}, device_id_type=MESH)

    pl.semaphore_wait(barrier, 4 + jnp.minimum(a, 1) + jnp.minimum(length - 1 - a, 1))

    pair_first = (True, True, False, False, False)

    def pair_copy(i, there):
        return push(src[i].at[2 * there + other], pair_in[i].at[there], pair_s.at[i, there], pair_r.at[i, there], mate)

    for i in range(count):
        if pair_first[i]:
            lax.fori_loop(0, length, lambda t, c, i=i: (pair_copy(i, t).start(), c)[1], 0)

    late = []
    for i, (s, d) in enumerate(((first, o_first), (second, o_second))):
        c = pltpu.make_async_copy(s.at[me], d.at[me], loc.at[i])
        c.start()
        late.append(c)
        for k, p in enumerate((across, diagonal, beside)):
            c = push(s.at[p], d.at[me], exp_s.at[i, k], exp_r.at[i, k], {"section": p})
            c.start()
            late.append(c)

    def slots(i, there):
        if pair_first[i]:
            return [(there, 2 * there + b)]
        return [(2 * there, 2 * there), (2 * there + 1, 2 * there + 1)]

    def line_copy(i, block, to_block, to):
        return push(acc[i].at[block], line_in[i].at[to_block], line_s.at[i, block], line_r.at[i, to_block], {"wide": to})

    def wide_of(i):
        return 1 if pair_first[i] else 2

    def ready(i, there, block, own):
        if pair_first[i]:
            pair_copy(i, there).wait_recv()
            add_rows(acc[i].at[block], src[i].at[own], pair_in[i].at[there])
        else:
            acc[i][block] = src[i][own]

    def flow(i, there, from_edge, to):
        n = wide_of(i)
        for j, (block, own) in enumerate(slots(i, there)):
            ready(i, there, block, own)

            @pl.when(from_edge)
            def _():
                line_copy(i, block, block, w).wait_recv()
                add_rows(acc[i].at[block], acc[i].at[block], line_in[i].at[block])

            if to == "down":
                line_copy(i, block, block, w - 2).start()
            else:
                target = jnp.where(there == a + 1, n * length + j, block)
                line_copy(i, block, target, w + 2).start()

    def step(t, carry):
        high = length - 1 - t
        for i in range(count):

            @pl.when(t < a)
            def _():
                flow(i, t, a < length - 1, "down")

            @pl.when(high > a)
            def _():
                flow(i, high, a > 0, "up")

        return carry

    lax.fori_loop(0, length, step, 0)
    finals = []
    for i in range(count):
        n = wide_of(i)
        for j, (block, own) in enumerate(slots(i, a)):
            ready(i, a, block, own)

            @pl.when(a < length - 1)
            def _():
                line_copy(i, block, block, w).wait_recv()
                add_rows(acc[i].at[block], acc[i].at[block], line_in[i].at[block])

            @pl.when(a > 0)
            def _():
                line_copy(i, block, n * length + j, w).wait_recv()
                add_rows(acc[i].at[block], acc[i].at[block], line_in[i].at[n * length + j])

        if not pair_first[i]:
            c = push(acc[i].at[2 * a + other], pair_in[i].at[0], pair_s.at[i, 0], pair_r.at[i, 0], mate)
            c.start()
            finals.append(c)
        else:
            out, k0 = ((o_qkv, 0), (o_in, 1))[i]
            st = (st_qkv, st_in)[i]
            small = st.shape[1]
            for p in range(4):
                st[p] = acc[i][a, pl.ds(p * small, small)]
            for k, p in enumerate(peers):
                c = push(st.at[p], out.at[me], cut_s.at[i, k], cut_r.at[i, k], {"section": p})
                c.start()
                late.append(c)
            c = pltpu.make_async_copy(st.at[me], out.at[me], loc.at[2 + i])
            c.start()
            late.append(c)
    for i, out in ((2, o_out), (3, o_back), (4, o_gain)):
        finals[i - 2].wait_recv()
        add_rows(out, acc[i].at[2 * a + b], pair_in[i].at[0])
    for c in finals:
        c.wait_send()
    for c in late:
        c.wait()

    def finish(t, carry):
        for i in range(count):
            if pair_first[i]:
                pair_copy(i, t).wait_send()

            @pl.when(t != a)
            def _():
                for block, _ in slots(i, t):
                    line_copy(i, block, block, w).wait_send()

        return carry

    lax.fori_loop(0, length, finish, 0)


def gradients_call(dense, first, second, collective_id):
    wide = dense[0].shape[0]
    length = wide // 2
    shapes = [d.shape[1:] for d in dense]
    kinds = [d.dtype for d in dense]
    small = shapes[0][0] // 4
    first_count = [length, length, wide, wide, wide]
    in_count = [length + 1, length + 1, wide + 2, wide + 2, wide + 2]
    pair_count = [length, length, 1, 1, 1]
    outs = [((4, small, shapes[0][1]), BF16), ((4, small, shapes[1][1]), BF16)]
    outs += [(s, F32) for s in shapes[2:]] + [(first.shape, BF16), (second.shape, BF16)]
    scratch = [pltpu.VMEM((n, *s), k) for n, s, k in zip(first_count, shapes, kinds)]
    scratch += [pltpu.VMEM((n, *s), k) for n, s, k in zip(in_count, shapes, kinds)]
    scratch += [pltpu.VMEM((n, *s), k) for n, s, k in zip(pair_count, shapes, kinds)]
    scratch += [
        pltpu.VMEM((4, small, shapes[0][1]), BF16),
        pltpu.VMEM((4, small, shapes[1][1]), BF16),
        DMA((4,)),
        DMA((2, 3)),
        DMA((2, 3)),
        DMA((2, 3)),
        DMA((2, 3)),
        DMA((5, length)),
        DMA((5, length)),
        DMA((5, wide)),
        DMA((5, wide + 2)),
    ]
    return call(
        gradients_kernel,
        tuple(jax.ShapeDtypeStruct(*o) for o in outs),
        [VM] * 5 + [ANY, ANY],
        (ANY, ANY, VM, VM, VM, ANY, ANY),
        scratch,
        collective_id,
        *dense,
        first,
        second,
    )


def dot(left, right):
    return jnp.dot(left, right, preferred_element_type=F32)


def dot_nt(left, right):
    return lax.dot_general(left, right, (((1,), (1,)), ((), ())), preferred_element_type=F32)


def dot_tn(left, right):
    return lax.dot_general(left, right, (((0,), (0,)), ((), ())), preferred_element_type=F32)


def gelu_value(v):
    return 0.5 * v * (1.0 + lax.erf(v * 0.7071067811865476))


def gelu_slope(v):
    return (
        0.5 * (1.0 + lax.erf(v * 0.7071067811865476))
        + v * jnp.exp(-0.5 * v * v) * 0.3989422804014327
    )


def unit_norm(v):
    centred = v - jnp.mean(v, axis=-1, keepdims=True)
    scale = lax.rsqrt(jnp.mean(centred * centred, axis=-1, keepdims=True) + 1e-05)
    return centred * scale, scale


IDS = {}


def id_of(*key):
    return IDS.setdefault(key, len(IDS))


def reduce_quarters(part, stats=None):
    return reduce_call(part.astype(BF16), stats, id_of("reduce", part.shape, stats is None))


def gather_quarters(quarter):
    return gather_call(quarter, id_of("gather", quarter.shape))


def wide_exchange(slots, spread):
    return exchange_call(slots, spread, id_of("exchange", spread))


def attention_probs(queries, keys, lengths):
    rows = queries.shape[2]
    raw = jnp.einsum("mhqd,mhkd->mhqk", queries, keys, preferred_element_type=F32)
    pos = jnp.arange(rows, dtype=jnp.int32)
    same = pos[None, :, None] // lengths[:, None, None] == pos[None, None, :] // lengths[:, None, None]
    allowed = (pos[:, None] >= pos[None, :])[None] & same
    scores = jnp.where(allowed[:, None], raw * HEAD_SIZE ** (-0.5), -1e30)
    highest = jnp.max(scores, axis=-1, keepdims=True)
    expo = jnp.exp(scores - highest)
    return expo / jnp.sum(expo, axis=-1, keepdims=True)


def body(
    tokens_in,
    cotangent,
    routes,
    seq_lengths,
    qkv_weight,
    out_weight,
    attn_gain,
    ffn_in,
    ffn_back,
    ffn_gain,
    centroids,
    first_gain,
    first_in,
    first_back,
    second_gain,
    second_in,
    second_back,
):
    sections = lax.axis_size("section")
    wide = lax.axis_size("wide")
    section_id = lax.axis_index("section")
    wide_id = lax.axis_index("wide")
    micro, rows, quarter = tokens_in.shape
    width = quarter * sections
    cap = 5 * rows // (4 * wide)
    tok_rows = micro * rows
    hid = first_back.shape[1]
    small = qkv_weight.shape[0]
    qkv_cols = qkv_weight.shape[1] // sections

    qkv_cut = (
        qkv_weight.reshape(small, 3, sections, quarter).transpose(2, 0, 1, 3).reshape(sections, small, qkv_cols)
    )
    in_cut = ffn_in.reshape(small, sections, hid).transpose(1, 0, 2)
    vectors = jnp.concatenate([first_gain[0], second_gain[0], centroids[0], attn_gain, ffn_gain]).astype(F32)
    vectors = jnp.pad(vectors, (0, 1024 - vectors.shape[0])).reshape(8, 128)
    tokens_q = tokens_in.reshape(tok_rows, quarter)

    def slice_in(weight):
        return weight[0].reshape(quarter, sections, hid).transpose(1, 0, 2)

    qkv_w, in_w, vectors, out_w, back_w, first_w, second_w, tokens = weights_call(
        qkv_cut,
        in_cut,
        vectors,
        out_weight,
        ffn_back,
        slice_in(first_in),
        slice_in(second_in),
        tokens_q,
        wide,
        id_of("weights"),
    )
    qkv_w = qkv_w.transpose(1, 0, 2, 3).reshape(width, qkv_cols)
    in_w = in_w.transpose(1, 0, 2, 3).reshape(width, hid)
    out_w = out_w.reshape(quarter, width)
    back_w = back_w.reshape(hid, width)
    first_w = first_w.reshape(width, hid)
    second_w = second_w.reshape(width, hid)
    vectors = vectors.reshape(wide, sections, 1024).transpose(1, 0, 2)
    own = lax.dynamic_index_in_dim(vectors, wide_id, axis=1, keepdims=False)
    gain_first = own[:, :quarter].reshape(1, width)
    gain_second = own[:, quarter : 2 * quarter].reshape(1, width)
    centre = own[:, 2 * quarter : 3 * quarter].reshape(1, width)
    gain_attn = vectors[:, :, 3 * quarter : 3 * quarter + small].reshape(1, width)
    gain_ffn = vectors[:, :, 3 * quarter + small : 3 * quarter + 2 * small].reshape(1, width)
    own_quarter = lambda v: lax.dynamic_slice_in_dim(v, section_id * quarter, quarter, axis=1)
    first_b = first_back[0]
    second_b = second_back[0]

    experts = jnp.arange(wide, dtype=jnp.int32)
    choose = (routes == experts).astype(jnp.int32)
    upto = (jnp.arange(rows)[:, None] >= jnp.arange(rows)[None, :]).astype(BF16)
    ranking = jnp.einsum("rk,mke->mre", upto, choose.astype(BF16), preferred_element_type=F32).astype(jnp.int32) - 1
    slot_of = routes[:, :, 0] * cap + jnp.sum(ranking * choose, axis=2)
    onehot = (jnp.arange(wide * cap, dtype=jnp.int32)[None, :, None] == slot_of[:, None, :]).astype(BF16)

    def to_experts(rows_q):
        packed = jnp.einsum("msr,mrd->msd", onehot, rows_q.reshape(micro, rows, quarter), preferred_element_type=F32)
        packed = packed.astype(BF16).reshape(micro, wide, cap, quarter).transpose(1, 0, 2, 3)
        return wide_exchange(packed.reshape(wide, micro * cap, quarter), True).reshape(wide * micro * cap, width)

    def to_tokens(slots_q):
        back = wide_exchange(slots_q.reshape(wide, micro * cap, quarter), False)
        back = back.reshape(wide, micro, cap, quarter).transpose(1, 0, 2, 3).reshape(micro, wide * cap, quarter)
        got = jnp.einsum("msr,msd->mrd", onehot, back, preferred_element_type=F32)
        return got.astype(BF16).reshape(tok_rows, quarter)

    unit_a, scale_a = unit_norm(tokens.astype(F32))
    normed_a = (unit_a * gain_attn).astype(BF16)
    packed = dot(normed_a, qkv_w).astype(BF16)
    heads = quarter // HEAD_SIZE

    def by_head(v):
        return v.reshape(micro, rows, heads, HEAD_SIZE).transpose(0, 2, 1, 3)

    def from_head(v):
        return v.transpose(0, 2, 1, 3).reshape(tok_rows, quarter)

    queries, keys, values = (by_head(packed[:, i * quarter : (i + 1) * quarter]) for i in range(3))
    probs = attention_probs(queries, keys, seq_lengths)
    probs_b = probs.astype(BF16)
    mixed = from_head(
        jnp.einsum("mhqk,mhkd->mhqd", probs_b, values, preferred_element_type=F32).astype(BF16)
    )
    attended_q = (tokens_q.astype(F32) + reduce_quarters(dot(mixed, out_w))).astype(BF16)
    attended = gather_quarters(attended_q)

    def branch(v, w_in, w_back, gain):
        unit, scale = unit_norm(v.astype(F32))
        normed = (unit * gain).astype(BF16)
        pre = dot(normed, w_in)
        hidden = gelu_value(pre).astype(BF16)
        return (normed, unit, scale, pre, hidden), dot(hidden, w_back)

    def branch_back(grad, saved, w_in, w_back, gain, more=None):
        normed, unit, scale, pre, hidden = saved
        d_back = dot_tn(hidden, grad)
        d_pre = (dot_nt(grad, w_back) * gelu_slope(pre)).astype(BF16)
        d_in = dot_tn(normed, d_pre)
        return d_in, d_back, norm_back(dot_nt(d_pre, w_in), unit, scale, gain, more)

    def norm_back(d_part, unit, scale, gain, more=None):
        d_unit = d_part * gain
        sums = jnp.stack([jnp.sum(d_unit, axis=1), jnp.sum(d_unit * unit, axis=1)])
        if more is not None:
            sums = jnp.concatenate([sums, more])
        d_q, sums = reduce_quarters(d_part, jnp.pad(sums, ((0, 8 - sums.shape[0]), (0, 0))))
        extra, sums = sums[2], sums / width
        unit_q = own_quarter(unit)
        d_rows = scale * (d_q * own_quarter(gain) - sums[0][:, None] - unit_q * sums[1][:, None])
        return d_rows, jnp.sum(d_q * unit_q, axis=0), extra

    saved_d, part = branch(attended, in_w, back_w, gain_ffn)
    fed_q = (attended_q.astype(F32) + reduce_quarters(part)).astype(BF16)
    routed = to_experts(fed_q)
    routed_q = own_quarter(routed)
    d_mixed = to_experts(cotangent.reshape(tok_rows, quarter)).astype(F32)
    d_mixed_q = own_quarter(d_mixed)
    saved_1, part = branch(routed, first_w, first_b, gain_first)
    first_q = (routed_q.astype(F32) + reduce_quarters(part)).astype(BF16)
    first = gather_quarters(first_q)
    saved_2, part = branch(first, second_w, second_b, gain_second)
    gate = jax.nn.sigmoid(jnp.sum(routed.astype(F32) * centre, axis=-1, keepdims=True))
    second_q = first_q.astype(F32) + reduce_quarters(part)
    mixed_q = routed_q.astype(F32) + gate * second_q
    block_out = to_tokens(mixed_q.astype(BF16)).reshape(micro, rows, quarter)

    d_second = gate * d_mixed
    d_second_q = gate * d_mixed_q
    d_second_in, d_second_back, (norm_q, second_gain_grad, d_logit) = branch_back(
        d_second.astype(BF16), saved_2, second_w, second_b, gain_second, jnp.sum(d_mixed_q * second_q, axis=-1)[None]
    )
    d_logit = d_logit[:, None] * gate * (1.0 - gate)
    centroids_grad = jnp.sum(d_logit * routed_q.astype(F32), axis=0)[None]
    d_gated_q = (d_mixed_q + d_logit * own_quarter(centre)).astype(BF16)
    d_first_q = (d_second_q + norm_q).astype(BF16)
    d_first_in, d_first_back, (norm_q, first_gain_grad, _) = branch_back(
        gather_quarters(d_first_q), saved_1, first_w, first_b, gain_first
    )
    d_routed_q = (d_first_q.astype(F32) + norm_q + d_gated_q.astype(F32)).astype(BF16)
    d_fed_q = to_tokens(d_routed_q)
    d_in, d_back, (norm_q, d_gain_ffn, _) = branch_back(gather_quarters(d_fed_q), saved_d, in_w, back_w, gain_ffn)
    d_attended_q = (d_fed_q.astype(F32) + norm_q).astype(BF16)
    d_attended = gather_quarters(d_attended_q)
    d_out = dot_tn(mixed, d_attended)
    d_mix = by_head(dot_nt(d_attended, out_w).astype(BF16))
    d_probs = jnp.einsum("mhqd,mhkd->mhqk", d_mix, values, preferred_element_type=F32)
    delta = jnp.sum(probs * d_probs, axis=-1, keepdims=True)
    d_scores = (probs * (d_probs - delta) * HEAD_SIZE ** (-0.5)).astype(BF16)
    d_queries = jnp.einsum("mhqk,mhkd->mhqd", d_scores, keys, preferred_element_type=F32)
    d_keys = jnp.einsum("mhqk,mhqd->mhkd", d_scores, queries, preferred_element_type=F32)
    d_values = jnp.einsum("mhqk,mhqd->mhkd", probs_b, d_mix, preferred_element_type=F32)
    d_packed = jnp.concatenate([from_head(v) for v in (d_queries, d_keys, d_values)], axis=1).astype(BF16)
    d_qkv = dot_tn(normed_a, d_packed)
    norm_q, d_gain_attn, _ = norm_back(dot_nt(d_packed, qkv_w), unit_a, scale_a, gain_attn)
    tokens_grad = (d_attended_q.astype(F32) + norm_q).reshape(micro, rows, quarter)

    def by_wide(grad):
        pieces = grad.astype(BF16).reshape(sections, wide, small, grad.shape[1]).transpose(1, 0, 2, 3)
        return pieces.reshape(wide, sections * small, grad.shape[1])

    def own_in(pieces):
        return pieces.transpose(1, 0, 2).reshape(1, quarter, sections * hid).astype(F32)

    d_gains = jnp.stack([d_gain_attn.reshape(wide, small), d_gain_ffn.reshape(wide, small)], axis=1)
    d_gains = jnp.pad(d_gains, ((0, 0), (0, 6), (0, 128 - small)))
    qkv_grad, ffn_in_grad, out_grad, ffn_back_grad, d_gains, d_first_in, d_second_in = gradients_call(
        (
            by_wide(d_qkv),
            by_wide(d_in),
            d_out.astype(BF16).reshape(wide, small, width),
            d_back.astype(BF16).reshape(wide, hid // wide, width),
            d_gains,
        ),
        d_first_in.astype(BF16).reshape(sections, quarter, hid),
        d_second_in.astype(BF16).reshape(sections, quarter, hid),
        id_of("gradients"),
    )
    qkv_grad = qkv_grad.astype(F32).reshape(sections, small, 3, quarter).transpose(1, 2, 0, 3)
    qkv_grad = qkv_grad.reshape(small, 3 * width)
    ffn_in_grad = ffn_in_grad.astype(F32).transpose(1, 0, 2).reshape(small, sections * hid)
    return (
        block_out,
        tokens_grad,
        qkv_grad,
        out_grad,
        d_gains[0, :small],
        ffn_in_grad,
        ffn_back_grad,
        d_gains[1, :small],
        centroids_grad,
        first_gain_grad[None],
        own_in(d_first_in),
        d_first_back[None],
        second_gain_grad[None],
        own_in(d_second_in),
        d_second_back[None],
    )


def solution(mesh):
    dense = P(("section", "wide"), None)
    dense_gain = P(("section", "wide"))
    tokens = P(None, "wide", "section")
    gain = P("wide", "section")
    expert = P("wide", "section", None)
    in_specs = (
        (tokens, tokens, P(None, "wide", None), P(), dense, dense, dense_gain, dense, dense, dense_gain)
        + (gain, gain, expert, expert, gain, expert, expert)
    )
    out_specs = (
        (tokens, tokens, dense, dense, dense_gain, dense, dense, dense_gain)
        + (gain, gain, expert, expert, gain, expert, expert)
    )
    return jax.shard_map(body, mesh=mesh, in_specs=in_specs, out_specs=out_specs, check_vma=False)
```

```python
import functools

import jax
import jax.numpy as jnp
from jax import lax
from jax.experimental import pallas as pl
from jax.experimental.pallas import tpu as pltpu
from jax.sharding import PartitionSpec as P

HEAD_SIZE = 64
F32 = jnp.float32
BF16 = jnp.bfloat16

MESH = pl.DeviceIdType.MESH
ANY = pl.BlockSpec(memory_space=pl.ANY)
VM = pl.BlockSpec(memory_space=pltpu.VMEM)
DMA = pltpu.SemaphoreType.DMA
VMEM_BYTES = 60 * 1024 * 1024
QUARTER = 256


def section_places():
    me = lax.axis_index("section")
    return me, me + 1 - 2 * lax.rem(me, 2), me + 2 - 4 * lax.div(me, 2)


def greet(peers):
    barrier = pltpu.get_barrier_semaphore()
    for peer in peers:
        pl.semaphore_signal(barrier, inc=1, device_id=peer, device_id_type=MESH)
    pl.semaphore_wait(barrier, len(peers))


def push(src, dst, send, recv, peer):
    return pltpu.make_async_remote_copy(
        src_ref=src, dst_ref=dst, send_sem=send, recv_sem=recv, device_id=peer, device_id_type=MESH
    )


def columns(which):
    return pl.ds(pl.multiple_of(which * QUARTER, QUARTER), QUARTER)


def call(kernel, out_shape, in_specs, out_specs, scratch, collective_id, *operands):
    return pl.pallas_call(
        kernel,
        out_shape=out_shape,
        in_specs=in_specs,
        out_specs=out_specs,
        scratch_shapes=scratch,
        compiler_params=pltpu.CompilerParams(
            collective_id=collective_id, has_side_effects=True, vmem_limit_bytes=VMEM_BYTES
        ),
    )(*operands)


def reduce_kernel(chunks, with_stats, *refs):
    if with_stats:
        part, stats, out, stats_out = refs[:4]
        first_in, far, far_in, s1, r1, s2, r2, st_in, st_mid, st_far, st_s, st_r = refs[4:]
    else:
        part, out, first_in, far, far_in, s1, r1, s2, r2 = refs
    me, beside, across = section_places()
    core, side = lax.rem(me, 2), lax.div(me, 2)
    greet([{"section": beside}, {"section": across}])
    rows = part.shape[0] // chunks
    beside_core = 1 - core
    sends = []
    if with_stats:
        st = push(stats, st_in, st_s.at[0], st_r.at[0], {"section": beside})
        st.start()
    for k in range(chunks):
        for which, half in ((1, 1 - side), (0, side)):
            at = pl.ds(k * rows, rows)
            c = push(
                part.at[at, columns(2 * half + beside_core)],
                first_in.at[which, at],
                s1.at[which, k],
                r1.at[which, k],
                {"section": beside},
            )
            c.start()
            sends.append(c)
    if with_stats:
        st.wait()
        st_mid[...] = stats[...] + st_in[...]
        st2 = push(st_mid, st_far, st_s.at[1], st_r.at[1], {"section": across})
        st2.start()
    crossing = []
    for k in range(chunks):
        at = pl.ds(k * rows, rows)
        sends[2 * k].wait()
        far[at] = (part[at, columns(2 * (1 - side) + core)].astype(F32) + first_in[1, at].astype(F32)).astype(BF16)
        c = push(far.at[at], far_in.at[at], s2.at[k], r2.at[k], {"section": across})
        c.start()
        crossing.append(c)
    for k in range(chunks):
        at = pl.ds(k * rows, rows)
        sends[2 * k + 1].wait()
        near = part[at, columns(me)].astype(F32) + first_in[0, at].astype(F32)
        crossing[k].wait()
        out[at] = near + far_in[at].astype(F32)
    if with_stats:
        st2.wait()
        stats_out[...] = st_mid[...] + st_far[...]


def reduce_call(part, stats, collective_id, chunks=4):
    rows, _ = part.shape
    scratch = [
        pltpu.VMEM((2, rows, QUARTER), BF16),
        pltpu.VMEM((rows, QUARTER), BF16),
        pltpu.VMEM((rows, QUARTER), BF16),
        DMA((2, chunks)),
        DMA((2, chunks)),
        DMA((chunks,)),
        DMA((chunks,)),
    ]
    out = jax.ShapeDtypeStruct((rows, QUARTER), F32)
    if stats is None:
        return call(
            functools.partial(reduce_kernel, chunks, False), out, [VM], VM, scratch, collective_id, part
        )
    st = pltpu.VMEM(stats.shape, F32)
    return call(
        functools.partial(reduce_kernel, chunks, True),
        (out, jax.ShapeDtypeStruct(stats.shape, F32)),
        [VM, VM],
        (VM, VM),
        scratch + [st, st, st, DMA((2,)), DMA((2,))],
        collective_id,
        part,
        stats,
    )


def gather_kernel(chunks, q, out, s, r):
    me, beside, across = section_places()
    greet([{"section": beside}, {"section": across}])
    rows = q.shape[0] // chunks
    copies = []
    for k in range(chunks):
        at = pl.ds(k * rows, rows)
        for kind, to in ((0, across), (1, beside)):
            c = push(q.at[at], out.at[at, columns(me)], s.at[kind, k], r.at[kind, k], {"section": to})
            c.start()
            copies.append(c)
    out[:, columns(me)] = q[...]
    for k in range(chunks):
        at = pl.ds(k * rows, rows)
        copies[2 * k].wait()
        here = out.at[at, columns(across)]
        c = push(here, here, s.at[2, k], r.at[2, k], {"section": beside})
        c.start()
        copies.append(c)
    for k in range(chunks):
        copies[2 * k + 1].wait()
        copies[2 * chunks + k].wait()


def gather_call(q, collective_id, chunks=4):
    rows = q.shape[0]
    return call(
        functools.partial(gather_kernel, chunks),
        jax.ShapeDtypeStruct((rows, 4 * QUARTER), BF16),
        [VM],
        VM,
        [DMA((3, chunks)), DMA((3, chunks))],
        collective_id,
        q,
    )


def exchange_kernel(spread, src, out, s, r):
    me, beside, across = section_places()
    w = lax.axis_index("wide")
    count = src.shape[0]
    peers = [{"wide": lax.rem(w + j, count)} for j in range(1, count)]
    greet(peers + ([{"section": beside}, {"section": across}] if spread else []))

    def place(which, block):
        return out.at[block, :, columns(which)] if spread else out.at[block]

    def wide_copy(to):
        return push(src.at[to], place(me, w), s.at[0, to], r.at[0, w], {"wide": to})

    def arrival(frm):
        return push(src.at[frm], place(me, frm), s.at[0, frm], r.at[0, frm], {"wide": frm})

    def spread_copy(kind, block, to):
        here = place(across, block) if kind == 3 else place(me, block)
        return push(here, here, s.at[kind, block], r.at[kind, block], {"section": to})

    for j in range(1, count):
        wide_copy(lax.rem(w + j, count)).start()
    if spread:
        out[w, :, columns(me)] = src[w]
    else:
        out[w] = src[w]
    for j in range(count):
        block = lax.rem(w + j, count)
        if j:
            arrival(block).wait_recv()
        if spread:
            spread_copy(1, block, across).start()
            spread_copy(2, block, beside).start()
    if spread:
        for j in range(count):
            block = lax.rem(w + j, count)
            spread_copy(1, block, across).wait_recv()
            spread_copy(3, block, beside).start()
        for j in range(count):
            block = lax.rem(w + j, count)
            spread_copy(1, block, across).wait_send()
            spread_copy(2, block, beside).wait()
            spread_copy(3, block, beside).wait()
    for j in range(1, count):
        wide_copy(lax.rem(w + j, count)).wait_send()


def exchange_call(slots, spread, collective_id):
    count, n, quarter = slots.shape
    return call(
        functools.partial(exchange_kernel, spread),
        jax.ShapeDtypeStruct((count, n, 4 * quarter if spread else quarter), BF16),
        [VM],
        VM,
        [DMA((4, count)), DMA((4, count))],
        collective_id,
        slots,
    )


def weights_kernel(qkv, inn, vec, outw, backw, first, second, tok, *refs):
    o_qkv, o_in, o_vec, o_out, o_back, o_first, o_second, o_tok = refs[:8]
    st_qkv, st_in, st_vec, loc, cut_s, cut_r, tok_s, tok_r, line_s, line_r, exp_s, exp_r = refs[8:]
    me, beside, across = section_places()
    w = lax.axis_index("wide")
    length = lax.axis_size("wide") // 2
    a, b = lax.div(w, 2), lax.rem(w, 2)
    other = 1 - b
    diagonal = beside + across - me
    peers = [beside, across, diagonal]
    barrier = pltpu.get_barrier_semaphore()
    for p in peers:
        pl.semaphore_signal(barrier, inc=1, device_id={"section": p}, device_id_type=MESH)
    pl.semaphore_signal(barrier, inc=1, device_id={"wide": 2 * a + other}, device_id_type=MESH)

    @pl.when(a > 0)
    def _():
        pl.semaphore_signal(barrier, inc=1, device_id={"wide": w - 2}, device_id_type=MESH)

    @pl.when(a < length - 1)
    def _():
        pl.semaphore_signal(barrier, inc=1, device_id={"wide": w + 2}, device_id_type=MESH)

    pl.semaphore_wait(barrier, 4 + jnp.minimum(a, 1) + jnp.minimum(length - 1 - a, 1))

    hid = o_first.shape[2]
    width = 4 * QUARTER
    sent, local_cuts = [], []

    def part_of(src, start, count):
        return src.at[:, pl.ds(pl.multiple_of(start, 128), count)]

    def cuts_for(p):
        got = [
            (0, part_of(qkv, j * width + p * QUARTER, QUARTER), st_qkv.at[me, :, pl.ds(j * QUARTER, QUARTER)])
            for j in range(3)
        ]
        return got + [(1, part_of(inn, p * hid, hid), st_in.at[me]), (2, vec, st_vec.at[me])]

    for k, p in enumerate(peers):
        for n, (i, src, dst) in enumerate(cuts_for(p)):
            c = push(src, dst, cut_s.at[n, k], cut_r.at[n, k], {"section": p})
            c.start()
            sent.append((i, c))
    for n, (i, src, dst) in enumerate(cuts_for(me)):
        c = pltpu.make_async_copy(src, dst, loc.at[11 + n])
        c.start()
        local_cuts.append((i, c))
    tok_c = [
        push(tok, o_tok.at[:, columns(me)], tok_s.at[k], tok_r.at[k], {"section": p})
        for k, p in enumerate((across, beside))
    ]
    for c in tok_c:
        c.start()
    own_tok = pltpu.make_async_copy(tok, o_tok.at[:, columns(me)], loc.at[3])
    own_tok.start()
    late = [own_tok]
    for i, (src, dst) in enumerate(((first, o_first), (second, o_second))):
        c = pltpu.make_async_copy(part_of(src, me * hid, hid), dst.at[me], loc.at[4 + i])
        c.start()
        late.append(c)
    exp_c = []
    for i, (src, dst) in enumerate(((first, o_first), (second, o_second))):
        for k, p in enumerate((across, diagonal, beside)):
            c = push(part_of(src, p * hid, hid), dst.at[me], exp_s.at[i, k], exp_r.at[i, k], {"section": p})
            c.start()
            exp_c.append(c)

    lines = (
        (st_qkv, o_qkv, True),
        (outw, o_out, False),
        (st_in, o_in, True),
        (backw, o_back, False),
        (st_vec, o_vec, False),
    )
    staged = {0: 0, 2: 1, 4: 2}

    def place(i, which):
        dst = lines[i][1]
        return dst.at[:, which] if i in staged else dst.at[which]

    def item(i, which, kind, to, own=False):
        src, _, _ = lines[i]
        spot = place(i, which)
        return push(src if own else spot, spot, line_s.at[kind, i, which], line_r.at[i, which], {"wide": to})

    up, down, pair = 0, 1, 2

    def along(i, which, kind, own, act):
        if kind == pair:
            act(item(i, which, pair, 2 * a + other, own))
            return

        @pl.when((a < length - 1) if kind == up else (a > 0))
        def _():
            act(item(i, which, kind, w + 2 if kind == up else w - 2, own))

    def start(c):
        c.start()

    def done(c):
        c.wait_send()

    for i, (src, dst, _) in enumerate(lines):
        if i in staged:
            for j, c in sent:
                if j == staged[i]:
                    c.wait_recv()
            for j, c in local_cuts:
                if j == staged[i]:
                    c.wait()
        for kind in (up, down, pair):
            along(i, w, kind, True, start)
        c = pltpu.make_async_copy(src, place(i, w), loc.at[6 + i])
        c.start()
        late.append(c)
    tok_c[0].wait_recv()
    spot = o_tok.at[:, columns(across)]
    tok_fwd = push(spot, spot, tok_s.at[2], tok_r.at[2], {"section": beside})
    tok_fwd.start()

    mate = 2 * a + other

    def arrived(i, which):
        item(i, which, pair, mate).wait_recv()

    for i in range(len(lines)):
        if not lines[i][2]:
            arrived(i, mate)
            for kind in (up, down):
                along(i, mate, kind, False, start)

    def step(t, carry):
        for i in range(len(lines)):
            for kind, there, ok in ((up, a - t, a - t >= 0), (down, a + t, a + t < length)):

                @pl.when(ok)
                def _():
                    arrived(i, 2 * there + b)
                    along(i, 2 * there + b, kind, False, start)
                    if lines[i][2]:
                        along(i, 2 * there + b, pair, False, start)
                    else:
                        arrived(i, 2 * there + other)
                        along(i, 2 * there + other, kind, False, start)

        return carry

    lax.fori_loop(1, length, step, 0)
    for i in range(len(lines)):
        if lines[i][2]:
            lax.fori_loop(0, length, lambda there, carry: (arrived(i, 2 * there + other), carry)[1], 0)
        for kind in (up, down, pair):
            along(i, w, kind, True, done)
        if not lines[i][2]:
            for kind in (up, down):
                along(i, mate, kind, False, done)

    def finish(t, carry):
        for i in range(len(lines)):
            for kind, there, ok in ((up, a - t, a - t >= 0), (down, a + t, a + t < length)):

                @pl.when(ok)
                def _():
                    along(i, 2 * there + b, kind, False, done)
                    if lines[i][2]:
                        along(i, 2 * there + b, pair, False, done)
                    else:
                        along(i, 2 * there + other, kind, False, done)

        return carry

    lax.fori_loop(1, length, finish, 0)
    for _, c in sent:
        c.wait_send()
    tok_c[0].wait_send()
    tok_c[1].wait()
    tok_fwd.wait()
    for c in exp_c:
        c.wait()
    for c in late:
        c.wait()


def weights_call(qkv, inn, vec, outw, backw, first, second, tok, wide, collective_id):
    small = qkv.shape[0]
    hid = inn.shape[1] // 4
    cut = 3 * QUARTER
    outs = [
        ((4, wide, small, cut), BF16),
        ((4, wide, small, hid), BF16),
        ((4, wide, *vec.shape), F32),
        ((wide, *outw.shape), BF16),
        ((wide, *backw.shape), BF16),
        ((4, first.shape[0], hid), BF16),
        ((4, first.shape[0], hid), BF16),
        ((tok.shape[0], 4 * QUARTER), BF16),
    ]
    return call(
        weights_kernel,
        tuple(jax.ShapeDtypeStruct(*o) for o in outs),
        [ANY] * 8,
        tuple([ANY] * 8),
        [
            pltpu.VMEM((4, small, cut), BF16),
            pltpu.VMEM((4, small, hid), BF16),
            pltpu.VMEM((4, *vec.shape), F32),
            DMA((16,)),
            DMA((5, 3)),
            DMA((5, 3)),
            DMA((3,)),
            DMA((3,)),
            DMA((3, 5, wide)),
            DMA((5, wide)),
            DMA((2, 3)),
            DMA((2, 3)),
        ],
        collective_id,
        qkv,
        inn,
        vec,
        outw,
        backw,
        first,
        second,
        tok,
    )


GROUP = 32


def add_rows(dst, left, right):
    if len(dst.shape) == 3:
        for j in range(dst.shape[0]):
            add_rows(dst.at[j], left.at[j], right.at[j])
        return
    rows = dst.shape[0]
    step = min(rows, GROUP)

    def one(j, carry):
        at = pl.ds(pl.multiple_of(j * step, step), step)
        dst[at] = (left[at].astype(F32) + right[at].astype(F32)).astype(dst.dtype)
        return carry

    lax.fori_loop(0, rows // step, one, 0)


def attention_pair(pair, qkv, mask):
    q2, k2, v2 = (qkv(j * QUARTER + pair * 128) for j in range(3))
    got = []
    for h in range(2):
        q, k, v = (x[:, h * HEAD_SIZE : (h + 1) * HEAD_SIZE] for x in (q2, k2, v2))
        scores = jnp.where(mask > 0.0, dot_nt(q, k) * HEAD_SIZE ** (-0.5), -1e30)
        expo = jnp.exp(scores - jnp.max(scores, axis=-1, keepdims=True))
        got.append((q, k, v, expo / jnp.sum(expo, axis=-1, keepdims=True)))
    return got


def row_norm(v):
    centred = v - jnp.mean(v, axis=-1, keepdims=True)
    scale = lax.rsqrt(jnp.mean(centred * centred, axis=-1, keepdims=True) + 1e-05)
    return centred * scale, scale


def line_of_wide():
    w = lax.axis_index("wide")
    length = lax.axis_size("wide") // 2
    return w, length, lax.div(w, 2), lax.rem(w, 2)


def greet_line(section_peers, all_wide):
    w, length, a, b = line_of_wide()
    barrier = pltpu.get_barrier_semaphore()
    for p in section_peers:
        pl.semaphore_signal(barrier, inc=1, device_id={"section": p}, device_id_type=MESH)
    if all_wide:
        for j in range(1, 2 * length):
            pl.semaphore_signal(
                barrier, inc=1, device_id={"wide": lax.rem(w + j, 2 * length)}, device_id_type=MESH
            )
        pl.semaphore_wait(barrier, len(section_peers) + 2 * length - 1)
        return
    pl.semaphore_signal(barrier, inc=1, device_id={"wide": 2 * a + 1 - b}, device_id_type=MESH)

    @pl.when(a > 0)
    def _():
        pl.semaphore_signal(barrier, inc=1, device_id={"wide": w - 2}, device_id_type=MESH)

    @pl.when(a < length - 1)
    def _():
        pl.semaphore_signal(barrier, inc=1, device_id={"wide": w + 2}, device_id_type=MESH)

    pl.semaphore_wait(barrier, len(section_peers) + 1 + jnp.minimum(a, 1) + jnp.minimum(length - 1 - a, 1))


def tail_kernel(*refs):
    (g_in, g_back, first, second, d_att, tok, n1, qkv, mixed, w_qkv, w_out, mask, gain, gain_d) = refs[:14]
    o_qkv, o_in, o_out, o_back, o_gain, o_first, o_second, o_tok = refs[14:22]
    g_qkv, g_out = refs[22:24]
    acc = refs[24:28]
    line_in = refs[28:32]
    pair_in = refs[32:36]
    (d_mix, d_qkv, part, unit, scales, stats, stats_in, stats_mid, stats_far, near_in, far, far_in, gains, gains_in) = refs[36:50]
    (loc, exp_s, exp_r, cut_s, cut_r, pair_s, pair_r, line_s, line_r, s1, r1, s2, r2, st_s, st_r, gn_s, gn_r) = refs[50:]
    src = (g_qkv, g_in, g_out, g_back)
    pair_first = (True, True, False, False)
    me, beside, across = section_places()
    diagonal = beside + across - me
    core, side = lax.rem(me, 2), lax.div(me, 2)
    w, length, a, b = line_of_wide()
    other = 1 - b
    mate = {"wide": 2 * a + other}
    peers = [beside, across, diagonal]
    greet_line(peers, True)
    hid = first.shape[2]
    rows = mask.shape[1]
    micro = mask.shape[0]
    late = []

    def spot(ref, which, count):
        return ref.at[:, pl.ds(pl.multiple_of(which * count, count), count)]

    def pair_copy(i, there):
        return push(
            src[i].at[:, 2 * there + other], pair_in[i].at[there], pair_s.at[i, there], pair_r.at[i, there], mate
        )

    def slots(i, there):
        if pair_first[i]:
            return [(there, 2 * there + b)]
        return [(2 * there, 2 * there), (2 * there + 1, 2 * there + 1)]

    def line_copy(i, block, to_block, to):
        return push(acc[i].at[block], line_in[i].at[to_block], line_s.at[i, block], line_r.at[i, to_block], {"wide": to})

    def ready(i, there, block, own):
        if pair_first[i]:
            pair_copy(i, there).wait_recv()
            add_rows(acc[i].at[block], src[i].at[:, own], pair_in[i].at[there])
        else:
            acc[i][block] = src[i][own]

    def flow(i, there, from_edge, to):
        n = 1 if pair_first[i] else 2
        for j, (block, own) in enumerate(slots(i, there)):
            ready(i, there, block, own)

            @pl.when(from_edge)
            def _():
                line_copy(i, block, block, w).wait_recv()
                add_rows(acc[i].at[block], acc[i].at[block], line_in[i].at[block])

            if to == "down":
                line_copy(i, block, block, w - 2).start()
            else:
                target = jnp.where(there == a + 1, n * length + j, block)
                line_copy(i, block, target, w + 2).start()

    def pairs(i):
        lax.fori_loop(0, length, lambda t, c: (pair_copy(i, t).start(), c)[1], 0)

    def steps(group, start, stop):
        def step(t, carry):
            high = length - 1 - t
            for i in group:

                @pl.when(t < a)
                def _():
                    flow(i, t, a < length - 1, "down")

                @pl.when(high > a)
                def _():
                    flow(i, high, a > 0, "up")

            return carry

        lax.fori_loop(start, stop, step, 0)

    finals = {}

    def own_block(i):
        n = 1 if pair_first[i] else 2
        for j, (block, own) in enumerate(slots(i, a)):
            ready(i, a, block, own)

            @pl.when(a < length - 1)
            def _():
                line_copy(i, block, block, w).wait_recv()
                add_rows(acc[i].at[block], acc[i].at[block], line_in[i].at[block])

            @pl.when(a > 0)
            def _():
                line_copy(i, block, n * length + j, w).wait_recv()
                add_rows(acc[i].at[block], acc[i].at[block], line_in[i].at[n * length + j])

        if not pair_first[i]:
            c = push(acc[i].at[2 * a + other], pair_in[i].at[0], pair_s.at[i, 0], pair_r.at[i, 0], mate)
            c.start()
            finals[i] = c
            return
        block = acc[i].at[a]

        def cut(p):
            if i == 1:
                return [(block.at[p], spot(o_in, me, hid))]
            third = [pl.ds(j * QUARTER, QUARTER) for j in range(3)]
            return [(block.at[p, :, third[j]], spot(o_qkv, 4 * j + me, QUARTER)) for j in range(3)]

        for k, p in enumerate(peers):
            for j, (here, there) in enumerate(cut(p)):
                n = 3 * i + j
                c = push(here, there, cut_s.at[n, k], cut_r.at[n, k], {"section": p})
                c.start()
                late.append(c)
        for j, (here, there) in enumerate(cut(me)):
            c = pltpu.make_async_copy(here, there, loc.at[2 + 3 * i + j])
            c.start()
            late.append(c)

    pairs(1)
    for i, (s, d) in enumerate(((first, o_first), (second, o_second))):
        c = pltpu.make_async_copy(s.at[me], spot(d, me, hid), loc.at[i])
        c.start()
        late.append(c)
        for k, p in enumerate((across, diagonal, beside)):
            c = push(s.at[p], spot(d, me, hid), exp_s.at[i, k], exp_r.at[i, k], {"section": p})
            c.start()
            late.append(c)
    group = (3, 1)
    cuts = [k * length // 4 for k in range(5)]
    small = g_out.shape[1]
    wide = 2 * length

    def store_blocks(ref, index, value):
        for j in range(wide):
            piece = value[j * small : (j + 1) * small].astype(BF16)
            if index is None:
                ref[j] = piece
            else:
                ref[index, j] = piece

    for m in range(micro):
        at = pl.ds(m * rows, rows)
        d_mix[at] = dot_nt(d_att[at], w_out[...]).astype(BF16)
    store_blocks(g_out, None, dot_tn(mixed[...], d_att[...]))
    steps(group, cuts[0], cuts[1])

    def micro_back(m, carry):
        at = pl.ds(pl.multiple_of(m * rows, rows), rows)
        for pair in range(2):
            heads = attention_pair(pair, lambda c: qkv[at, pl.ds(c, 128)], mask[m])
            d_pair = d_mix[at, pl.ds(pair * 128, 128)]
            grads = []
            for h, (q, k, v, probs) in enumerate(heads):
                d_out = d_pair[:, h * HEAD_SIZE : (h + 1) * HEAD_SIZE]
                d_probs = dot_nt(d_out, v)
                delta = jnp.sum(probs * d_probs, axis=-1, keepdims=True)
                d_scores = (probs * (d_probs - delta) * HEAD_SIZE ** (-0.5)).astype(BF16)
                grads.append((dot(d_scores, k), dot_tn(d_scores, q), dot_tn(probs.astype(BF16), d_out)))
            for j in range(3):
                both = jnp.concatenate([grads[0][j], grads[1][j]], axis=1).astype(BF16)
                d_qkv[at, pl.ds(j * QUARTER + pair * 128, 128)] = both
        return carry

    for m in range(micro):
        micro_back(m, 0)
        steps(group, cuts[1 + m], cuts[2 + m])
    for p in range(4):
        store_blocks(g_qkv, p, dot_tn(n1[:, pl.ds(p * QUARTER, QUARTER)], d_qkv[...]))
    pairs(0)
    steps((2,), 0, length)

    count = d_att.shape[0]
    chunk = 128
    chunks = count // chunk
    lane = lax.broadcasted_iota(jnp.int32, (chunk, 128), 1)
    beside_core = 1 - core
    sends = []
    for k in range(chunks):
        at = pl.ds(k * chunk, chunk)
        u, scale = row_norm(tok[at].astype(F32))
        unit[at] = u
        scales[at] = jnp.broadcast_to(scale, (chunk, 128))
        d_normed = dot_nt(d_qkv[at], w_qkv[...])
        part[at] = d_normed.astype(BF16)
        d_unit = d_normed * gain[...]
        sum_a = jnp.sum(d_unit, axis=-1, keepdims=True)
        sum_b = jnp.sum(d_unit * u, axis=-1, keepdims=True)
        both = jnp.where(lane == 0, sum_a, jnp.where(lane == 1, sum_b, 0.0))
        stats[:, at] = both.T[:8]
        for which, half in ((1, 1 - side), (0, side)):
            c = push(
                part.at[at, columns(2 * half + beside_core)],
                near_in.at[which, at],
                s1.at[which, k],
                r1.at[which, k],
                {"section": beside},
            )
            c.start()
            sends.append(c)
    st1 = push(stats, stats_in, st_s.at[0], st_r.at[0], {"section": beside})
    st1.start()
    crossing = []
    for k in range(chunks):
        at = pl.ds(k * chunk, chunk)
        sends[2 * k].wait()
        far[at] = (part[at, columns(2 * (1 - side) + core)].astype(F32) + near_in[1, at].astype(F32)).astype(BF16)
        c = push(far.at[at], far_in.at[at], s2.at[k], r2.at[k], {"section": across})
        c.start()
        crossing.append(c)
    st1.wait()
    stats_mid[...] = stats[...] + stats_in[...]
    st2 = push(stats_mid, stats_far, st_s.at[1], st_r.at[1], {"section": across})
    st2.start()
    steps(group, cuts[3], cuts[4])
    steps((0,), 0, length)
    st2.wait()
    stats[...] = (stats_mid[...] + stats_far[...]) * (1.0 / gain.shape[1])
    total = jnp.zeros((1, QUARTER), F32)
    gain_q = gain[:, columns(me)]
    for k in range(chunks):
        at = pl.ds(k * chunk, chunk)
        sends[2 * k + 1].wait()
        near = part[at, columns(me)].astype(F32) + near_in[0, at].astype(F32)
        crossing[k].wait()
        d_q = near + far_in[at].astype(F32)
        u = unit[at, columns(me)]
        sums = jnp.concatenate([stats[:, at], jnp.zeros((chunk - 8, chunk), F32)], axis=0).T
        norm = scales[at, pl.ds(0, 1)] * (d_q * gain_q - sums[:, 0:1] - u * sums[:, 1:2])
        o_tok[at] = d_att[at, columns(me)].astype(F32) + norm
        total = total + jnp.sum(d_q * u, axis=0, keepdims=True)
    row = lax.broadcasted_iota(jnp.int32, (8, QUARTER), 0)
    gains[...] = jnp.where(row == 0, total, jnp.where(row == 1, gain_d[...], 0.0))

    def gain_copy(to, frm):
        return push(gains, gains_in.at[frm], gn_s.at[to], gn_r.at[frm], {"wide": to})

    for j in range(1, wide):
        gain_copy(lax.rem(w + j, wide), w).start()
    for i in (3, 1, 2, 0):
        own_block(i)
    gathered = gains[...]
    for j in range(1, wide):
        frm = lax.rem(w + j, wide)
        gain_copy(frm, frm).wait_recv()
        gathered = gathered + gains_in[frm]
    o_gain[...] = gathered
    for i, out in ((3, o_back), (2, o_out)):
        finals[i].wait_recv()
        add_rows(out, acc[i].at[2 * a + b], pair_in[i].at[0])
    for c in finals.values():
        c.wait_send()
    for c in late:
        c.wait()
    for j in range(1, wide):
        gain_copy(lax.rem(w + j, wide), w).wait_send()

    def finish(t, carry):
        for i in range(4):
            if pair_first[i]:
                pair_copy(i, t).wait_send()

            @pl.when(t != a)
            def _():
                for block, _ in slots(i, t):
                    line_copy(i, block, block, w).wait_send()

        return carry

    lax.fori_loop(0, length, finish, 0)


def tail_call(g_in, g_back, first, second, d_att, tok, n1, qkv, mixed, w_qkv, w_out, mask, gain, gain_d, collective_id):
    wide = g_back.shape[0]
    length = wide // 2
    small = g_in.shape[2]
    hid = first.shape[2]
    count, width = d_att.shape
    chunks = count // 128
    shapes = [(4, small, 3 * QUARTER), (4, small, hid), (small, width), g_back.shape[1:]]
    expert = ((first.shape[1], 4 * hid), BF16)
    outs = [
        ((small, 3 * width), BF16),
        ((small, 4 * hid), BF16),
        (shapes[2], F32),
        (shapes[3], F32),
        ((8, QUARTER), F32),
        expert,
        expert,
        ((count, QUARTER), F32),
    ]
    scratch = [pltpu.VMEM((4, wide, small, 3 * QUARTER), BF16), pltpu.VMEM((wide, small, width), BF16)]
    for counts in (
        [length, length, wide, wide],
        [length + 1, length + 1, wide + 2, wide + 2],
        [length, length, 1, 1],
    ):
        scratch += [pltpu.VMEM((n, *s), BF16) for n, s in zip(counts, shapes)]
    scratch += [
        pltpu.VMEM((count, QUARTER), BF16),
        pltpu.VMEM((count, 3 * QUARTER), BF16),
        pltpu.VMEM((count, width), BF16),
        pltpu.VMEM((count, width), F32),
        pltpu.VMEM((count, 128), F32),
        pltpu.VMEM((8, count), F32),
        pltpu.VMEM((8, count), F32),
        pltpu.VMEM((8, count), F32),
        pltpu.VMEM((8, count), F32),
        pltpu.VMEM((2, count, QUARTER), BF16),
        pltpu.VMEM((count, QUARTER), BF16),
        pltpu.VMEM((count, QUARTER), BF16),
        pltpu.VMEM((8, QUARTER), F32),
        pltpu.VMEM((wide, 8, QUARTER), F32),
        DMA((8,)),
        DMA((2, 3)),
        DMA((2, 3)),
        DMA((4, 3)),
        DMA((4, 3)),
        DMA((4, length)),
        DMA((4, length)),
        DMA((4, wide)),
        DMA((4, wide + 2)),
        DMA((2, chunks)),
        DMA((2, chunks)),
        DMA((chunks,)),
        DMA((chunks,)),
        DMA((2,)),
        DMA((2,)),
        DMA((wide,)),
        DMA((wide,)),
    ]
    return call(
        tail_kernel,
        tuple(jax.ShapeDtypeStruct(*o) for o in outs),
        [VM, VM, ANY, ANY] + [VM] * 10,
        (ANY, ANY, VM, VM, VM, ANY, ANY, VM),
        scratch,
        collective_id,
        *(g_in, g_back, first, second, d_att, tok, n1, qkv, mixed, w_qkv, w_out, mask, gain, gain_d),
    )


def dot(left, right):
    return jnp.dot(left, right, preferred_element_type=F32)


def dot_nt(left, right):
    return lax.dot_general(left, right, (((1,), (1,)), ((), ())), preferred_element_type=F32)


def dot_tn(left, right):
    return lax.dot_general(left, right, (((0,), (0,)), ((), ())), preferred_element_type=F32)


def gelu_value(v):
    return 0.5 * v * (1.0 + lax.erf(v * 0.7071067811865476))


def gelu_slope(v):
    return (
        0.5 * (1.0 + lax.erf(v * 0.7071067811865476))
        + v * jnp.exp(-0.5 * v * v) * 0.3989422804014327
    )


def unit_norm(v):
    centred = v - jnp.mean(v, axis=-1, keepdims=True)
    scale = lax.rsqrt(jnp.mean(centred * centred, axis=-1, keepdims=True) + 1e-05)
    return centred * scale, scale


IDS = {}


def id_of(*key):
    return IDS.setdefault(key, len(IDS))


def reduce_quarters(part, stats=None):
    return reduce_call(part.astype(BF16), stats, id_of("reduce", part.shape, stats is None))


def gather_quarters(quarter):
    return gather_call(quarter, id_of("gather", quarter.shape))


def wide_exchange(slots, spread):
    return exchange_call(slots, spread, id_of("exchange", spread))


def allowed_of(lengths, rows):
    pos = jnp.arange(rows, dtype=jnp.int32)
    group = pos[None] // lengths[:, None]
    return ((pos[:, None] >= pos[None, :])[None] & (group[:, :, None] == group[:, None, :])).astype(F32)


def attention_probs(queries, keys, lengths):
    rows = queries.shape[2]
    raw = jnp.einsum("mhqd,mhkd->mhqk", queries, keys, preferred_element_type=F32)
    pos = jnp.arange(rows, dtype=jnp.int32)
    same = pos[None, :, None] // lengths[:, None, None] == pos[None, None, :] // lengths[:, None, None]
    allowed = (pos[:, None] >= pos[None, :])[None] & same
    scores = jnp.where(allowed[:, None], raw * HEAD_SIZE ** (-0.5), -1e30)
    highest = jnp.max(scores, axis=-1, keepdims=True)
    expo = jnp.exp(scores - highest)
    return expo / jnp.sum(expo, axis=-1, keepdims=True)


def body(
    tokens_in,
    cotangent,
    routes,
    seq_lengths,
    qkv_weight,
    out_weight,
    attn_gain,
    ffn_in,
    ffn_back,
    ffn_gain,
    centroids,
    first_gain,
    first_in,
    first_back,
    second_gain,
    second_in,
    second_back,
):
    sections = lax.axis_size("section")
    wide = lax.axis_size("wide")
    section_id = lax.axis_index("section")
    wide_id = lax.axis_index("wide")
    micro, rows, quarter = tokens_in.shape
    width = quarter * sections
    cap = 5 * rows // (4 * wide)
    tok_rows = micro * rows
    hid = first_back.shape[1]
    small = qkv_weight.shape[0]
    qkv_cols = qkv_weight.shape[1] // sections

    vectors = jnp.concatenate([first_gain[0], second_gain[0], centroids[0], attn_gain, ffn_gain]).astype(F32)
    vectors = jnp.pad(vectors, (0, 1024 - vectors.shape[0])).reshape(8, 128)
    tokens_q = tokens_in.reshape(tok_rows, quarter)

    qkv_w, in_w, vectors, out_w, back_w, first_w, second_w, tokens = weights_call(
        qkv_weight,
        ffn_in,
        vectors,
        out_weight,
        ffn_back,
        first_in[0],
        second_in[0],
        tokens_q,
        wide,
        id_of("weights"),
    )
    qkv_w = qkv_w.reshape(width, qkv_cols)
    in_w = in_w.reshape(width, hid)
    out_w = out_w.reshape(quarter, width)
    back_w = back_w.reshape(hid, width)
    first_w = first_w.reshape(width, hid)
    second_w = second_w.reshape(width, hid)
    vectors = vectors.reshape(sections, wide, 1024)
    own = lax.dynamic_index_in_dim(vectors, wide_id, axis=1, keepdims=False)
    gain_first = own[:, :quarter].reshape(1, width)
    gain_second = own[:, quarter : 2 * quarter].reshape(1, width)
    centre = own[:, 2 * quarter : 3 * quarter].reshape(1, width)
    gain_attn = vectors[:, :, 3 * quarter : 3 * quarter + small].reshape(1, width)
    gain_ffn = vectors[:, :, 3 * quarter + small : 3 * quarter + 2 * small].reshape(1, width)
    own_quarter = lambda v: lax.dynamic_slice_in_dim(v, section_id * quarter, quarter, axis=1)
    first_b = first_back[0]
    second_b = second_back[0]

    experts = jnp.arange(wide, dtype=jnp.int32)
    choose = (routes == experts).astype(jnp.int32)
    upto = (jnp.arange(rows)[:, None] >= jnp.arange(rows)[None, :]).astype(BF16)
    ranking = jnp.einsum("rk,mke->mre", upto, choose.astype(BF16), preferred_element_type=F32).astype(jnp.int32) - 1
    slot_of = routes[:, :, 0] * cap + jnp.sum(ranking * choose, axis=2)
    onehot = (jnp.arange(wide * cap, dtype=jnp.int32)[None, :, None] == slot_of[:, None, :]).astype(BF16)

    def to_experts(rows_q):
        packed = jnp.einsum("msr,mrd->msd", onehot, rows_q.reshape(micro, rows, quarter), preferred_element_type=F32)
        packed = packed.astype(BF16).reshape(micro, wide, cap, quarter).transpose(1, 0, 2, 3)
        return wide_exchange(packed.reshape(wide, micro * cap, quarter), True).reshape(wide * micro * cap, width)

    def to_tokens(slots_q):
        back = wide_exchange(slots_q.reshape(wide, micro * cap, quarter), False)
        back = back.reshape(wide, micro, cap, quarter).transpose(1, 0, 2, 3).reshape(micro, wide * cap, quarter)
        got = jnp.einsum("msr,msd->mrd", onehot, back, preferred_element_type=F32)
        return got.astype(BF16).reshape(tok_rows, quarter)

    unit_a, scale_a = unit_norm(tokens.astype(F32))
    normed_a = (unit_a * gain_attn).astype(BF16)
    packed = dot(normed_a, qkv_w).astype(BF16)
    heads = quarter // HEAD_SIZE

    def by_head(v):
        return v.reshape(micro, rows, heads, HEAD_SIZE).transpose(0, 2, 1, 3)

    def from_head(v):
        return v.transpose(0, 2, 1, 3).reshape(tok_rows, quarter)

    queries, keys, values = (by_head(packed[:, i * quarter : (i + 1) * quarter]) for i in range(3))
    probs = attention_probs(queries, keys, seq_lengths)
    probs_b = probs.astype(BF16)
    mixed = from_head(
        jnp.einsum("mhqk,mhkd->mhqd", probs_b, values, preferred_element_type=F32).astype(BF16)
    )
    attended_q = (tokens_q.astype(F32) + reduce_quarters(dot(mixed, out_w))).astype(BF16)
    attended = gather_quarters(attended_q)

    def branch(v, w_in, w_back, gain):
        unit, scale = unit_norm(v.astype(F32))
        normed = (unit * gain).astype(BF16)
        pre = dot(normed, w_in)
        hidden = gelu_value(pre).astype(BF16)
        return (normed, unit, scale, pre, hidden), dot(hidden, w_back)

    def branch_back(grad, saved, w_in, w_back, gain, more=None):
        normed, unit, scale, pre, hidden = saved
        d_back = dot_tn(hidden, grad)
        d_pre = (dot_nt(grad, w_back) * gelu_slope(pre)).astype(BF16)
        d_in = dot_tn(normed, d_pre)
        return d_in, d_back, norm_back(dot_nt(d_pre, w_in), unit, scale, gain, more)

    def norm_back(d_part, unit, scale, gain, more=None):
        d_unit = d_part * gain
        sums = jnp.stack([jnp.sum(d_unit, axis=1), jnp.sum(d_unit * unit, axis=1)])
        if more is not None:
            sums = jnp.concatenate([sums, more])
        d_q, sums = reduce_quarters(d_part, jnp.pad(sums, ((0, 8 - sums.shape[0]), (0, 0))))
        extra, sums = sums[2], sums / width
        unit_q = own_quarter(unit)
        d_rows = scale * (d_q * own_quarter(gain) - sums[0][:, None] - unit_q * sums[1][:, None])
        return d_rows, jnp.sum(d_q * unit_q, axis=0), extra

    saved_d, part = branch(attended, in_w, back_w, gain_ffn)
    fed_q = (attended_q.astype(F32) + reduce_quarters(part)).astype(BF16)
    routed = to_experts(fed_q)
    routed_q = own_quarter(routed)
    d_mixed = to_experts(cotangent.reshape(tok_rows, quarter)).astype(F32)
    d_mixed_q = own_quarter(d_mixed)
    saved_1, part = branch(routed, first_w, first_b, gain_first)
    first_q = (routed_q.astype(F32) + reduce_quarters(part)).astype(BF16)
    first = gather_quarters(first_q)
    saved_2, part = branch(first, second_w, second_b, gain_second)
    gate = jax.nn.sigmoid(jnp.sum(routed.astype(F32) * centre, axis=-1, keepdims=True))
    second_q = first_q.astype(F32) + reduce_quarters(part)
    mixed_q = routed_q.astype(F32) + gate * second_q
    block_out = to_tokens(mixed_q.astype(BF16)).reshape(micro, rows, quarter)

    d_second = gate * d_mixed
    d_second_q = gate * d_mixed_q
    d_second_in, d_second_back, (norm_q, second_gain_grad, d_logit) = branch_back(
        d_second.astype(BF16), saved_2, second_w, second_b, gain_second, jnp.sum(d_mixed_q * second_q, axis=-1)[None]
    )
    d_logit = d_logit[:, None] * gate * (1.0 - gate)
    centroids_grad = jnp.sum(d_logit * routed_q.astype(F32), axis=0)[None]
    d_gated_q = (d_mixed_q + d_logit * own_quarter(centre)).astype(BF16)
    d_first_q = (d_second_q + norm_q).astype(BF16)
    d_first_in, d_first_back, (norm_q, first_gain_grad, _) = branch_back(
        gather_quarters(d_first_q), saved_1, first_w, first_b, gain_first
    )
    d_routed_q = (d_first_q.astype(F32) + norm_q + d_gated_q.astype(F32)).astype(BF16)
    d_fed_q = to_tokens(d_routed_q)
    d_in, d_back, (norm_q, d_gain_ffn, _) = branch_back(gather_quarters(d_fed_q), saved_d, in_w, back_w, gain_ffn)
    d_attended_q = (d_fed_q.astype(F32) + norm_q).astype(BF16)
    d_attended = gather_quarters(d_attended_q)
    def by_row(grad):
        return grad.astype(BF16).reshape(sections, wide, small, grad.shape[1])

    qkv_grad, ffn_in_grad, out_grad, ffn_back_grad, d_gains, d_first_in, d_second_in, tokens_grad = tail_call(
        by_row(d_in),
        d_back.astype(BF16).reshape(wide, hid // wide, width),
        d_first_in.astype(BF16).reshape(sections, quarter, hid),
        d_second_in.astype(BF16).reshape(sections, quarter, hid),
        d_attended,
        tokens,
        normed_a,
        packed,
        mixed,
        qkv_w,
        out_w,
        allowed_of(seq_lengths, rows),
        gain_attn,
        d_gain_ffn[None],
        id_of("tail"),
    )
    d_gains = lax.dynamic_slice_in_dim(d_gains, wide_id * small, small, axis=1)
    tokens_grad = tokens_grad.reshape(micro, rows, quarter)
    return (
        block_out,
        tokens_grad,
        qkv_grad.astype(F32),
        out_grad,
        d_gains[0],
        ffn_in_grad.astype(F32),
        ffn_back_grad,
        d_gains[1],
        centroids_grad,
        first_gain_grad[None],
        d_first_in[None].astype(F32),
        d_first_back[None],
        second_gain_grad[None],
        d_second_in[None].astype(F32),
        d_second_back[None],
    )


def solution(mesh):
    dense = P(("section", "wide"), None)
    dense_gain = P(("section", "wide"))
    tokens = P(None, "wide", "section")
    gain = P("wide", "section")
    expert = P("wide", "section", None)
    in_specs = (
        (tokens, tokens, P(None, "wide", None), P(), dense, dense, dense_gain, dense, dense, dense_gain)
        + (gain, gain, expert, expert, gain, expert, expert)
    )
    out_specs = (
        (tokens, tokens, dense, dense, dense_gain, dense, dense, dense_gain)
        + (gain, gain, expert, expert, gain, expert, expert)
    )
    return jax.shard_map(body, mesh=mesh, in_specs=in_specs, out_specs=out_specs, check_vma=False)
```

```python
import functools

import jax
import jax.numpy as jnp
from jax import lax
from jax.experimental import pallas as pl
from jax.experimental.pallas import tpu as pltpu
from jax.sharding import PartitionSpec as P

HEAD_SIZE = 64
F32 = jnp.float32
BF16 = jnp.bfloat16

MESH = pl.DeviceIdType.MESH
ANY = pl.BlockSpec(memory_space=pl.ANY)
VM = pl.BlockSpec(memory_space=pltpu.VMEM)
DMA = pltpu.SemaphoreType.DMA
VMEM_BYTES = 60 * 1024 * 1024
QUARTER = 256


def section_places():
    me = lax.axis_index("section")
    return me, me + 1 - 2 * lax.rem(me, 2), me + 2 - 4 * lax.div(me, 2)


def greet(peers):
    barrier = pltpu.get_barrier_semaphore()
    for peer in peers:
        pl.semaphore_signal(barrier, inc=1, device_id=peer, device_id_type=MESH)
    pl.semaphore_wait(barrier, len(peers))


def push(src, dst, send, recv, peer):
    return pltpu.make_async_remote_copy(
        src_ref=src, dst_ref=dst, send_sem=send, recv_sem=recv, device_id=peer, device_id_type=MESH
    )


def columns(which):
    return pl.ds(pl.multiple_of(which * QUARTER, QUARTER), QUARTER)


def call(kernel, out_shape, in_specs, out_specs, scratch, collective_id, *operands):
    return pl.pallas_call(
        kernel,
        out_shape=out_shape,
        in_specs=in_specs,
        out_specs=out_specs,
        scratch_shapes=scratch,
        compiler_params=pltpu.CompilerParams(
            collective_id=collective_id, has_side_effects=True, vmem_limit_bytes=VMEM_BYTES
        ),
    )(*operands)


def reduce_kernel(chunks, with_stats, *refs):
    if with_stats:
        part, stats, out, stats_out = refs[:4]
        first_in, far, far_in, s1, r1, s2, r2, st_in, st_mid, st_far, st_s, st_r = refs[4:]
    else:
        part, out, first_in, far, far_in, s1, r1, s2, r2 = refs
    me, beside, across = section_places()
    core, side = lax.rem(me, 2), lax.div(me, 2)
    greet([{"section": beside}, {"section": across}])
    rows = part.shape[0] // chunks
    beside_core = 1 - core
    sends = []
    if with_stats:
        st = push(stats, st_in, st_s.at[0], st_r.at[0], {"section": beside})
        st.start()
    for k in range(chunks):
        for which, half in ((1, 1 - side), (0, side)):
            at = pl.ds(k * rows, rows)
            c = push(
                part.at[at, columns(2 * half + beside_core)],
                first_in.at[which, at],
                s1.at[which, k],
                r1.at[which, k],
                {"section": beside},
            )
            c.start()
            sends.append(c)
    if with_stats:
        st.wait()
        st_mid[...] = stats[...] + st_in[...]
        st2 = push(st_mid, st_far, st_s.at[1], st_r.at[1], {"section": across})
        st2.start()
    crossing = []
    for k in range(chunks):
        at = pl.ds(k * rows, rows)
        sends[2 * k].wait()
        far[at] = (part[at, columns(2 * (1 - side) + core)].astype(F32) + first_in[1, at].astype(F32)).astype(BF16)
        c = push(far.at[at], far_in.at[at], s2.at[k], r2.at[k], {"section": across})
        c.start()
        crossing.append(c)
    for k in range(chunks):
        at = pl.ds(k * rows, rows)
        sends[2 * k + 1].wait()
        near = part[at, columns(me)].astype(F32) + first_in[0, at].astype(F32)
        crossing[k].wait()
        out[at] = near + far_in[at].astype(F32)
    if with_stats:
        st2.wait()
        stats_out[...] = st_mid[...] + st_far[...]


def reduce_call(part, stats, collective_id, chunks=4):
    rows, _ = part.shape
    scratch = [
        pltpu.VMEM((2, rows, QUARTER), BF16),
        pltpu.VMEM((rows, QUARTER), BF16),
        pltpu.VMEM((rows, QUARTER), BF16),
        DMA((2, chunks)),
        DMA((2, chunks)),
        DMA((chunks,)),
        DMA((chunks,)),
    ]
    out = jax.ShapeDtypeStruct((rows, QUARTER), F32)
    if stats is None:
        return call(
            functools.partial(reduce_kernel, chunks, False), out, [VM], VM, scratch, collective_id, part
        )
    st = pltpu.VMEM(stats.shape, F32)
    return call(
        functools.partial(reduce_kernel, chunks, True),
        (out, jax.ShapeDtypeStruct(stats.shape, F32)),
        [VM, VM],
        (VM, VM),
        scratch + [st, st, st, DMA((2,)), DMA((2,))],
        collective_id,
        part,
        stats,
    )


def gather_kernel(chunks, q, out, s, r):
    me, beside, across = section_places()
    greet([{"section": beside}, {"section": across}])
    rows = q.shape[0] // chunks
    copies = []
    for k in range(chunks):
        at = pl.ds(k * rows, rows)
        for kind, to in ((0, across), (1, beside)):
            c = push(q.at[at], out.at[at, columns(me)], s.at[kind, k], r.at[kind, k], {"section": to})
            c.start()
            copies.append(c)
    out[:, columns(me)] = q[...]
    for k in range(chunks):
        at = pl.ds(k * rows, rows)
        copies[2 * k].wait()
        here = out.at[at, columns(across)]
        c = push(here, here, s.at[2, k], r.at[2, k], {"section": beside})
        c.start()
        copies.append(c)
    for k in range(chunks):
        copies[2 * k + 1].wait()
        copies[2 * chunks + k].wait()


def gather_call(q, collective_id, chunks=4):
    rows = q.shape[0]
    return call(
        functools.partial(gather_kernel, chunks),
        jax.ShapeDtypeStruct((rows, 4 * QUARTER), BF16),
        [VM],
        VM,
        [DMA((3, chunks)), DMA((3, chunks))],
        collective_id,
        q,
    )


def exchange_kernel(spread, src, out, s, r):
    me, beside, across = section_places()
    w = lax.axis_index("wide")
    count = src.shape[0]
    peers = [{"wide": lax.rem(w + j, count)} for j in range(1, count)]
    greet(peers + ([{"section": beside}, {"section": across}] if spread else []))

    def place(which, block):
        return out.at[block, :, columns(which)] if spread else out.at[block]

    def wide_copy(to):
        return push(src.at[to], place(me, w), s.at[0, to], r.at[0, w], {"wide": to})

    def arrival(frm):
        return push(src.at[frm], place(me, frm), s.at[0, frm], r.at[0, frm], {"wide": frm})

    def spread_copy(kind, block, to):
        here = place(across, block) if kind == 3 else place(me, block)
        return push(here, here, s.at[kind, block], r.at[kind, block], {"section": to})

    for j in range(1, count):
        wide_copy(lax.rem(w + j, count)).start()
    if spread:
        out[w, :, columns(me)] = src[w]
    else:
        out[w] = src[w]
    for j in range(count):
        block = lax.rem(w + j, count)
        if j:
            arrival(block).wait_recv()
        if spread:
            spread_copy(1, block, across).start()
            spread_copy(2, block, beside).start()
    if spread:
        for j in range(count):
            block = lax.rem(w + j, count)
            spread_copy(1, block, across).wait_recv()
            spread_copy(3, block, beside).start()
        for j in range(count):
            block = lax.rem(w + j, count)
            spread_copy(1, block, across).wait_send()
            spread_copy(2, block, beside).wait()
            spread_copy(3, block, beside).wait()
    for j in range(1, count):
        wide_copy(lax.rem(w + j, count)).wait_send()


def exchange_call(slots, spread, collective_id):
    count, n, quarter = slots.shape
    return call(
        functools.partial(exchange_kernel, spread),
        jax.ShapeDtypeStruct((count, n, 4 * quarter if spread else quarter), BF16),
        [VM],
        VM,
        [DMA((4, count)), DMA((4, count))],
        collective_id,
        slots,
    )


GROUP = 32


def add_rows(dst, left, right):
    if len(dst.shape) == 3:
        for j in range(dst.shape[0]):
            add_rows(dst.at[j], left.at[j], right.at[j])
        return
    rows = dst.shape[0]
    step = min(rows, GROUP)

    def one(j, carry):
        at = pl.ds(pl.multiple_of(j * step, step), step)
        dst[at] = (left[at].astype(F32) + right[at].astype(F32)).astype(dst.dtype)
        return carry

    lax.fori_loop(0, rows // step, one, 0)


def attention_pair(pair, qkv, mask):
    q2, k2, v2 = (qkv(j * QUARTER + pair * 128) for j in range(3))
    got = []
    for h in range(2):
        q, k, v = (x[:, h * HEAD_SIZE : (h + 1) * HEAD_SIZE] for x in (q2, k2, v2))
        scores = jnp.where(mask > 0.0, dot_nt(q, k) * HEAD_SIZE ** (-0.5), -1e30)
        expo = jnp.exp(scores - jnp.max(scores, axis=-1, keepdims=True))
        got.append((q, k, v, expo / jnp.sum(expo, axis=-1, keepdims=True)))
    return got


def row_norm(v):
    centred = v - jnp.mean(v, axis=-1, keepdims=True)
    scale = lax.rsqrt(jnp.mean(centred * centred, axis=-1, keepdims=True) + 1e-05)
    return centred * scale, scale


def line_of_wide():
    w = lax.axis_index("wide")
    length = lax.axis_size("wide") // 2
    return w, length, lax.div(w, 2), lax.rem(w, 2)


def greet_line(section_peers, all_wide):
    w, length, a, b = line_of_wide()
    barrier = pltpu.get_barrier_semaphore()
    for p in section_peers:
        pl.semaphore_signal(barrier, inc=1, device_id={"section": p}, device_id_type=MESH)
    if all_wide:
        for j in range(1, 2 * length):
            pl.semaphore_signal(
                barrier, inc=1, device_id={"wide": lax.rem(w + j, 2 * length)}, device_id_type=MESH
            )
        pl.semaphore_wait(barrier, len(section_peers) + 2 * length - 1)
        return
    pl.semaphore_signal(barrier, inc=1, device_id={"wide": 2 * a + 1 - b}, device_id_type=MESH)

    @pl.when(a > 0)
    def _():
        pl.semaphore_signal(barrier, inc=1, device_id={"wide": w - 2}, device_id_type=MESH)

    @pl.when(a < length - 1)
    def _():
        pl.semaphore_signal(barrier, inc=1, device_id={"wide": w + 2}, device_id_type=MESH)

    pl.semaphore_wait(barrier, len(section_peers) + 1 + jnp.minimum(a, 1) + jnp.minimum(length - 1 - a, 1))


def tail_kernel(*refs):
    (g_in, g_back, first, second, d_att, tok, n1, qkv, mixed, w_qkv, w_out, mask, gain, gain_d) = refs[:14]
    o_qkv, o_in, o_out, o_back, o_gain, o_first, o_second, o_tok = refs[14:22]
    g_qkv, g_out = refs[22:24]
    acc = refs[24:28]
    line_in = refs[28:32]
    pair_in = refs[32:36]
    (d_mix, d_qkv, part, unit, scales, stats, stats_in, stats_mid, stats_far, near_in, far, far_in, gains, gains_in) = refs[36:50]
    (loc, exp_s, exp_r, cut_s, cut_r, pair_s, pair_r, line_s, line_r, s1, r1, s2, r2, st_s, st_r, gn_s, gn_r) = refs[50:]
    src = (g_qkv, g_in, g_out, g_back)
    pair_first = (True, True, False, False)
    me, beside, across = section_places()
    diagonal = beside + across - me
    core, side = lax.rem(me, 2), lax.div(me, 2)
    w, length, a, b = line_of_wide()
    other = 1 - b
    mate = {"wide": 2 * a + other}
    peers = [beside, across, diagonal]
    greet_line(peers, True)
    hid = first.shape[2]
    rows = mask.shape[1]
    micro = mask.shape[0]
    late = []

    def spot(ref, which, count):
        return ref.at[:, pl.ds(pl.multiple_of(which * count, count), count)]

    def pair_copy(i, there):
        return push(
            src[i].at[:, 2 * there + other], pair_in[i].at[there], pair_s.at[i, there], pair_r.at[i, there], mate
        )

    def slots(i, there):
        if pair_first[i]:
            return [(there, 2 * there + b)]
        return [(2 * there, 2 * there), (2 * there + 1, 2 * there + 1)]

    def line_copy(i, block, to_block, to):
        return push(acc[i].at[block], line_in[i].at[to_block], line_s.at[i, block], line_r.at[i, to_block], {"wide": to})

    def ready(i, there, block, own):
        if pair_first[i]:
            pair_copy(i, there).wait_recv()
            add_rows(acc[i].at[block], src[i].at[:, own], pair_in[i].at[there])
        else:
            acc[i][block] = src[i][own]

    def flow(i, there, from_edge, to):
        n = 1 if pair_first[i] else 2
        for j, (block, own) in enumerate(slots(i, there)):
            ready(i, there, block, own)

            @pl.when(from_edge)
            def _():
                line_copy(i, block, block, w).wait_recv()
                add_rows(acc[i].at[block], acc[i].at[block], line_in[i].at[block])

            if to == "down":
                line_copy(i, block, block, w - 2).start()
            else:
                target = jnp.where(there == a + 1, n * length + j, block)
                line_copy(i, block, target, w + 2).start()

    def pairs(i):
        lax.fori_loop(0, length, lambda t, c: (pair_copy(i, t).start(), c)[1], 0)

    def steps(group, start, stop):
        def step(t, carry):
            high = length - 1 - t
            for i in group:

                @pl.when(t < a)
                def _():
                    flow(i, t, a < length - 1, "down")

                @pl.when(high > a)
                def _():
                    flow(i, high, a > 0, "up")

            return carry

        lax.fori_loop(start, stop, step, 0)

    finals = {}

    def own_block(i):
        n = 1 if pair_first[i] else 2
        for j, (block, own) in enumerate(slots(i, a)):
            ready(i, a, block, own)

            @pl.when(a < length - 1)
            def _():
                line_copy(i, block, block, w).wait_recv()
                add_rows(acc[i].at[block], acc[i].at[block], line_in[i].at[block])

            @pl.when(a > 0)
            def _():
                line_copy(i, block, n * length + j, w).wait_recv()
                add_rows(acc[i].at[block], acc[i].at[block], line_in[i].at[n * length + j])

        if not pair_first[i]:
            c = push(acc[i].at[2 * a + other], pair_in[i].at[0], pair_s.at[i, 0], pair_r.at[i, 0], mate)
            c.start()
            finals[i] = c
            return
        block = acc[i].at[a]

        def cut(p):
            if i == 1:
                return [(block.at[p], spot(o_in, me, hid))]
            third = [pl.ds(j * QUARTER, QUARTER) for j in range(3)]
            return [(block.at[p, :, third[j]], spot(o_qkv, 4 * j + me, QUARTER)) for j in range(3)]

        for k, p in enumerate(peers):
            for j, (here, there) in enumerate(cut(p)):
                n = 3 * i + j
                c = push(here, there, cut_s.at[n, k], cut_r.at[n, k], {"section": p})
                c.start()
                late.append(c)
        for j, (here, there) in enumerate(cut(me)):
            c = pltpu.make_async_copy(here, there, loc.at[2 + 3 * i + j])
            c.start()
            late.append(c)

    pairs(1)
    for i, (s, d) in enumerate(((first, o_first), (second, o_second))):
        c = pltpu.make_async_copy(s.at[me], spot(d, me, hid), loc.at[i])
        c.start()
        late.append(c)
        for k, p in enumerate((across, diagonal, beside)):
            c = push(s.at[p], spot(d, me, hid), exp_s.at[i, k], exp_r.at[i, k], {"section": p})
            c.start()
            late.append(c)
    group = (3, 1)
    cuts = [k * length // 4 for k in range(5)]
    small = g_out.shape[1]
    wide = 2 * length

    def store_blocks(ref, index, value):
        for j in range(wide):
            piece = value[j * small : (j + 1) * small].astype(BF16)
            if index is None:
                ref[j] = piece
            else:
                ref[index, j] = piece

    for m in range(micro):
        at = pl.ds(m * rows, rows)
        d_mix[at] = dot_nt(d_att[at], w_out[...]).astype(BF16)
    store_blocks(g_out, None, dot_tn(mixed[...], d_att[...]))
    steps(group, cuts[0], cuts[1])

    def micro_back(m, carry):
        at = pl.ds(pl.multiple_of(m * rows, rows), rows)
        for pair in range(2):
            heads = attention_pair(pair, lambda c: qkv[at, pl.ds(c, 128)], mask[m])
            d_pair = d_mix[at, pl.ds(pair * 128, 128)]
            grads = []
            for h, (q, k, v, probs) in enumerate(heads):
                d_out = d_pair[:, h * HEAD_SIZE : (h + 1) * HEAD_SIZE]
                d_probs = dot_nt(d_out, v)
                delta = jnp.sum(probs * d_probs, axis=-1, keepdims=True)
                d_scores = (probs * (d_probs - delta) * HEAD_SIZE ** (-0.5)).astype(BF16)
                grads.append((dot(d_scores, k), dot_tn(d_scores, q), dot_tn(probs.astype(BF16), d_out)))
            for j in range(3):
                both = jnp.concatenate([grads[0][j], grads[1][j]], axis=1).astype(BF16)
                d_qkv[at, pl.ds(j * QUARTER + pair * 128, 128)] = both
        return carry

    for m in range(micro):
        micro_back(m, 0)
        steps(group, cuts[1 + m], cuts[2 + m])
    for p in range(4):
        store_blocks(g_qkv, p, dot_tn(n1[:, pl.ds(p * QUARTER, QUARTER)], d_qkv[...]))
    pairs(0)
    steps((2,), 0, length)

    count = d_att.shape[0]
    chunk = 128
    chunks = count // chunk
    lane = lax.broadcasted_iota(jnp.int32, (chunk, 128), 1)
    beside_core = 1 - core
    sends = []
    for k in range(chunks):
        at = pl.ds(k * chunk, chunk)
        u, scale = row_norm(tok[at].astype(F32))
        unit[at] = u
        scales[at] = jnp.broadcast_to(scale, (chunk, 128))
        d_normed = dot_nt(d_qkv[at], w_qkv[...])
        part[at] = d_normed.astype(BF16)
        d_unit = d_normed * gain[...]
        sum_a = jnp.sum(d_unit, axis=-1, keepdims=True)
        sum_b = jnp.sum(d_unit * u, axis=-1, keepdims=True)
        both = jnp.where(lane == 0, sum_a, jnp.where(lane == 1, sum_b, 0.0))
        stats[:, at] = both.T[:8]
        for which, half in ((1, 1 - side), (0, side)):
            c = push(
                part.at[at, columns(2 * half + beside_core)],
                near_in.at[which, at],
                s1.at[which, k],
                r1.at[which, k],
                {"section": beside},
            )
            c.start()
            sends.append(c)
    st1 = push(stats, stats_in, st_s.at[0], st_r.at[0], {"section": beside})
    st1.start()
    crossing = []
    for k in range(chunks):
        at = pl.ds(k * chunk, chunk)
        sends[2 * k].wait()
        far[at] = (part[at, columns(2 * (1 - side) + core)].astype(F32) + near_in[1, at].astype(F32)).astype(BF16)
        c = push(far.at[at], far_in.at[at], s2.at[k], r2.at[k], {"section": across})
        c.start()
        crossing.append(c)
    st1.wait()
    stats_mid[...] = stats[...] + stats_in[...]
    st2 = push(stats_mid, stats_far, st_s.at[1], st_r.at[1], {"section": across})
    st2.start()
    steps(group, cuts[3], cuts[4])
    steps((0,), 0, length)
    st2.wait()
    stats[...] = (stats_mid[...] + stats_far[...]) * (1.0 / gain.shape[1])
    total = jnp.zeros((1, QUARTER), F32)
    gain_q = gain[:, columns(me)]
    for k in range(chunks):
        at = pl.ds(k * chunk, chunk)
        sends[2 * k + 1].wait()
        near = part[at, columns(me)].astype(F32) + near_in[0, at].astype(F32)
        crossing[k].wait()
        d_q = near + far_in[at].astype(F32)
        u = unit[at, columns(me)]
        sums = jnp.concatenate([stats[:, at], jnp.zeros((chunk - 8, chunk), F32)], axis=0).T
        norm = scales[at, pl.ds(0, 1)] * (d_q * gain_q - sums[:, 0:1] - u * sums[:, 1:2])
        o_tok[at] = d_att[at, columns(me)].astype(F32) + norm
        total = total + jnp.sum(d_q * u, axis=0, keepdims=True)
    row = lax.broadcasted_iota(jnp.int32, (8, QUARTER), 0)
    gains[...] = jnp.where(row == 0, total, jnp.where(row == 1, gain_d[...], 0.0))

    def gain_copy(to, frm):
        return push(gains, gains_in.at[frm], gn_s.at[to], gn_r.at[frm], {"wide": to})

    for j in range(1, wide):
        gain_copy(lax.rem(w + j, wide), w).start()
    for i in (3, 1, 2, 0):
        own_block(i)
    gathered = gains[...]
    for j in range(1, wide):
        frm = lax.rem(w + j, wide)
        gain_copy(frm, frm).wait_recv()
        gathered = gathered + gains_in[frm]
    o_gain[...] = gathered
    for i, out in ((3, o_back), (2, o_out)):
        finals[i].wait_recv()
        add_rows(out, acc[i].at[2 * a + b], pair_in[i].at[0])
    for c in finals.values():
        c.wait_send()
    for c in late:
        c.wait()
    for j in range(1, wide):
        gain_copy(lax.rem(w + j, wide), w).wait_send()

    def finish(t, carry):
        for i in range(4):
            if pair_first[i]:
                pair_copy(i, t).wait_send()

            @pl.when(t != a)
            def _():
                for block, _ in slots(i, t):
                    line_copy(i, block, block, w).wait_send()

        return carry

    lax.fori_loop(0, length, finish, 0)


def tail_call(g_in, g_back, first, second, d_att, tok, n1, qkv, mixed, w_qkv, w_out, mask, gain, gain_d, collective_id):
    wide = g_back.shape[0]
    length = wide // 2
    small = g_in.shape[2]
    hid = first.shape[2]
    count, width = d_att.shape
    chunks = count // 128
    shapes = [(4, small, 3 * QUARTER), (4, small, hid), (small, width), g_back.shape[1:]]
    expert = ((first.shape[1], 4 * hid), BF16)
    outs = [
        ((small, 3 * width), BF16),
        ((small, 4 * hid), BF16),
        (shapes[2], F32),
        (shapes[3], F32),
        ((8, QUARTER), F32),
        expert,
        expert,
        ((count, QUARTER), F32),
    ]
    scratch = [pltpu.VMEM((4, wide, small, 3 * QUARTER), BF16), pltpu.VMEM((wide, small, width), BF16)]
    for counts in (
        [length, length, wide, wide],
        [length + 1, length + 1, wide + 2, wide + 2],
        [length, length, 1, 1],
    ):
        scratch += [pltpu.VMEM((n, *s), BF16) for n, s in zip(counts, shapes)]
    scratch += [
        pltpu.VMEM((count, QUARTER), BF16),
        pltpu.VMEM((count, 3 * QUARTER), BF16),
        pltpu.VMEM((count, width), BF16),
        pltpu.VMEM((count, width), F32),
        pltpu.VMEM((count, 128), F32),
        pltpu.VMEM((8, count), F32),
        pltpu.VMEM((8, count), F32),
        pltpu.VMEM((8, count), F32),
        pltpu.VMEM((8, count), F32),
        pltpu.VMEM((2, count, QUARTER), BF16),
        pltpu.VMEM((count, QUARTER), BF16),
        pltpu.VMEM((count, QUARTER), BF16),
        pltpu.VMEM((8, QUARTER), F32),
        pltpu.VMEM((wide, 8, QUARTER), F32),
        DMA((8,)),
        DMA((2, 3)),
        DMA((2, 3)),
        DMA((4, 3)),
        DMA((4, 3)),
        DMA((4, length)),
        DMA((4, length)),
        DMA((4, wide)),
        DMA((4, wide + 2)),
        DMA((2, chunks)),
        DMA((2, chunks)),
        DMA((chunks,)),
        DMA((chunks,)),
        DMA((2,)),
        DMA((2,)),
        DMA((wide,)),
        DMA((wide,)),
    ]
    return call(
        tail_kernel,
        tuple(jax.ShapeDtypeStruct(*o) for o in outs),
        [VM, VM, ANY, ANY] + [VM] * 10,
        (ANY, ANY, VM, VM, VM, ANY, ANY, VM),
        scratch,
        collective_id,
        *(g_in, g_back, first, second, d_att, tok, n1, qkv, mixed, w_qkv, w_out, mask, gain, gain_d),
    )


def head_kernel(*refs):
    qkv, inn, vec, outw, backw, first, second, tok, mask = refs[:9]
    o_qkv, o_in, o_vec, o_out, o_back, o_first, o_second, o_tok, o_n1, o_act, o_mixed, o_att = refs[9:21]
    st_qkv, st_in, st_vec, gain, part, near_in, far, far_in = refs[21:29]
    loc, cut_s, cut_r, tok_s, tok_r, line_s, line_r, exp_s, exp_r, s1, r1, s2, r2, g_s, g_r = refs[29:]
    me, beside, across = section_places()
    core, side = lax.rem(me, 2), lax.div(me, 2)
    w, length, a, b = line_of_wide()
    other = 1 - b
    mate = 2 * a + other
    diagonal = beside + across - me
    peers = [beside, across, diagonal]
    greet_line(peers, False)
    hid = o_first.shape[2]
    width = 4 * QUARTER
    sent, local_cuts = [], []

    def part_of(src, start, count):
        return src.at[:, pl.ds(pl.multiple_of(start, 128), count)]

    def cuts_for(p):
        got = [
            (0, part_of(qkv, j * width + p * QUARTER, QUARTER), st_qkv.at[me, :, pl.ds(j * QUARTER, QUARTER)])
            for j in range(3)
        ]
        return got + [(1, part_of(inn, p * hid, hid), st_in.at[me]), (2, vec, st_vec.at[me])]

    for k, p in enumerate(peers):
        for n, (i, src, dst) in enumerate(cuts_for(p)):
            c = push(src, dst, cut_s.at[n, k], cut_r.at[n, k], {"section": p})
            c.start()
            sent.append((i, c))
    for n, (i, src, dst) in enumerate(cuts_for(me)):
        c = pltpu.make_async_copy(src, dst, loc.at[11 + n])
        c.start()
        local_cuts.append((i, c))
    tok_c = [
        push(tok, o_tok.at[:, columns(me)], tok_s.at[k], tok_r.at[k], {"section": p})
        for k, p in enumerate((across, beside))
    ]
    for c in tok_c:
        c.start()
    own_tok = pltpu.make_async_copy(tok, o_tok.at[:, columns(me)], loc.at[3])
    own_tok.start()
    late = []
    exp_c = []
    for i, (src, dst) in enumerate(((first, o_first), (second, o_second))):
        c = pltpu.make_async_copy(part_of(src, me * hid, hid), dst.at[me], loc.at[4 + i])
        c.start()
        late.append(c)
        for k, p in enumerate((across, diagonal, beside)):
            c = push(part_of(src, p * hid, hid), dst.at[me], exp_s.at[i, k], exp_r.at[i, k], {"section": p})
            c.start()
            exp_c.append(c)

    lines = (
        (st_qkv, o_qkv, True),
        (outw, o_out, False),
        (st_in, o_in, True),
        (backw, o_back, False),
        (st_vec, o_vec, False),
    )
    staged = {0: 0, 2: 1, 4: 2}
    up, down, pair = 0, 1, 2

    def place(i, which):
        dst = lines[i][1]
        return dst.at[:, which] if i in staged else dst.at[which]

    def item(i, which, kind, to, own=False):
        spot = place(i, which)
        return push(lines[i][0] if own else spot, spot, line_s.at[kind, i, which], line_r.at[i, which], {"wide": to})

    def along(i, which, kind, own, act):
        if kind == pair:
            act(item(i, which, pair, mate, own))
            return

        @pl.when((a < length - 1) if kind == up else (a > 0))
        def _():
            act(item(i, which, kind, w + 2 if kind == up else w - 2, own))

    def start(c):
        c.start()

    def done(c):
        c.wait_send()

    def arrived(i, which):
        item(i, which, pair, mate).wait_recv()

    def own_item(i):
        if i in staged:
            for j, c in sent:
                if j == staged[i]:
                    c.wait_recv()
            for j, c in local_cuts:
                if j == staged[i]:
                    c.wait()
        for kind in (up, down, pair):
            along(i, w, kind, True, start)
        c = pltpu.make_async_copy(lines[i][0], place(i, w), loc.at[6 + i])
        c.start()
        return c

    def mate_item(i):
        if not lines[i][2]:
            arrived(i, mate)
            for kind in (up, down):
                along(i, mate, kind, False, start)

    def both_ways(t, what):
        for kind, there, ok in ((up, a - t, a - t >= 0), (down, a + t, a + t < length)):

            @pl.when(ok)
            def _():
                what(kind, there)

    def steps(group, begin, end):
        def step(t, carry):
            for i in group:

                def pass_on(kind, there):
                    arrived(i, 2 * there + b)
                    along(i, 2 * there + b, kind, False, start)
                    if lines[i][2]:
                        along(i, 2 * there + b, pair, False, start)
                    else:
                        arrived(i, 2 * there + other)
                        along(i, 2 * there + other, kind, False, start)

                both_ways(t, pass_on)
            return carry

        lax.fori_loop(begin, end, step, 0)

    def pair_items(i):
        if lines[i][2]:
            lax.fori_loop(0, length, lambda there, carry: (arrived(i, 2 * there + other), carry)[1], 0)

    def all_sent(i):
        for kind in (up, down, pair):
            along(i, w, kind, True, done)
        if not lines[i][2]:
            for kind in (up, down):
                along(i, mate, kind, False, done)

        def finish(t, carry):
            def one(kind, there):
                along(i, 2 * there + b, kind, False, done)
                if lines[i][2]:
                    along(i, 2 * there + b, pair, False, done)
                else:
                    along(i, 2 * there + other, kind, False, done)

            both_ways(t, one)
            return carry

        lax.fori_loop(1, length, finish, 0)

    early, later = (4, 0, 1), (2, 3)
    soon = [own_item(i) for i in early]
    tok_c[0].wait_recv()
    spot = o_tok.at[:, columns(across)]
    tok_fwd = push(spot, spot, tok_s.at[2], tok_r.at[2], {"section": beside})
    tok_fwd.start()
    for i in early:
        mate_item(i)
    steps(early, 1, 2)
    late += [own_item(i) for i in later]
    steps(early, 2, length)
    for i in later:
        mate_item(i)
    for i in early:
        pair_items(i)
    for c in soon:
        c.wait()
    own_tok.wait()
    tok_c[1].wait_recv()
    tok_fwd.wait_recv()

    wide = 2 * length
    small = qkv.shape[0]
    per = 128 // small
    for p in range(4):
        for g in range(wide // per):
            total = o_vec[p, g * per, 6:7]
            for j in range(1, per):
                total = total + o_vec[p, g * per + j, 6:7]
            gain[:, pl.ds((p * (wide // per) + g) * 128, 128)] = total
    micro, rows = mask.shape[:2]
    count = micro * rows
    chunk = 128
    chunks = count // chunk

    def project(k, carry):
        at = pl.ds(pl.multiple_of(k * chunk, chunk), chunk)
        unit, _ = row_norm(o_tok[at].astype(F32))
        o_n1[at] = (unit * gain[...]).astype(BF16)
        total = jnp.zeros((chunk, 3 * QUARTER), F32)
        for p in range(4):
            total = total + dot(o_n1[at, pl.ds(p * QUARTER, QUARTER)], o_qkv[p].reshape(QUARTER, 3 * QUARTER))
        o_act[at] = total.astype(BF16)
        return carry

    lax.fori_loop(0, chunks, project, 0)
    cuts = [1 + k * (length - 1) // 3 for k in range(4)]
    beside_core = 1 - core
    sends, crossing, spread = [], [], []
    for m in range(micro):
        at = pl.ds(m * rows, rows)
        for n in range(2):
            heads = attention_pair(n, lambda c: o_act[at, pl.ds(c, 128)], mask[m])
            got = [dot(probs.astype(BF16), v) for _, _, v, probs in heads]
            o_mixed[at, pl.ds(n * 128, 128)] = jnp.concatenate(got, axis=1).astype(BF16)
        for k in range(m * rows // chunk, (m + 1) * rows // chunk):
            at = pl.ds(k * chunk, chunk)
            part[at] = dot(o_mixed[at], o_out[...].reshape(QUARTER, width)).astype(BF16)
            for which, half in ((1, 1 - side), (0, side)):
                c = push(
                    part.at[at, columns(2 * half + beside_core)],
                    near_in.at[which, at],
                    s1.at[which, k],
                    r1.at[which, k],
                    {"section": beside},
                )
                c.start()
                sends.append(c)
        steps(later, cuts[m], cuts[m + 1])
    for k in range(chunks):
        at = pl.ds(k * chunk, chunk)
        sends[2 * k].wait()
        far[at] = (part[at, columns(2 * (1 - side) + core)].astype(F32) + near_in[1, at].astype(F32)).astype(BF16)
        c = push(far.at[at], far_in.at[at], s2.at[k], r2.at[k], {"section": across})
        c.start()
        crossing.append(c)
    for k in range(chunks):
        at = pl.ds(k * chunk, chunk)
        sends[2 * k + 1].wait()
        near = part[at, columns(me)].astype(F32) + near_in[0, at].astype(F32)
        crossing[k].wait()
        o_att[at, columns(me)] = (o_tok[at, columns(me)].astype(F32) + (near + far_in[at].astype(F32))).astype(BF16)
        here = o_att.at[at, columns(me)]
        for kind, to in ((0, across), (1, beside)):
            c = push(here, here, g_s.at[kind, k], g_r.at[kind, k], {"section": to})
            c.start()
            spread.append(c)
    steps(later, cuts[micro], cuts[3])
    for k in range(chunks):
        spread[2 * k].wait()
        here = o_att.at[pl.ds(k * chunk, chunk), columns(across)]
        c = push(here, here, g_s.at[2, k], g_r.at[2, k], {"section": beside})
        c.start()
        spread.append(c)
    for i in later:
        pair_items(i)
    for k in range(chunks):
        spread[2 * k + 1].wait()
        spread[2 * chunks + k].wait()
    for i in early + later:
        all_sent(i)
    for _, c in sent:
        c.wait_send()
    for c in tok_c + [tok_fwd]:
        c.wait_send()
    for c in exp_c + late:
        c.wait()


def head_call(qkv, inn, vec, outw, backw, first, second, tok, mask, wide, collective_id):
    small = qkv.shape[0]
    hid = inn.shape[1] // 4
    cut = 3 * QUARTER
    count = tok.shape[0]
    width = 4 * QUARTER
    chunks = count // 128
    outs = [
        ((4, wide, small, cut), BF16),
        ((4, wide, small, hid), BF16),
        ((4, wide, *vec.shape), F32),
        ((wide, *outw.shape), BF16),
        ((wide, *backw.shape), BF16),
        ((4, first.shape[0], hid), BF16),
        ((4, first.shape[0], hid), BF16),
        ((count, width), BF16),
        ((count, width), BF16),
        ((count, cut), BF16),
        ((count, QUARTER), BF16),
        ((count, width), BF16),
    ]
    return call(
        head_kernel,
        tuple(jax.ShapeDtypeStruct(*o) for o in outs),
        [ANY] * 8 + [VM],
        (VM, ANY, VM, VM, ANY, ANY, ANY, VM, VM, VM, VM, VM),
        [
            pltpu.VMEM((4, small, cut), BF16),
            pltpu.VMEM((4, small, hid), BF16),
            pltpu.VMEM((4, *vec.shape), F32),
            pltpu.VMEM((1, width), F32),
            pltpu.VMEM((count, width), BF16),
            pltpu.VMEM((2, count, QUARTER), BF16),
            pltpu.VMEM((count, QUARTER), BF16),
            pltpu.VMEM((count, QUARTER), BF16),
            DMA((16,)),
            DMA((5, 3)),
            DMA((5, 3)),
            DMA((3,)),
            DMA((3,)),
            DMA((3, 5, wide)),
            DMA((5, wide)),
            DMA((2, 3)),
            DMA((2, 3)),
            DMA((2, chunks)),
            DMA((2, chunks)),
            DMA((chunks,)),
            DMA((chunks,)),
            DMA((3, chunks)),
            DMA((3, chunks)),
        ],
        collective_id,
        *(qkv, inn, vec, outw, backw, first, second, tok, mask),
    )


def dot(left, right):
    return jnp.dot(left, right, preferred_element_type=F32)


def dot_nt(left, right):
    return lax.dot_general(left, right, (((1,), (1,)), ((), ())), preferred_element_type=F32)


def dot_tn(left, right):
    return lax.dot_general(left, right, (((0,), (0,)), ((), ())), preferred_element_type=F32)


def gelu_value(v):
    return 0.5 * v * (1.0 + lax.erf(v * 0.7071067811865476))


def gelu_slope(v):
    return (
        0.5 * (1.0 + lax.erf(v * 0.7071067811865476))
        + v * jnp.exp(-0.5 * v * v) * 0.3989422804014327
    )


def unit_norm(v):
    centred = v - jnp.mean(v, axis=-1, keepdims=True)
    scale = lax.rsqrt(jnp.mean(centred * centred, axis=-1, keepdims=True) + 1e-05)
    return centred * scale, scale


IDS = {}


def id_of(*key):
    return IDS.setdefault(key, len(IDS))


def reduce_quarters(part, stats=None):
    return reduce_call(part.astype(BF16), stats, id_of("reduce", part.shape, stats is None))


def gather_quarters(quarter):
    return gather_call(quarter, id_of("gather", quarter.shape))


def wide_exchange(slots, spread):
    return exchange_call(slots, spread, id_of("exchange", spread))


def allowed_of(lengths, rows):
    pos = jnp.arange(rows, dtype=jnp.int32)
    group = pos[None] // lengths[:, None]
    return ((pos[:, None] >= pos[None, :])[None] & (group[:, :, None] == group[:, None, :])).astype(F32)


def body(
    tokens_in,
    cotangent,
    routes,
    seq_lengths,
    qkv_weight,
    out_weight,
    attn_gain,
    ffn_in,
    ffn_back,
    ffn_gain,
    centroids,
    first_gain,
    first_in,
    first_back,
    second_gain,
    second_in,
    second_back,
):
    sections = lax.axis_size("section")
    wide = lax.axis_size("wide")
    section_id = lax.axis_index("section")
    wide_id = lax.axis_index("wide")
    micro, rows, quarter = tokens_in.shape
    width = quarter * sections
    cap = 5 * rows // (4 * wide)
    tok_rows = micro * rows
    hid = first_back.shape[1]
    small = qkv_weight.shape[0]
    qkv_cols = qkv_weight.shape[1] // sections

    per = 128 // small
    spread = lambda v: lax.dynamic_update_slice_in_dim(
        jnp.zeros((1, 128), F32), v.astype(F32)[None], lax.rem(wide_id, per) * small, 1
    )
    vectors = [v.astype(F32).reshape(2, 128) for v in (first_gain, second_gain, centroids)]
    vectors = jnp.concatenate(vectors + [spread(attn_gain), spread(ffn_gain)], axis=0)
    allowed = allowed_of(seq_lengths, rows)
    tokens_q = tokens_in.reshape(tok_rows, quarter)

    (qkv_w, in_w, vectors, out_w, back_w, first_w, second_w, tokens, normed_a, packed, mixed, attended) = head_call(
        qkv_weight,
        ffn_in,
        vectors,
        out_weight,
        ffn_back,
        first_in[0],
        second_in[0],
        tokens_q,
        allowed,
        wide,
        id_of("head"),
    )
    qkv_w = qkv_w.reshape(width, qkv_cols)
    in_w = in_w.reshape(width, hid)
    out_w = out_w.reshape(quarter, width)
    back_w = back_w.reshape(hid, width)
    first_w = first_w.reshape(width, hid)
    second_w = second_w.reshape(width, hid)
    own = lax.dynamic_index_in_dim(vectors, wide_id, axis=1, keepdims=False)
    gain_first, gain_second, centre = (own[:, 2 * j : 2 * j + 2].reshape(1, width) for j in range(3))
    gain_attn, gain_ffn = (
        jnp.sum(vectors[:, :, j].reshape(sections, wide // per, per, 128), axis=2).reshape(1, width) for j in (6, 7)
    )
    own_quarter = lambda v: lax.dynamic_slice_in_dim(v, section_id * quarter, quarter, axis=1)
    first_b = first_back[0]
    second_b = second_back[0]

    experts = jnp.arange(wide, dtype=jnp.int32)
    choose = (routes == experts).astype(jnp.int32)
    upto = (jnp.arange(rows)[:, None] >= jnp.arange(rows)[None, :]).astype(BF16)
    ranking = jnp.einsum("rk,mke->mre", upto, choose.astype(BF16), preferred_element_type=F32).astype(jnp.int32) - 1
    slot_of = routes[:, :, 0] * cap + jnp.sum(ranking * choose, axis=2)
    onehot = (jnp.arange(wide * cap, dtype=jnp.int32)[None, :, None] == slot_of[:, None, :]).astype(BF16)

    def to_experts(rows_q):
        packed = jnp.einsum("msr,mrd->msd", onehot, rows_q.reshape(micro, rows, quarter), preferred_element_type=F32)
        packed = packed.astype(BF16).reshape(micro, wide, cap, quarter).transpose(1, 0, 2, 3)
        return wide_exchange(packed.reshape(wide, micro * cap, quarter), True).reshape(wide * micro * cap, width)

    def to_tokens(slots_q):
        back = wide_exchange(slots_q.reshape(wide, micro * cap, quarter), False)
        back = back.reshape(wide, micro, cap, quarter).transpose(1, 0, 2, 3).reshape(micro, wide * cap, quarter)
        got = jnp.einsum("msr,msd->mrd", onehot, back, preferred_element_type=F32)
        return got.astype(BF16).reshape(tok_rows, quarter)

    attended_q = own_quarter(attended)

    def branch(v, w_in, w_back, gain):
        unit, scale = unit_norm(v.astype(F32))
        normed = (unit * gain).astype(BF16)
        pre = dot(normed, w_in)
        hidden = gelu_value(pre).astype(BF16)
        return (normed, unit, scale, pre, hidden), dot(hidden, w_back)

    def branch_back(grad, saved, w_in, w_back, gain, more=None):
        normed, unit, scale, pre, hidden = saved
        d_back = dot_tn(hidden, grad)
        d_pre = (dot_nt(grad, w_back) * gelu_slope(pre)).astype(BF16)
        d_in = dot_tn(normed, d_pre)
        return d_in, d_back, norm_back(dot_nt(d_pre, w_in), unit, scale, gain, more)

    def norm_back(d_part, unit, scale, gain, more=None):
        d_unit = d_part * gain
        sums = jnp.stack([jnp.sum(d_unit, axis=1), jnp.sum(d_unit * unit, axis=1)])
        if more is not None:
            sums = jnp.concatenate([sums, more])
        d_q, sums = reduce_quarters(d_part, jnp.pad(sums, ((0, 8 - sums.shape[0]), (0, 0))))
        extra, sums = sums[2], sums / width
        unit_q = own_quarter(unit)
        d_rows = scale * (d_q * own_quarter(gain) - sums[0][:, None] - unit_q * sums[1][:, None])
        return d_rows, jnp.sum(d_q * unit_q, axis=0), extra

    saved_d, part = branch(attended, in_w, back_w, gain_ffn)
    fed_q = (attended_q.astype(F32) + reduce_quarters(part)).astype(BF16)
    routed = to_experts(fed_q)
    routed_q = own_quarter(routed)
    d_mixed = to_experts(cotangent.reshape(tok_rows, quarter)).astype(F32)
    d_mixed_q = own_quarter(d_mixed)
    saved_1, part = branch(routed, first_w, first_b, gain_first)
    first_q = (routed_q.astype(F32) + reduce_quarters(part)).astype(BF16)
    first = gather_quarters(first_q)
    saved_2, part = branch(first, second_w, second_b, gain_second)
    gate = jax.nn.sigmoid(jnp.sum(routed.astype(F32) * centre, axis=-1, keepdims=True))
    second_q = first_q.astype(F32) + reduce_quarters(part)
    mixed_q = routed_q.astype(F32) + gate * second_q
    block_out = to_tokens(mixed_q.astype(BF16)).reshape(micro, rows, quarter)

    d_second = gate * d_mixed
    d_second_q = gate * d_mixed_q
    d_second_in, d_second_back, (norm_q, second_gain_grad, d_logit) = branch_back(
        d_second.astype(BF16), saved_2, second_w, second_b, gain_second, jnp.sum(d_mixed_q * second_q, axis=-1)[None]
    )
    d_logit = d_logit[:, None] * gate * (1.0 - gate)
    centroids_grad = jnp.sum(d_logit * routed_q.astype(F32), axis=0)[None]
    d_gated_q = (d_mixed_q + d_logit * own_quarter(centre)).astype(BF16)
    d_first_q = (d_second_q + norm_q).astype(BF16)
    d_first_in, d_first_back, (norm_q, first_gain_grad, _) = branch_back(
        gather_quarters(d_first_q), saved_1, first_w, first_b, gain_first
    )
    d_routed_q = (d_first_q.astype(F32) + norm_q + d_gated_q.astype(F32)).astype(BF16)
    d_fed_q = to_tokens(d_routed_q)
    d_in, d_back, (norm_q, d_gain_ffn, _) = branch_back(gather_quarters(d_fed_q), saved_d, in_w, back_w, gain_ffn)
    d_attended_q = (d_fed_q.astype(F32) + norm_q).astype(BF16)
    d_attended = gather_quarters(d_attended_q)
    def by_row(grad):
        return grad.astype(BF16).reshape(sections, wide, small, grad.shape[1])

    qkv_grad, ffn_in_grad, out_grad, ffn_back_grad, d_gains, d_first_in, d_second_in, tokens_grad = tail_call(
        by_row(d_in),
        d_back.astype(BF16).reshape(wide, hid // wide, width),
        d_first_in.astype(BF16).reshape(sections, quarter, hid),
        d_second_in.astype(BF16).reshape(sections, quarter, hid),
        d_attended,
        tokens,
        normed_a,
        packed,
        mixed,
        qkv_w,
        out_w,
        allowed,
        gain_attn,
        d_gain_ffn[None],
        id_of("tail"),
    )
    d_gains = lax.dynamic_slice_in_dim(d_gains, wide_id * small, small, axis=1)
    tokens_grad = tokens_grad.reshape(micro, rows, quarter)
    return (
        block_out,
        tokens_grad,
        qkv_grad.astype(F32),
        out_grad,
        d_gains[0],
        ffn_in_grad.astype(F32),
        ffn_back_grad,
        d_gains[1],
        centroids_grad,
        first_gain_grad[None],
        d_first_in[None].astype(F32),
        d_first_back[None],
        second_gain_grad[None],
        d_second_in[None].astype(F32),
        d_second_back[None],
    )


def solution(mesh):
    dense = P(("section", "wide"), None)
    dense_gain = P(("section", "wide"))
    tokens = P(None, "wide", "section")
    gain = P("wide", "section")
    expert = P("wide", "section", None)
    in_specs = (
        (tokens, tokens, P(None, "wide", None), P(), dense, dense, dense_gain, dense, dense, dense_gain)
        + (gain, gain, expert, expert, gain, expert, expert)
    )
    out_specs = (
        (tokens, tokens, dense, dense, dense_gain, dense, dense, dense_gain)
        + (gain, gain, expert, expert, gain, expert, expert)
    )
    return jax.shard_map(body, mesh=mesh, in_specs=in_specs, out_specs=out_specs, check_vma=False)
```

```python
import functools

import jax
import jax.numpy as jnp
from jax import lax
from jax.experimental import pallas as pl
from jax.experimental.pallas import tpu as pltpu
from jax.sharding import PartitionSpec as P

HEAD_SIZE = 64
F32 = jnp.float32
BF16 = jnp.bfloat16

MESH = pl.DeviceIdType.MESH
ANY = pl.BlockSpec(memory_space=pl.ANY)
VM = pl.BlockSpec(memory_space=pltpu.VMEM)
DMA = pltpu.SemaphoreType.DMA
VMEM_BYTES = 60 * 1024 * 1024
QUARTER = 256


def section_places():
    me = lax.axis_index("section")
    return me, me + 1 - 2 * lax.rem(me, 2), me + 2 - 4 * lax.div(me, 2)


def greet(peers):
    barrier = pltpu.get_barrier_semaphore()
    for peer in peers:
        pl.semaphore_signal(barrier, inc=1, device_id=peer, device_id_type=MESH)
    pl.semaphore_wait(barrier, len(peers))


def push(src, dst, send, recv, peer):
    return pltpu.make_async_remote_copy(
        src_ref=src, dst_ref=dst, send_sem=send, recv_sem=recv, device_id=peer, device_id_type=MESH
    )


def columns(which):
    return pl.ds(pl.multiple_of(which * QUARTER, QUARTER), QUARTER)


def call(kernel, out_shape, in_specs, out_specs, scratch, collective_id, *operands):
    return pl.pallas_call(
        kernel,
        out_shape=out_shape,
        in_specs=in_specs,
        out_specs=out_specs,
        scratch_shapes=scratch,
        compiler_params=pltpu.CompilerParams(
            collective_id=collective_id, has_side_effects=True, vmem_limit_bytes=VMEM_BYTES
        ),
    )(*operands)


def reduce_kernel(chunks, with_stats, *refs):
    if with_stats:
        part, stats, out, stats_out = refs[:4]
        first_in, far, far_in, s1, r1, s2, r2, st_in, st_mid, st_far, st_s, st_r = refs[4:]
    else:
        part, out, first_in, far, far_in, s1, r1, s2, r2 = refs
    me, beside, across = section_places()
    core, side = lax.rem(me, 2), lax.div(me, 2)
    greet([{"section": beside}, {"section": across}])
    rows = part.shape[0] // chunks
    beside_core = 1 - core
    sends = []
    if with_stats:
        st = push(stats, st_in, st_s.at[0], st_r.at[0], {"section": beside})
        st.start()
    for k in range(chunks):
        for which, half in ((1, 1 - side), (0, side)):
            at = pl.ds(k * rows, rows)
            c = push(
                part.at[at, columns(2 * half + beside_core)],
                first_in.at[which, at],
                s1.at[which, k],
                r1.at[which, k],
                {"section": beside},
            )
            c.start()
            sends.append(c)
    if with_stats:
        st.wait()
        st_mid[...] = stats[...] + st_in[...]
        st2 = push(st_mid, st_far, st_s.at[1], st_r.at[1], {"section": across})
        st2.start()
    crossing = []
    for k in range(chunks):
        at = pl.ds(k * rows, rows)
        sends[2 * k].wait()
        far[at] = (part[at, columns(2 * (1 - side) + core)].astype(F32) + first_in[1, at].astype(F32)).astype(BF16)
        c = push(far.at[at], far_in.at[at], s2.at[k], r2.at[k], {"section": across})
        c.start()
        crossing.append(c)
    for k in range(chunks):
        at = pl.ds(k * rows, rows)
        sends[2 * k + 1].wait()
        near = part[at, columns(me)].astype(F32) + first_in[0, at].astype(F32)
        crossing[k].wait()
        out[at] = near + far_in[at].astype(F32)
    if with_stats:
        st2.wait()
        stats_out[...] = st_mid[...] + st_far[...]


def reduce_call(part, stats, collective_id, chunks=4):
    rows, _ = part.shape
    scratch = [
        pltpu.VMEM((2, rows, QUARTER), BF16),
        pltpu.VMEM((rows, QUARTER), BF16),
        pltpu.VMEM((rows, QUARTER), BF16),
        DMA((2, chunks)),
        DMA((2, chunks)),
        DMA((chunks,)),
        DMA((chunks,)),
    ]
    out = jax.ShapeDtypeStruct((rows, QUARTER), F32)
    if stats is None:
        return call(
            functools.partial(reduce_kernel, chunks, False), out, [VM], VM, scratch, collective_id, part
        )
    st = pltpu.VMEM(stats.shape, F32)
    return call(
        functools.partial(reduce_kernel, chunks, True),
        (out, jax.ShapeDtypeStruct(stats.shape, F32)),
        [VM, VM],
        (VM, VM),
        scratch + [st, st, st, DMA((2,)), DMA((2,))],
        collective_id,
        part,
        stats,
    )


def gather_kernel(chunks, q, out, s, r):
    me, beside, across = section_places()
    greet([{"section": beside}, {"section": across}])
    rows = q.shape[0] // chunks
    copies = []
    for k in range(chunks):
        at = pl.ds(k * rows, rows)
        for kind, to in ((0, across), (1, beside)):
            c = push(q.at[at], out.at[at, columns(me)], s.at[kind, k], r.at[kind, k], {"section": to})
            c.start()
            copies.append(c)
    out[:, columns(me)] = q[...]
    for k in range(chunks):
        at = pl.ds(k * rows, rows)
        copies[2 * k].wait()
        here = out.at[at, columns(across)]
        c = push(here, here, s.at[2, k], r.at[2, k], {"section": beside})
        c.start()
        copies.append(c)
    for k in range(chunks):
        copies[2 * k + 1].wait()
        copies[2 * chunks + k].wait()


def gather_call(q, collective_id, chunks=4):
    rows = q.shape[0]
    return call(
        functools.partial(gather_kernel, chunks),
        jax.ShapeDtypeStruct((rows, 4 * QUARTER), BF16),
        [VM],
        VM,
        [DMA((3, chunks)), DMA((3, chunks))],
        collective_id,
        q,
    )


def exchange_kernel(spread, src, out, s, r):
    me, beside, across = section_places()
    w = lax.axis_index("wide")
    count = src.shape[0]
    peers = [{"wide": lax.rem(w + j, count)} for j in range(1, count)]
    greet(peers + ([{"section": beside}, {"section": across}] if spread else []))

    def place(which, block):
        return out.at[block, :, columns(which)] if spread else out.at[block]

    def wide_copy(to):
        return push(src.at[to], place(me, w), s.at[0, to], r.at[0, w], {"wide": to})

    def arrival(frm):
        return push(src.at[frm], place(me, frm), s.at[0, frm], r.at[0, frm], {"wide": frm})

    def spread_copy(kind, block, to):
        here = place(across, block) if kind == 3 else place(me, block)
        return push(here, here, s.at[kind, block], r.at[kind, block], {"section": to})

    for j in range(1, count):
        wide_copy(lax.rem(w + j, count)).start()
    if spread:
        out[w, :, columns(me)] = src[w]
    else:
        out[w] = src[w]
    for j in range(count):
        block = lax.rem(w + j, count)
        if j:
            arrival(block).wait_recv()
        if spread:
            spread_copy(1, block, across).start()
            spread_copy(2, block, beside).start()
    if spread:
        for j in range(count):
            block = lax.rem(w + j, count)
            spread_copy(1, block, across).wait_recv()
            spread_copy(3, block, beside).start()
        for j in range(count):
            block = lax.rem(w + j, count)
            spread_copy(1, block, across).wait_send()
            spread_copy(2, block, beside).wait()
            spread_copy(3, block, beside).wait()
    for j in range(1, count):
        wide_copy(lax.rem(w + j, count)).wait_send()


def exchange_call(slots, spread, collective_id):
    count, n, quarter = slots.shape
    return call(
        functools.partial(exchange_kernel, spread),
        jax.ShapeDtypeStruct((count, n, 4 * quarter if spread else quarter), BF16),
        [VM],
        VM,
        [DMA((4, count)), DMA((4, count))],
        collective_id,
        slots,
    )


GROUP = 32


def add_rows(dst, left, right):
    if len(dst.shape) == 3:
        for j in range(dst.shape[0]):
            add_rows(dst.at[j], left.at[j], right.at[j])
        return
    rows = dst.shape[0]
    step = min(rows, GROUP)

    def one(j, carry):
        at = pl.ds(pl.multiple_of(j * step, step), step)
        dst[at] = (left[at].astype(F32) + right[at].astype(F32)).astype(dst.dtype)
        return carry

    lax.fori_loop(0, rows // step, one, 0)


def attention_pair(pair, qkv, mask):
    q2, k2, v2 = (qkv(j * QUARTER + pair * 128) for j in range(3))
    got = []
    for h in range(2):
        q, k, v = (x[:, h * HEAD_SIZE : (h + 1) * HEAD_SIZE] for x in (q2, k2, v2))
        scores = jnp.where(mask > 0.0, dot_nt(q, k) * HEAD_SIZE ** (-0.5), -1e30)
        expo = jnp.exp(scores - jnp.max(scores, axis=-1, keepdims=True))
        got.append((q, k, v, expo / jnp.sum(expo, axis=-1, keepdims=True)))
    return got


def row_norm(v):
    centred = v - jnp.mean(v, axis=-1, keepdims=True)
    scale = lax.rsqrt(jnp.mean(centred * centred, axis=-1, keepdims=True) + 1e-05)
    return centred * scale, scale


def line_of_wide():
    w = lax.axis_index("wide")
    length = lax.axis_size("wide") // 2
    return w, length, lax.div(w, 2), lax.rem(w, 2)


def greet_line(section_peers, all_wide):
    w, length, a, b = line_of_wide()
    barrier = pltpu.get_barrier_semaphore()
    for p in section_peers:
        pl.semaphore_signal(barrier, inc=1, device_id={"section": p}, device_id_type=MESH)
    if all_wide:
        for j in range(1, 2 * length):
            pl.semaphore_signal(
                barrier, inc=1, device_id={"wide": lax.rem(w + j, 2 * length)}, device_id_type=MESH
            )
        pl.semaphore_wait(barrier, len(section_peers) + 2 * length - 1)
        return
    pl.semaphore_signal(barrier, inc=1, device_id={"wide": 2 * a + 1 - b}, device_id_type=MESH)

    @pl.when(a > 0)
    def _():
        pl.semaphore_signal(barrier, inc=1, device_id={"wide": w - 2}, device_id_type=MESH)

    @pl.when(a < length - 1)
    def _():
        pl.semaphore_signal(barrier, inc=1, device_id={"wide": w + 2}, device_id_type=MESH)

    pl.semaphore_wait(barrier, len(section_peers) + 1 + jnp.minimum(a, 1) + jnp.minimum(length - 1 - a, 1))


def tail_kernel(*refs):
    (g_in, g_back, first, second, d_att, tok, n1, qkv, mixed, w_qkv, w_out, mask, gain, gain_d, res) = refs[:15]
    o_qkv, o_in, o_out, o_back, o_gain, o_first, o_second, o_tok, o_res = refs[15:24]
    g_qkv, g_out = refs[24:26]
    acc = refs[26:30]
    line_in = refs[30:34]
    pair_in = refs[34:38]
    (d_mix, d_qkv, part, unit, scales, stats, stats_in, stats_mid, stats_far, near_in, far, far_in, gains, gains_in) = refs[38:52]
    (loc, exp_s, exp_r, cut_s, cut_r, pair_s, pair_r, line_s, line_r, s1, r1, s2, r2, st_s, st_r, gn_s, gn_r, o_s, o_r) = refs[52:]
    src = (g_qkv, g_in, g_out, g_back)
    pair_first = (True, True, False, False)
    me, beside, across = section_places()
    diagonal = beside + across - me
    core, side = lax.rem(me, 2), lax.div(me, 2)
    w, length, a, b = line_of_wide()
    other = 1 - b
    mate = {"wide": 2 * a + other}
    peers = [beside, across, diagonal]
    greet_line(peers, True)
    hid = first.shape[2]
    rows = mask.shape[1]
    micro = mask.shape[0]
    late = []

    def spot(ref, which, count):
        return ref.at[:, pl.ds(pl.multiple_of(which * count, count), count)]

    def pair_copy(i, there):
        return push(
            src[i].at[:, 2 * there + other], pair_in[i].at[there], pair_s.at[i, there], pair_r.at[i, there], mate
        )

    def slots(i, there):
        if pair_first[i]:
            return [(there, 2 * there + b)]
        return [(2 * there, 2 * there), (2 * there + 1, 2 * there + 1)]

    def line_copy(i, block, to_block, to):
        return push(acc[i].at[block], line_in[i].at[to_block], line_s.at[i, block], line_r.at[i, to_block], {"wide": to})

    def ready(i, there, block, own):
        if pair_first[i]:
            pair_copy(i, there).wait_recv()
            add_rows(acc[i].at[block], src[i].at[:, own], pair_in[i].at[there])
        else:
            acc[i][block] = src[i][own]

    def flow(i, there, from_edge, to):
        n = 1 if pair_first[i] else 2
        for j, (block, own) in enumerate(slots(i, there)):
            ready(i, there, block, own)

            @pl.when(from_edge)
            def _():
                line_copy(i, block, block, w).wait_recv()
                add_rows(acc[i].at[block], acc[i].at[block], line_in[i].at[block])

            if to == "down":
                line_copy(i, block, block, w - 2).start()
            else:
                target = jnp.where(there == a + 1, n * length + j, block)
                line_copy(i, block, target, w + 2).start()

    def pairs(i):
        lax.fori_loop(0, length, lambda t, c: (pair_copy(i, t).start(), c)[1], 0)

    def steps(group, start, stop):
        def step(t, carry):
            high = length - 1 - t
            for i in group:

                @pl.when(t < a)
                def _():
                    flow(i, t, a < length - 1, "down")

                @pl.when(high > a)
                def _():
                    flow(i, high, a > 0, "up")

            return carry

        lax.fori_loop(start, stop, step, 0)

    finals = {}

    def own_block(i):
        n = 1 if pair_first[i] else 2
        for j, (block, own) in enumerate(slots(i, a)):
            ready(i, a, block, own)

            @pl.when(a < length - 1)
            def _():
                line_copy(i, block, block, w).wait_recv()
                add_rows(acc[i].at[block], acc[i].at[block], line_in[i].at[block])

            @pl.when(a > 0)
            def _():
                line_copy(i, block, n * length + j, w).wait_recv()
                add_rows(acc[i].at[block], acc[i].at[block], line_in[i].at[n * length + j])

        if not pair_first[i]:
            c = push(acc[i].at[2 * a + other], pair_in[i].at[0], pair_s.at[i, 0], pair_r.at[i, 0], mate)
            c.start()
            finals[i] = c
            return
        block = acc[i].at[a]

        def cut(p):
            if i == 1:
                return [(block.at[p], spot(o_in, me, hid))]
            third = [pl.ds(j * QUARTER, QUARTER) for j in range(3)]
            return [(block.at[p, :, third[j]], spot(o_qkv, 4 * j + me, QUARTER)) for j in range(3)]

        for k, p in enumerate(peers):
            for j, (here, there) in enumerate(cut(p)):
                n = 3 * i + j
                c = push(here, there, cut_s.at[n, k], cut_r.at[n, k], {"section": p})
                c.start()
                late.append(c)
        for j, (here, there) in enumerate(cut(me)):
            c = pltpu.make_async_copy(here, there, loc.at[2 + 3 * i + j])
            c.start()
            late.append(c)

    pairs(1)
    for i, (s, d) in enumerate(((first, o_first), (second, o_second))):
        c = pltpu.make_async_copy(s.at[me], spot(d, me, hid), loc.at[i])
        c.start()
        late.append(c)
        for k, p in enumerate((across, diagonal, beside)):
            c = push(s.at[p], spot(d, me, hid), exp_s.at[i, k], exp_r.at[i, k], {"section": p})
            c.start()
            late.append(c)
    def res_copy(to, frm):
        return push(res.at[to], o_res.at[frm], o_s.at[to], o_r.at[frm], {"wide": to})

    for j in range(1, 2 * length):
        res_copy(lax.rem(w + j, 2 * length), w).start()
    o_res[w] = res[w]
    group = (3, 1)
    cuts = [k * length // 4 for k in range(5)]
    small = g_out.shape[1]
    wide = 2 * length

    def store_blocks(ref, index, value):
        for j in range(wide):
            piece = value[j * small : (j + 1) * small].astype(BF16)
            if index is None:
                ref[j] = piece
            else:
                ref[index, j] = piece

    for m in range(micro):
        at = pl.ds(m * rows, rows)
        d_mix[at] = dot_nt(d_att[at], w_out[...]).astype(BF16)
    store_blocks(g_out, None, dot_tn(mixed[...], d_att[...]))
    steps(group, cuts[0], cuts[1])

    def micro_back(m, carry):
        at = pl.ds(pl.multiple_of(m * rows, rows), rows)
        for pair in range(2):
            heads = attention_pair(pair, lambda c: qkv[at, pl.ds(c, 128)], mask[m])
            d_pair = d_mix[at, pl.ds(pair * 128, 128)]
            grads = []
            for h, (q, k, v, probs) in enumerate(heads):
                d_out = d_pair[:, h * HEAD_SIZE : (h + 1) * HEAD_SIZE]
                d_probs = dot_nt(d_out, v)
                delta = jnp.sum(probs * d_probs, axis=-1, keepdims=True)
                d_scores = (probs * (d_probs - delta) * HEAD_SIZE ** (-0.5)).astype(BF16)
                grads.append((dot(d_scores, k), dot_tn(d_scores, q), dot_tn(probs.astype(BF16), d_out)))
            for j in range(3):
                both = jnp.concatenate([grads[0][j], grads[1][j]], axis=1).astype(BF16)
                d_qkv[at, pl.ds(j * QUARTER + pair * 128, 128)] = both
        return carry

    for m in range(micro):
        micro_back(m, 0)
        steps(group, cuts[1 + m], cuts[2 + m])
    for p in range(4):
        store_blocks(g_qkv, p, dot_tn(n1[:, pl.ds(p * QUARTER, QUARTER)], d_qkv[...]))
    pairs(0)
    steps((2,), 0, length)

    count = d_att.shape[0]
    chunk = 128
    chunks = count // chunk
    lane = lax.broadcasted_iota(jnp.int32, (chunk, 128), 1)
    beside_core = 1 - core
    sends = []
    for k in range(chunks):
        at = pl.ds(k * chunk, chunk)
        u, scale = row_norm(tok[at].astype(F32))
        unit[at] = u
        scales[at] = jnp.broadcast_to(scale, (chunk, 128))
        d_normed = dot_nt(d_qkv[at], w_qkv[...])
        part[at] = d_normed.astype(BF16)
        d_unit = d_normed * gain[...]
        sum_a = jnp.sum(d_unit, axis=-1, keepdims=True)
        sum_b = jnp.sum(d_unit * u, axis=-1, keepdims=True)
        both = jnp.where(lane == 0, sum_a, jnp.where(lane == 1, sum_b, 0.0))
        stats[:, at] = both.T[:8]
        for which, half in ((1, 1 - side), (0, side)):
            c = push(
                part.at[at, columns(2 * half + beside_core)],
                near_in.at[which, at],
                s1.at[which, k],
                r1.at[which, k],
                {"section": beside},
            )
            c.start()
            sends.append(c)
    st1 = push(stats, stats_in, st_s.at[0], st_r.at[0], {"section": beside})
    st1.start()
    crossing = []
    for k in range(chunks):
        at = pl.ds(k * chunk, chunk)
        sends[2 * k].wait()
        far[at] = (part[at, columns(2 * (1 - side) + core)].astype(F32) + near_in[1, at].astype(F32)).astype(BF16)
        c = push(far.at[at], far_in.at[at], s2.at[k], r2.at[k], {"section": across})
        c.start()
        crossing.append(c)
    st1.wait()
    stats_mid[...] = stats[...] + stats_in[...]
    st2 = push(stats_mid, stats_far, st_s.at[1], st_r.at[1], {"section": across})
    st2.start()
    steps(group, cuts[3], cuts[4])
    steps((0,), 0, length)
    st2.wait()
    stats[...] = (stats_mid[...] + stats_far[...]) * (1.0 / gain.shape[1])
    total = jnp.zeros((1, QUARTER), F32)
    gain_q = gain[:, columns(me)]
    for k in range(chunks):
        at = pl.ds(k * chunk, chunk)
        sends[2 * k + 1].wait()
        near = part[at, columns(me)].astype(F32) + near_in[0, at].astype(F32)
        crossing[k].wait()
        d_q = near + far_in[at].astype(F32)
        u = unit[at, columns(me)]
        sums = jnp.concatenate([stats[:, at], jnp.zeros((chunk - 8, chunk), F32)], axis=0).T
        norm = scales[at, pl.ds(0, 1)] * (d_q * gain_q - sums[:, 0:1] - u * sums[:, 1:2])
        o_tok[at] = d_att[at, columns(me)].astype(F32) + norm
        total = total + jnp.sum(d_q * u, axis=0, keepdims=True)
    row = lax.broadcasted_iota(jnp.int32, (8, QUARTER), 0)
    gains[...] = jnp.where(row == 0, total, jnp.where(row == 1, gain_d[...], 0.0))

    def gain_copy(to, frm):
        return push(gains, gains_in.at[frm], gn_s.at[to], gn_r.at[frm], {"wide": to})

    for j in range(1, wide):
        gain_copy(lax.rem(w + j, wide), w).start()
    for i in (3, 1, 2, 0):
        own_block(i)
    gathered = gains[...]
    for j in range(1, wide):
        frm = lax.rem(w + j, wide)
        gain_copy(frm, frm).wait_recv()
        gathered = gathered + gains_in[frm]
    o_gain[...] = gathered
    for i, out in ((3, o_back), (2, o_out)):
        finals[i].wait_recv()
        add_rows(out, acc[i].at[2 * a + b], pair_in[i].at[0])
    for c in finals.values():
        c.wait_send()
    for c in late:
        c.wait()
    for j in range(1, wide):
        to = lax.rem(w + j, wide)
        gain_copy(to, w).wait_send()
        res_copy(to, w).wait_send()
        res_copy(to, to).wait_recv()

    def finish(t, carry):
        for i in range(4):
            if pair_first[i]:
                pair_copy(i, t).wait_send()

            @pl.when(t != a)
            def _():
                for block, _ in slots(i, t):
                    line_copy(i, block, block, w).wait_send()

        return carry

    lax.fori_loop(0, length, finish, 0)


def tail_call(g_in, g_back, first, second, d_att, tok, n1, qkv, mixed, w_qkv, w_out, mask, gain, gain_d, res, collective_id):
    wide = g_back.shape[0]
    length = wide // 2
    small = g_in.shape[2]
    hid = first.shape[2]
    count, width = d_att.shape
    chunks = count // 128
    shapes = [(4, small, 3 * QUARTER), (4, small, hid), (small, width), g_back.shape[1:]]
    expert = ((first.shape[1], 4 * hid), BF16)
    outs = [
        ((small, 3 * width), BF16),
        ((small, 4 * hid), BF16),
        (shapes[2], F32),
        (shapes[3], F32),
        ((8, QUARTER), F32),
        expert,
        expert,
        ((count, QUARTER), F32),
        (res.shape, BF16),
    ]
    scratch = [pltpu.VMEM((4, wide, small, 3 * QUARTER), BF16), pltpu.VMEM((wide, small, width), BF16)]
    for counts in (
        [length, length, wide, wide],
        [length + 1, length + 1, wide + 2, wide + 2],
        [length, length, 1, 1],
    ):
        scratch += [pltpu.VMEM((n, *s), BF16) for n, s in zip(counts, shapes)]
    scratch += [
        pltpu.VMEM((count, QUARTER), BF16),
        pltpu.VMEM((count, 3 * QUARTER), BF16),
        pltpu.VMEM((count, width), BF16),
        pltpu.VMEM((count, width), F32),
        pltpu.VMEM((count, 128), F32),
        pltpu.VMEM((8, count), F32),
        pltpu.VMEM((8, count), F32),
        pltpu.VMEM((8, count), F32),
        pltpu.VMEM((8, count), F32),
        pltpu.VMEM((2, count, QUARTER), BF16),
        pltpu.VMEM((count, QUARTER), BF16),
        pltpu.VMEM((count, QUARTER), BF16),
        pltpu.VMEM((8, QUARTER), F32),
        pltpu.VMEM((wide, 8, QUARTER), F32),
        DMA((8,)),
        DMA((2, 3)),
        DMA((2, 3)),
        DMA((4, 3)),
        DMA((4, 3)),
        DMA((4, length)),
        DMA((4, length)),
        DMA((4, wide)),
        DMA((4, wide + 2)),
        DMA((2, chunks)),
        DMA((2, chunks)),
        DMA((chunks,)),
        DMA((chunks,)),
        DMA((2,)),
        DMA((2,)),
        DMA((wide,)),
        DMA((wide,)),
        DMA((wide,)),
        DMA((wide,)),
    ]
    return call(
        tail_kernel,
        tuple(jax.ShapeDtypeStruct(*o) for o in outs),
        [VM, VM, ANY, ANY] + [VM] * 11,
        (ANY, ANY, VM, VM, VM, ANY, ANY, VM, VM),
        scratch,
        collective_id,
        *(g_in, g_back, first, second, d_att, tok, n1, qkv, mixed, w_qkv, w_out, mask, gain, gain_d, res),
    )


def head_kernel(*refs):
    qkv, inn, vec, outw, backw, first, second, tok, mask, cot = refs[:10]
    o_qkv, o_in, o_vec, o_out, o_back, o_first, o_second, o_tok, o_n1, o_act, o_mixed, o_att, o_cot = refs[10:23]
    st_qkv, st_in, st_vec, gain, part, near_in, far, far_in = refs[23:31]
    loc, cut_s, cut_r, tok_s, tok_r, line_s, line_r, exp_s, exp_r, s1, r1, s2, r2, g_s, g_r, c_s, c_r = refs[31:]
    me, beside, across = section_places()
    core, side = lax.rem(me, 2), lax.div(me, 2)
    w, length, a, b = line_of_wide()
    other = 1 - b
    mate = 2 * a + other
    diagonal = beside + across - me
    peers = [beside, across, diagonal]
    greet_line(peers, True)
    hid = o_first.shape[2]
    width = 4 * QUARTER
    sent, local_cuts = [], []

    def part_of(src, start, count):
        return src.at[:, pl.ds(pl.multiple_of(start, 128), count)]

    def cuts_for(p):
        got = [
            (0, part_of(qkv, j * width + p * QUARTER, QUARTER), st_qkv.at[me, :, pl.ds(j * QUARTER, QUARTER)])
            for j in range(3)
        ]
        return got + [(1, part_of(inn, p * hid, hid), st_in.at[me]), (2, vec, st_vec.at[me])]

    for k, p in enumerate(peers):
        for n, (i, src, dst) in enumerate(cuts_for(p)):
            c = push(src, dst, cut_s.at[n, k], cut_r.at[n, k], {"section": p})
            c.start()
            sent.append((i, c))
    for n, (i, src, dst) in enumerate(cuts_for(me)):
        c = pltpu.make_async_copy(src, dst, loc.at[11 + n])
        c.start()
        local_cuts.append((i, c))
    tok_c = [
        push(tok, o_tok.at[:, columns(me)], tok_s.at[k], tok_r.at[k], {"section": p})
        for k, p in enumerate((across, beside))
    ]
    for c in tok_c:
        c.start()
    own_tok = pltpu.make_async_copy(tok, o_tok.at[:, columns(me)], loc.at[3])
    own_tok.start()
    late = []
    exp_c = []
    for i, (src, dst) in enumerate(((first, o_first), (second, o_second))):
        c = pltpu.make_async_copy(part_of(src, me * hid, hid), dst.at[me], loc.at[4 + i])
        c.start()
        late.append(c)
        for k, p in enumerate((across, diagonal, beside)):
            c = push(part_of(src, p * hid, hid), dst.at[me], exp_s.at[i, k], exp_r.at[i, k], {"section": p})
            c.start()
            exp_c.append(c)

    lines = (
        (st_qkv, o_qkv, True),
        (outw, o_out, False),
        (st_in, o_in, True),
        (backw, o_back, False),
        (st_vec, o_vec, False),
    )
    staged = {0: 0, 2: 1, 4: 2}
    up, down, pair = 0, 1, 2

    def place(i, which):
        dst = lines[i][1]
        return dst.at[:, which] if i in staged else dst.at[which]

    def item(i, which, kind, to, own=False):
        spot = place(i, which)
        return push(lines[i][0] if own else spot, spot, line_s.at[kind, i, which], line_r.at[i, which], {"wide": to})

    def along(i, which, kind, own, act):
        if kind == pair:
            act(item(i, which, pair, mate, own))
            return

        @pl.when((a < length - 1) if kind == up else (a > 0))
        def _():
            act(item(i, which, kind, w + 2 if kind == up else w - 2, own))

    def start(c):
        c.start()

    def done(c):
        c.wait_send()

    def arrived(i, which):
        item(i, which, pair, mate).wait_recv()

    def own_item(i):
        if i in staged:
            for j, c in sent:
                if j == staged[i]:
                    c.wait_recv()
            for j, c in local_cuts:
                if j == staged[i]:
                    c.wait()
        for kind in (up, down, pair):
            along(i, w, kind, True, start)
        c = pltpu.make_async_copy(lines[i][0], place(i, w), loc.at[6 + i])
        c.start()
        return c

    def mate_item(i):
        if not lines[i][2]:
            arrived(i, mate)
            for kind in (up, down):
                along(i, mate, kind, False, start)

    def both_ways(t, what):
        for kind, there, ok in ((up, a - t, a - t >= 0), (down, a + t, a + t < length)):

            @pl.when(ok)
            def _():
                what(kind, there)

    def steps(group, begin, end):
        def step(t, carry):
            for i in group:

                def pass_on(kind, there):
                    arrived(i, 2 * there + b)
                    along(i, 2 * there + b, kind, False, start)
                    if lines[i][2]:
                        along(i, 2 * there + b, pair, False, start)
                    else:
                        arrived(i, 2 * there + other)
                        along(i, 2 * there + other, kind, False, start)

                both_ways(t, pass_on)
            return carry

        lax.fori_loop(begin, end, step, 0)

    def pair_items(i):
        if lines[i][2]:
            lax.fori_loop(0, length, lambda there, carry: (arrived(i, 2 * there + other), carry)[1], 0)

    def all_sent(i):
        for kind in (up, down, pair):
            along(i, w, kind, True, done)
        if not lines[i][2]:
            for kind in (up, down):
                along(i, mate, kind, False, done)

        def finish(t, carry):
            def one(kind, there):
                along(i, 2 * there + b, kind, False, done)
                if lines[i][2]:
                    along(i, 2 * there + b, pair, False, done)
                else:
                    along(i, 2 * there + other, kind, False, done)

            both_ways(t, one)
            return carry

        lax.fori_loop(1, length, finish, 0)

    early, later = (4, 0, 1), (2, 3)
    soon = [own_item(i) for i in early]
    tok_c[0].wait_recv()
    spot = o_tok.at[:, columns(across)]
    tok_fwd = push(spot, spot, tok_s.at[2], tok_r.at[2], {"section": beside})
    tok_fwd.start()
    for i in early:
        mate_item(i)
    steps(early, 1, 2)
    late += [own_item(i) for i in later]
    steps(early, 2, length)

    def cot_place(which, block):
        return o_cot.at[block, :, columns(which)]

    def cot_wide(to, frm):
        return push(cot.at[to], cot_place(me, frm), c_s.at[0, to], c_r.at[0, frm], {"wide": to})

    def cot_spread(kind, block, to):
        here = cot_place(across if kind == 3 else me, block)
        return push(here, here, c_s.at[kind, block], c_r.at[kind, block], {"section": to})

    for j in range(1, 2 * length):
        cot_wide(lax.rem(w + j, 2 * length), w).start()
    o_cot[w, :, columns(me)] = cot[w]
    for i in later:
        mate_item(i)
    for i in early:
        pair_items(i)
    for c in soon:
        c.wait()
    own_tok.wait()
    tok_c[1].wait_recv()
    tok_fwd.wait_recv()

    wide = 2 * length
    small = qkv.shape[0]
    per = 128 // small
    for p in range(4):
        for g in range(wide // per):
            total = o_vec[p, g * per, 6:7]
            for j in range(1, per):
                total = total + o_vec[p, g * per + j, 6:7]
            gain[:, pl.ds((p * (wide // per) + g) * 128, 128)] = total
    micro, rows = mask.shape[:2]
    count = micro * rows
    chunk = 128
    chunks = count // chunk

    def project(k, carry):
        at = pl.ds(pl.multiple_of(k * chunk, chunk), chunk)
        unit, _ = row_norm(o_tok[at].astype(F32))
        o_n1[at] = (unit * gain[...]).astype(BF16)
        total = jnp.zeros((chunk, 3 * QUARTER), F32)
        for p in range(4):
            total = total + dot(o_n1[at, pl.ds(p * QUARTER, QUARTER)], o_qkv[p].reshape(QUARTER, 3 * QUARTER))
        o_act[at] = total.astype(BF16)
        return carry

    lax.fori_loop(0, chunks, project, 0)
    cuts = [1 + k * (length - 1) // 3 for k in range(4)]
    beside_core = 1 - core
    sends, crossing, spread = [], [], []
    for m in range(micro):
        at = pl.ds(m * rows, rows)
        for n in range(2):
            heads = attention_pair(n, lambda c: o_act[at, pl.ds(c, 128)], mask[m])
            got = [dot(probs.astype(BF16), v) for _, _, v, probs in heads]
            o_mixed[at, pl.ds(n * 128, 128)] = jnp.concatenate(got, axis=1).astype(BF16)
        for k in range(m * rows // chunk, (m + 1) * rows // chunk):
            at = pl.ds(k * chunk, chunk)
            part[at] = dot(o_mixed[at], o_out[...].reshape(QUARTER, width)).astype(BF16)
            for which, half in ((1, 1 - side), (0, side)):
                c = push(
                    part.at[at, columns(2 * half + beside_core)],
                    near_in.at[which, at],
                    s1.at[which, k],
                    r1.at[which, k],
                    {"section": beside},
                )
                c.start()
                sends.append(c)
        steps(later, cuts[m], cuts[m + 1])
    for k in range(chunks):
        at = pl.ds(k * chunk, chunk)
        sends[2 * k].wait()
        far[at] = (part[at, columns(2 * (1 - side) + core)].astype(F32) + near_in[1, at].astype(F32)).astype(BF16)
        c = push(far.at[at], far_in.at[at], s2.at[k], r2.at[k], {"section": across})
        c.start()
        crossing.append(c)
    for k in range(chunks):
        at = pl.ds(k * chunk, chunk)
        sends[2 * k + 1].wait()
        near = part[at, columns(me)].astype(F32) + near_in[0, at].astype(F32)
        crossing[k].wait()
        o_att[at, columns(me)] = (o_tok[at, columns(me)].astype(F32) + (near + far_in[at].astype(F32))).astype(BF16)
        here = o_att.at[at, columns(me)]
        for kind, to in ((0, across), (1, beside)):
            c = push(here, here, g_s.at[kind, k], g_r.at[kind, k], {"section": to})
            c.start()
            spread.append(c)
    steps(later, cuts[micro], cuts[3])
    for j in range(wide):
        block = lax.rem(w + j, wide)
        if j:
            cot_wide(block, block).wait_recv()
        cot_spread(1, block, across).start()
        cot_spread(2, block, beside).start()
    for k in range(chunks):
        spread[2 * k].wait()
        here = o_att.at[pl.ds(k * chunk, chunk), columns(across)]
        c = push(here, here, g_s.at[2, k], g_r.at[2, k], {"section": beside})
        c.start()
        spread.append(c)
    for j in range(wide):
        block = lax.rem(w + j, wide)
        cot_spread(1, block, across).wait_recv()
        cot_spread(3, block, beside).start()
    for i in later:
        pair_items(i)
    for j in range(wide):
        block = lax.rem(w + j, wide)
        cot_spread(1, block, across).wait_send()
        cot_spread(2, block, beside).wait()
        cot_spread(3, block, beside).wait()
        if j:
            cot_wide(block, w).wait_send()
    for k in range(chunks):
        spread[2 * k + 1].wait()
        spread[2 * chunks + k].wait()
    for i in early + later:
        all_sent(i)
    for _, c in sent:
        c.wait_send()
    for c in tok_c + [tok_fwd]:
        c.wait_send()
    for c in exp_c + late:
        c.wait()


def head_call(qkv, inn, vec, outw, backw, first, second, tok, mask, cot, collective_id):
    wide = cot.shape[0]
    small = qkv.shape[0]
    hid = inn.shape[1] // 4
    cut = 3 * QUARTER
    count = tok.shape[0]
    width = 4 * QUARTER
    chunks = count // 128
    outs = [
        ((4, wide, small, cut), BF16),
        ((4, wide, small, hid), BF16),
        ((4, wide, *vec.shape), F32),
        ((wide, *outw.shape), BF16),
        ((wide, *backw.shape), BF16),
        ((4, first.shape[0], hid), BF16),
        ((4, first.shape[0], hid), BF16),
        ((count, width), BF16),
        ((count, width), BF16),
        ((count, cut), BF16),
        ((count, QUARTER), BF16),
        ((count, width), BF16),
        ((*cot.shape[:2], width), BF16),
    ]
    return call(
        head_kernel,
        tuple(jax.ShapeDtypeStruct(*o) for o in outs),
        [ANY] * 8 + [VM, VM],
        (VM, ANY, VM, VM, ANY, ANY, ANY, VM, VM, VM, VM, VM, VM),
        [
            pltpu.VMEM((4, small, cut), BF16),
            pltpu.VMEM((4, small, hid), BF16),
            pltpu.VMEM((4, *vec.shape), F32),
            pltpu.VMEM((1, width), F32),
            pltpu.VMEM((count, width), BF16),
            pltpu.VMEM((2, count, QUARTER), BF16),
            pltpu.VMEM((count, QUARTER), BF16),
            pltpu.VMEM((count, QUARTER), BF16),
            DMA((16,)),
            DMA((5, 3)),
            DMA((5, 3)),
            DMA((3,)),
            DMA((3,)),
            DMA((3, 5, wide)),
            DMA((5, wide)),
            DMA((2, 3)),
            DMA((2, 3)),
            DMA((2, chunks)),
            DMA((2, chunks)),
            DMA((chunks,)),
            DMA((chunks,)),
            DMA((3, chunks)),
            DMA((3, chunks)),
            DMA((4, wide)),
            DMA((4, wide)),
        ],
        collective_id,
        *(qkv, inn, vec, outw, backw, first, second, tok, mask, cot),
    )


def dot(left, right):
    return jnp.dot(left, right, preferred_element_type=F32)


def dot_nt(left, right):
    return lax.dot_general(left, right, (((1,), (1,)), ((), ())), preferred_element_type=F32)


def dot_tn(left, right):
    return lax.dot_general(left, right, (((0,), (0,)), ((), ())), preferred_element_type=F32)


def gelu_value(v):
    return 0.5 * v * (1.0 + lax.erf(v * 0.7071067811865476))


def gelu_slope(v):
    return (
        0.5 * (1.0 + lax.erf(v * 0.7071067811865476))
        + v * jnp.exp(-0.5 * v * v) * 0.3989422804014327
    )


def unit_norm(v):
    centred = v - jnp.mean(v, axis=-1, keepdims=True)
    scale = lax.rsqrt(jnp.mean(centred * centred, axis=-1, keepdims=True) + 1e-05)
    return centred * scale, scale


IDS = {}


def id_of(*key):
    return IDS.setdefault(key, len(IDS))


def reduce_quarters(part, stats=None):
    return reduce_call(part.astype(BF16), stats, id_of("reduce", part.shape, stats is None))


def gather_quarters(quarter):
    return gather_call(quarter, id_of("gather", quarter.shape))


def wide_exchange(slots, spread):
    return exchange_call(slots, spread, id_of("exchange", spread))


def allowed_of(lengths, rows):
    pos = jnp.arange(rows, dtype=jnp.int32)
    group = pos[None] // lengths[:, None]
    return ((pos[:, None] >= pos[None, :])[None] & (group[:, :, None] == group[:, None, :])).astype(F32)


def body(
    tokens_in,
    cotangent,
    routes,
    seq_lengths,
    qkv_weight,
    out_weight,
    attn_gain,
    ffn_in,
    ffn_back,
    ffn_gain,
    centroids,
    first_gain,
    first_in,
    first_back,
    second_gain,
    second_in,
    second_back,
):
    sections = lax.axis_size("section")
    wide = lax.axis_size("wide")
    section_id = lax.axis_index("section")
    wide_id = lax.axis_index("wide")
    micro, rows, quarter = tokens_in.shape
    width = quarter * sections
    cap = 5 * rows // (4 * wide)
    tok_rows = micro * rows
    hid = first_back.shape[1]
    small = qkv_weight.shape[0]
    qkv_cols = qkv_weight.shape[1] // sections

    experts = jnp.arange(wide, dtype=jnp.int32)
    choose = (routes == experts).astype(jnp.int32)
    upto = (jnp.arange(rows)[:, None] >= jnp.arange(rows)[None, :]).astype(BF16)
    ranking = jnp.einsum("rk,mke->mre", upto, choose.astype(BF16), preferred_element_type=F32).astype(jnp.int32) - 1
    slot_of = routes[:, :, 0] * cap + jnp.sum(ranking * choose, axis=2)
    onehot = (jnp.arange(wide * cap, dtype=jnp.int32)[None, :, None] == slot_of[:, None, :]).astype(BF16)

    def to_slots(rows_q):
        packed = jnp.einsum("msr,mrd->msd", onehot, rows_q.reshape(micro, rows, quarter), preferred_element_type=F32)
        packed = packed.astype(BF16).reshape(micro, wide, cap, quarter).transpose(1, 0, 2, 3)
        return packed.reshape(wide, micro * cap, quarter)

    def to_experts(rows_q):
        return wide_exchange(to_slots(rows_q), True).reshape(wide * micro * cap, width)

    def from_slots(back):
        back = back.reshape(wide, micro, cap, quarter).transpose(1, 0, 2, 3).reshape(micro, wide * cap, quarter)
        got = jnp.einsum("msr,msd->mrd", onehot, back, preferred_element_type=F32)
        return got.astype(BF16).reshape(tok_rows, quarter)

    def to_tokens(slots_q):
        return from_slots(wide_exchange(slots_q.reshape(wide, micro * cap, quarter), False))

    per = 128 // small
    spread = lambda v: lax.dynamic_update_slice_in_dim(
        jnp.zeros((1, 128), F32), v.astype(F32)[None], lax.rem(wide_id, per) * small, 1
    )
    vectors = [v.astype(F32).reshape(2, 128) for v in (first_gain, second_gain, centroids)]
    vectors = jnp.concatenate(vectors + [spread(attn_gain), spread(ffn_gain)], axis=0)
    allowed = allowed_of(seq_lengths, rows)
    tokens_q = tokens_in.reshape(tok_rows, quarter)

    (qkv_w, in_w, vectors, out_w, back_w, first_w, second_w, tokens, normed_a, packed, mixed, attended, d_mixed) = head_call(
        qkv_weight,
        ffn_in,
        vectors,
        out_weight,
        ffn_back,
        first_in[0],
        second_in[0],
        tokens_q,
        allowed,
        to_slots(cotangent.reshape(tok_rows, quarter)),
        id_of("head"),
    )
    qkv_w = qkv_w.reshape(width, qkv_cols)
    in_w = in_w.reshape(width, hid)
    out_w = out_w.reshape(quarter, width)
    back_w = back_w.reshape(hid, width)
    first_w = first_w.reshape(width, hid)
    second_w = second_w.reshape(width, hid)
    own = lax.dynamic_index_in_dim(vectors, wide_id, axis=1, keepdims=False)
    gain_first, gain_second, centre = (own[:, 2 * j : 2 * j + 2].reshape(1, width) for j in range(3))
    gain_attn, gain_ffn = (
        jnp.sum(vectors[:, :, j].reshape(sections, wide // per, per, 128), axis=2).reshape(1, width) for j in (6, 7)
    )
    own_quarter = lambda v: lax.dynamic_slice_in_dim(v, section_id * quarter, quarter, axis=1)
    first_b = first_back[0]
    second_b = second_back[0]

    attended_q = own_quarter(attended)

    def branch(v, w_in, w_back, gain):
        unit, scale = unit_norm(v.astype(F32))
        normed = (unit * gain).astype(BF16)
        pre = dot(normed, w_in)
        hidden = gelu_value(pre).astype(BF16)
        return (normed, unit, scale, pre, hidden), dot(hidden, w_back)

    def branch_back(grad, saved, w_in, w_back, gain, more=None):
        normed, unit, scale, pre, hidden = saved
        d_back = dot_tn(hidden, grad)
        d_pre = (dot_nt(grad, w_back) * gelu_slope(pre)).astype(BF16)
        d_in = dot_tn(normed, d_pre)
        return d_in, d_back, norm_back(dot_nt(d_pre, w_in), unit, scale, gain, more)

    def norm_back(d_part, unit, scale, gain, more=None):
        d_unit = d_part * gain
        sums = jnp.stack([jnp.sum(d_unit, axis=1), jnp.sum(d_unit * unit, axis=1)])
        if more is not None:
            sums = jnp.concatenate([sums, more])
        d_q, sums = reduce_quarters(d_part, jnp.pad(sums, ((0, 8 - sums.shape[0]), (0, 0))))
        extra, sums = sums[2], sums / width
        unit_q = own_quarter(unit)
        d_rows = scale * (d_q * own_quarter(gain) - sums[0][:, None] - unit_q * sums[1][:, None])
        return d_rows, jnp.sum(d_q * unit_q, axis=0), extra

    saved_d, part = branch(attended, in_w, back_w, gain_ffn)
    fed_q = (attended_q.astype(F32) + reduce_quarters(part)).astype(BF16)
    routed = to_experts(fed_q)
    routed_q = own_quarter(routed)
    d_mixed = d_mixed.reshape(wide * micro * cap, width).astype(F32)
    d_mixed_q = own_quarter(d_mixed)
    saved_1, part = branch(routed, first_w, first_b, gain_first)
    first_q = (routed_q.astype(F32) + reduce_quarters(part)).astype(BF16)
    first = gather_quarters(first_q)
    saved_2, part = branch(first, second_w, second_b, gain_second)
    gate = jax.nn.sigmoid(jnp.sum(routed.astype(F32) * centre, axis=-1, keepdims=True))
    second_q = first_q.astype(F32) + reduce_quarters(part)
    mixed_q = routed_q.astype(F32) + gate * second_q

    d_second = gate * d_mixed
    d_second_q = gate * d_mixed_q
    d_second_in, d_second_back, (norm_q, second_gain_grad, d_logit) = branch_back(
        d_second.astype(BF16), saved_2, second_w, second_b, gain_second, jnp.sum(d_mixed_q * second_q, axis=-1)[None]
    )
    d_logit = d_logit[:, None] * gate * (1.0 - gate)
    centroids_grad = jnp.sum(d_logit * routed_q.astype(F32), axis=0)[None]
    d_gated_q = (d_mixed_q + d_logit * own_quarter(centre)).astype(BF16)
    d_first_q = (d_second_q + norm_q).astype(BF16)
    d_first_in, d_first_back, (norm_q, first_gain_grad, _) = branch_back(
        gather_quarters(d_first_q), saved_1, first_w, first_b, gain_first
    )
    d_routed_q = (d_first_q.astype(F32) + norm_q + d_gated_q.astype(F32)).astype(BF16)
    d_fed_q = to_tokens(d_routed_q)
    d_in, d_back, (norm_q, d_gain_ffn, _) = branch_back(gather_quarters(d_fed_q), saved_d, in_w, back_w, gain_ffn)
    d_attended_q = (d_fed_q.astype(F32) + norm_q).astype(BF16)
    d_attended = gather_quarters(d_attended_q)
    def by_row(grad):
        return grad.astype(BF16).reshape(sections, wide, small, grad.shape[1])

    qkv_grad, ffn_in_grad, out_grad, ffn_back_grad, d_gains, d_first_in, d_second_in, tokens_grad, result = tail_call(
        by_row(d_in),
        d_back.astype(BF16).reshape(wide, hid // wide, width),
        d_first_in.astype(BF16).reshape(sections, quarter, hid),
        d_second_in.astype(BF16).reshape(sections, quarter, hid),
        d_attended,
        tokens,
        normed_a,
        packed,
        mixed,
        qkv_w,
        out_w,
        allowed,
        gain_attn,
        d_gain_ffn[None],
        mixed_q.astype(BF16).reshape(wide, micro * cap, quarter),
        id_of("tail"),
    )
    block_out = from_slots(result).reshape(micro, rows, quarter)
    d_gains = lax.dynamic_slice_in_dim(d_gains, wide_id * small, small, axis=1)
    tokens_grad = tokens_grad.reshape(micro, rows, quarter)
    return (
        block_out,
        tokens_grad,
        qkv_grad.astype(F32),
        out_grad,
        d_gains[0],
        ffn_in_grad.astype(F32),
        ffn_back_grad,
        d_gains[1],
        centroids_grad,
        first_gain_grad[None],
        d_first_in[None].astype(F32),
        d_first_back[None],
        second_gain_grad[None],
        d_second_in[None].astype(F32),
        d_second_back[None],
    )


def solution(mesh):
    dense = P(("section", "wide"), None)
    dense_gain = P(("section", "wide"))
    tokens = P(None, "wide", "section")
    gain = P("wide", "section")
    expert = P("wide", "section", None)
    in_specs = (
        (tokens, tokens, P(None, "wide", None), P(), dense, dense, dense_gain, dense, dense, dense_gain)
        + (gain, gain, expert, expert, gain, expert, expert)
    )
    out_specs = (
        (tokens, tokens, dense, dense, dense_gain, dense, dense, dense_gain)
        + (gain, gain, expert, expert, gain, expert, expert)
    )
    return jax.shard_map(body, mesh=mesh, in_specs=in_specs, out_specs=out_specs, check_vma=False)
```

```python
import functools

import jax
import jax.numpy as jnp
from jax import lax
from jax.experimental import pallas as pl
from jax.experimental.pallas import tpu as pltpu
from jax.sharding import PartitionSpec as P

HEAD_SIZE = 64
F32 = jnp.float32
BF16 = jnp.bfloat16

MESH = pl.DeviceIdType.MESH
ANY = pl.BlockSpec(memory_space=pl.ANY)
VM = pl.BlockSpec(memory_space=pltpu.VMEM)
DMA = pltpu.SemaphoreType.DMA
VMEM_BYTES = 60 * 1024 * 1024
QUARTER = 256


def section_places():
    me = lax.axis_index("section")
    return me, me + 1 - 2 * lax.rem(me, 2), me + 2 - 4 * lax.div(me, 2)


def greet(peers):
    barrier = pltpu.get_barrier_semaphore()
    for peer in peers:
        pl.semaphore_signal(barrier, inc=1, device_id=peer, device_id_type=MESH)
    pl.semaphore_wait(barrier, len(peers))


def push(src, dst, send, recv, peer):
    return pltpu.make_async_remote_copy(
        src_ref=src, dst_ref=dst, send_sem=send, recv_sem=recv, device_id=peer, device_id_type=MESH
    )


def columns(which):
    return pl.ds(pl.multiple_of(which * QUARTER, QUARTER), QUARTER)


def call(kernel, out_shape, in_specs, out_specs, scratch, collective_id, *operands):
    return pl.pallas_call(
        kernel,
        out_shape=out_shape,
        in_specs=in_specs,
        out_specs=out_specs,
        scratch_shapes=scratch,
        compiler_params=pltpu.CompilerParams(
            collective_id=collective_id, has_side_effects=True, vmem_limit_bytes=VMEM_BYTES
        ),
    )(*operands)


def reduce_kernel(chunks, with_stats, *refs):
    if with_stats:
        part, stats, out, stats_out = refs[:4]
        first_in, far, far_in, s1, r1, s2, r2, st_in, st_mid, st_far, st_s, st_r = refs[4:]
    else:
        part, out, first_in, far, far_in, s1, r1, s2, r2 = refs
    me, beside, across = section_places()
    core, side = lax.rem(me, 2), lax.div(me, 2)
    greet([{"section": beside}, {"section": across}])
    rows = part.shape[0] // chunks
    beside_core = 1 - core
    sends = []
    if with_stats:
        st = push(stats, st_in, st_s.at[0], st_r.at[0], {"section": beside})
        st.start()
    for k in range(chunks):
        for which, half in ((1, 1 - side), (0, side)):
            at = pl.ds(k * rows, rows)
            c = push(
                part.at[at, columns(2 * half + beside_core)],
                first_in.at[which, at],
                s1.at[which, k],
                r1.at[which, k],
                {"section": beside},
            )
            c.start()
            sends.append(c)
    if with_stats:
        st.wait()
        st_mid[...] = stats[...] + st_in[...]
        st2 = push(st_mid, st_far, st_s.at[1], st_r.at[1], {"section": across})
        st2.start()
    crossing = []
    for k in range(chunks):
        at = pl.ds(k * rows, rows)
        sends[2 * k].wait()
        far[at] = (part[at, columns(2 * (1 - side) + core)].astype(F32) + first_in[1, at].astype(F32)).astype(BF16)
        c = push(far.at[at], far_in.at[at], s2.at[k], r2.at[k], {"section": across})
        c.start()
        crossing.append(c)
    for k in range(chunks):
        at = pl.ds(k * rows, rows)
        sends[2 * k + 1].wait()
        near = part[at, columns(me)].astype(F32) + first_in[0, at].astype(F32)
        crossing[k].wait()
        out[at] = near + far_in[at].astype(F32)
    if with_stats:
        st2.wait()
        stats_out[...] = st_mid[...] + st_far[...]


def reduce_call(part, stats, collective_id, chunks=4):
    rows, _ = part.shape
    scratch = [
        pltpu.VMEM((2, rows, QUARTER), BF16),
        pltpu.VMEM((rows, QUARTER), BF16),
        pltpu.VMEM((rows, QUARTER), BF16),
        DMA((2, chunks)),
        DMA((2, chunks)),
        DMA((chunks,)),
        DMA((chunks,)),
    ]
    out = jax.ShapeDtypeStruct((rows, QUARTER), F32)
    if stats is None:
        return call(
            functools.partial(reduce_kernel, chunks, False), out, [VM], VM, scratch, collective_id, part
        )
    st = pltpu.VMEM(stats.shape, F32)
    return call(
        functools.partial(reduce_kernel, chunks, True),
        (out, jax.ShapeDtypeStruct(stats.shape, F32)),
        [VM, VM],
        (VM, VM),
        scratch + [st, st, st, DMA((2,)), DMA((2,))],
        collective_id,
        part,
        stats,
    )


def gather_kernel(chunks, q, out, s, r):
    me, beside, across = section_places()
    greet([{"section": beside}, {"section": across}])
    rows = q.shape[0] // chunks
    copies = []
    for k in range(chunks):
        at = pl.ds(k * rows, rows)
        for kind, to in ((0, across), (1, beside)):
            c = push(q.at[at], out.at[at, columns(me)], s.at[kind, k], r.at[kind, k], {"section": to})
            c.start()
            copies.append(c)
    out[:, columns(me)] = q[...]
    for k in range(chunks):
        at = pl.ds(k * rows, rows)
        copies[2 * k].wait()
        here = out.at[at, columns(across)]
        c = push(here, here, s.at[2, k], r.at[2, k], {"section": beside})
        c.start()
        copies.append(c)
    for k in range(chunks):
        copies[2 * k + 1].wait()
        copies[2 * chunks + k].wait()


def gather_call(q, collective_id, chunks=4):
    rows = q.shape[0]
    return call(
        functools.partial(gather_kernel, chunks),
        jax.ShapeDtypeStruct((rows, 4 * QUARTER), BF16),
        [VM],
        VM,
        [DMA((3, chunks)), DMA((3, chunks))],
        collective_id,
        q,
    )


def exchange_kernel(spread, src, out, s, r):
    me, beside, across = section_places()
    w = lax.axis_index("wide")
    count = src.shape[0]
    peers = [{"wide": lax.rem(w + j, count)} for j in range(1, count)]
    greet(peers + ([{"section": beside}, {"section": across}] if spread else []))

    def place(which, block):
        return out.at[block, :, columns(which)] if spread else out.at[block]

    def wide_copy(to):
        return push(src.at[to], place(me, w), s.at[0, to], r.at[0, w], {"wide": to})

    def arrival(frm):
        return push(src.at[frm], place(me, frm), s.at[0, frm], r.at[0, frm], {"wide": frm})

    def spread_copy(kind, block, to):
        here = place(across, block) if kind == 3 else place(me, block)
        return push(here, here, s.at[kind, block], r.at[kind, block], {"section": to})

    for j in range(1, count):
        wide_copy(lax.rem(w + j, count)).start()
    if spread:
        out[w, :, columns(me)] = src[w]
    else:
        out[w] = src[w]
    for j in range(count):
        block = lax.rem(w + j, count)
        if j:
            arrival(block).wait_recv()
        if spread:
            spread_copy(1, block, across).start()
            spread_copy(2, block, beside).start()
    if spread:
        for j in range(count):
            block = lax.rem(w + j, count)
            spread_copy(1, block, across).wait_recv()
            spread_copy(3, block, beside).start()
        for j in range(count):
            block = lax.rem(w + j, count)
            spread_copy(1, block, across).wait_send()
            spread_copy(2, block, beside).wait()
            spread_copy(3, block, beside).wait()
    for j in range(1, count):
        wide_copy(lax.rem(w + j, count)).wait_send()


def exchange_call(slots, spread, collective_id):
    count, n, quarter = slots.shape
    return call(
        functools.partial(exchange_kernel, spread),
        jax.ShapeDtypeStruct((count, n, 4 * quarter if spread else quarter), BF16),
        [VM],
        VM,
        [DMA((4, count)), DMA((4, count))],
        collective_id,
        slots,
    )


GROUP = 32


def add_rows(dst, left, right):
    if len(dst.shape) == 3:
        for j in range(dst.shape[0]):
            add_rows(dst.at[j], left.at[j], right.at[j])
        return
    rows = dst.shape[0]
    step = min(rows, GROUP)

    def one(j, carry):
        at = pl.ds(pl.multiple_of(j * step, step), step)
        dst[at] = (left[at].astype(F32) + right[at].astype(F32)).astype(dst.dtype)
        return carry

    lax.fori_loop(0, rows // step, one, 0)


def attention_pair(pair, qkv, mask):
    q2, k2, v2 = (qkv(j * QUARTER + pair * 128) for j in range(3))
    got = []
    for h in range(2):
        q, k, v = (x[:, h * HEAD_SIZE : (h + 1) * HEAD_SIZE] for x in (q2, k2, v2))
        scores = jnp.where(mask > 0.0, dot_nt(q, k) * HEAD_SIZE ** (-0.5), -1e30)
        expo = jnp.exp(scores - jnp.max(scores, axis=-1, keepdims=True))
        got.append((q, k, v, expo / jnp.sum(expo, axis=-1, keepdims=True)))
    return got


def row_norm(v):
    centred = v - jnp.mean(v, axis=-1, keepdims=True)
    scale = lax.rsqrt(jnp.mean(centred * centred, axis=-1, keepdims=True) + 1e-05)
    return centred * scale, scale


def line_of_wide():
    w = lax.axis_index("wide")
    length = lax.axis_size("wide") // 2
    return w, length, lax.div(w, 2), lax.rem(w, 2)


def greet_line(section_peers, all_wide):
    w, length, a, b = line_of_wide()
    barrier = pltpu.get_barrier_semaphore()
    for p in section_peers:
        pl.semaphore_signal(barrier, inc=1, device_id={"section": p}, device_id_type=MESH)
    if all_wide:
        for j in range(1, 2 * length):
            pl.semaphore_signal(
                barrier, inc=1, device_id={"wide": lax.rem(w + j, 2 * length)}, device_id_type=MESH
            )
        pl.semaphore_wait(barrier, len(section_peers) + 2 * length - 1)
        return
    pl.semaphore_signal(barrier, inc=1, device_id={"wide": 2 * a + 1 - b}, device_id_type=MESH)

    @pl.when(a > 0)
    def _():
        pl.semaphore_signal(barrier, inc=1, device_id={"wide": w - 2}, device_id_type=MESH)

    @pl.when(a < length - 1)
    def _():
        pl.semaphore_signal(barrier, inc=1, device_id={"wide": w + 2}, device_id_type=MESH)

    pl.semaphore_wait(barrier, len(section_peers) + 1 + jnp.minimum(a, 1) + jnp.minimum(length - 1 - a, 1))


def tail_kernel(*refs):
    (g_in, g_back, first, second, d_att, tok, n1, qkv, mixed, w_qkv, w_out, mask, gain, gain_d, res) = refs[:15]
    o_qkv, o_in, o_out, o_back, o_gain, o_first, o_second, o_tok, o_res = refs[15:24]
    g_qkv, g_out = refs[24:26]
    acc = refs[26:30]
    line_in = refs[30:34]
    pair_in = refs[34:38]
    (d_mix, d_qkv, part, unit, scales, stats, stats_in, stats_mid, stats_far, near_in, far, far_in, gains, gains_in) = refs[38:52]
    (loc, exp_s, exp_r, cut_s, cut_r, pair_s, pair_r, line_s, line_r, s1, r1, s2, r2, st_s, st_r, gn_s, gn_r, o_s, o_r) = refs[52:]
    src = (g_qkv, g_in, g_out, g_back)
    pair_first = (True, True, False, False)
    me, beside, across = section_places()
    diagonal = beside + across - me
    core, side = lax.rem(me, 2), lax.div(me, 2)
    w, length, a, b = line_of_wide()
    other = 1 - b
    mate = {"wide": 2 * a + other}
    peers = [beside, across, diagonal]
    greet_line(peers, True)
    hid = first.shape[2]
    rows = mask.shape[1]
    micro = mask.shape[0]
    late = []

    def spot(ref, which, count):
        return ref.at[:, pl.ds(pl.multiple_of(which * count, count), count)]

    def pair_copy(i, there):
        return push(
            src[i].at[:, 2 * there + other], pair_in[i].at[there], pair_s.at[i, there], pair_r.at[i, there], mate
        )

    def slots(i, there):
        if pair_first[i]:
            return [(there, 2 * there + b)]
        return [(2 * there, 2 * there), (2 * there + 1, 2 * there + 1)]

    def line_copy(i, block, to_block, to):
        return push(acc[i].at[block], line_in[i].at[to_block], line_s.at[i, block], line_r.at[i, to_block], {"wide": to})

    def ready(i, there, block, own):
        if pair_first[i]:
            pair_copy(i, there).wait_recv()
            add_rows(acc[i].at[block], src[i].at[:, own], pair_in[i].at[there])
        else:
            acc[i][block] = src[i][own]

    def flow(i, there, from_edge, to):
        n = 1 if pair_first[i] else 2
        for j, (block, own) in enumerate(slots(i, there)):
            ready(i, there, block, own)

            @pl.when(from_edge)
            def _():
                line_copy(i, block, block, w).wait_recv()
                add_rows(acc[i].at[block], acc[i].at[block], line_in[i].at[block])

            if to == "down":
                line_copy(i, block, block, w - 2).start()
            else:
                target = jnp.where(there == a + 1, n * length + j, block)
                line_copy(i, block, target, w + 2).start()

    def pairs(i):
        lax.fori_loop(0, length, lambda t, c: (pair_copy(i, t).start(), c)[1], 0)

    def steps(group, start, stop):
        def step(t, carry):
            high = length - 1 - t
            for i in group:

                @pl.when(t < a)
                def _():
                    flow(i, t, a < length - 1, "down")

                @pl.when(high > a)
                def _():
                    flow(i, high, a > 0, "up")

            return carry

        lax.fori_loop(start, stop, step, 0)

    finals = {}

    def own_block(i):
        n = 1 if pair_first[i] else 2
        for j, (block, own) in enumerate(slots(i, a)):
            ready(i, a, block, own)

            @pl.when(a < length - 1)
            def _():
                line_copy(i, block, block, w).wait_recv()
                add_rows(acc[i].at[block], acc[i].at[block], line_in[i].at[block])

            @pl.when(a > 0)
            def _():
                line_copy(i, block, n * length + j, w).wait_recv()
                add_rows(acc[i].at[block], acc[i].at[block], line_in[i].at[n * length + j])

        if not pair_first[i]:
            c = push(acc[i].at[2 * a + other], pair_in[i].at[0], pair_s.at[i, 0], pair_r.at[i, 0], mate)
            c.start()
            finals[i] = c
            return
        block = acc[i].at[a]

        def cut(p):
            if i == 1:
                return [(block.at[p], spot(o_in, me, hid))]
            third = [pl.ds(j * QUARTER, QUARTER) for j in range(3)]
            return [(block.at[p, :, third[j]], spot(o_qkv, 4 * j + me, QUARTER)) for j in range(3)]

        for k, p in enumerate(peers):
            for j, (here, there) in enumerate(cut(p)):
                n = 3 * i + j
                c = push(here, there, cut_s.at[n, k], cut_r.at[n, k], {"section": p})
                c.start()
                late.append(c)
        for j, (here, there) in enumerate(cut(me)):
            c = pltpu.make_async_copy(here, there, loc.at[2 + 3 * i + j])
            c.start()
            late.append(c)

    pairs(1)
    for i, (s, d) in enumerate(((first, o_first), (second, o_second))):
        c = pltpu.make_async_copy(s.at[me], spot(d, me, hid), loc.at[i])
        c.start()
        late.append(c)
        for k, p in enumerate((across, diagonal, beside)):
            c = push(s.at[p], spot(d, me, hid), exp_s.at[i, k], exp_r.at[i, k], {"section": p})
            c.start()
            late.append(c)
    def res_copy(to, frm):
        return push(res.at[to], o_res.at[frm], o_s.at[to], o_r.at[frm], {"wide": to})

    for j in range(1, 2 * length):
        res_copy(lax.rem(w + j, 2 * length), w).start()
    o_res[w] = res[w]
    group = (3, 1)
    cuts = [k * length // 4 for k in range(5)]
    small = g_out.shape[1]
    wide = 2 * length

    def store_blocks(ref, index, value):
        for j in range(wide):
            piece = value[j * small : (j + 1) * small].astype(BF16)
            if index is None:
                ref[j] = piece
            else:
                ref[index, j] = piece

    for m in range(micro):
        at = pl.ds(m * rows, rows)
        d_mix[at] = dot_nt(d_att[at], w_out[...]).astype(BF16)
    store_blocks(g_out, None, dot_tn(mixed[...], d_att[...]))
    steps(group, cuts[0], cuts[1])

    def micro_back(m, carry):
        at = pl.ds(pl.multiple_of(m * rows, rows), rows)
        for pair in range(2):
            heads = attention_pair(pair, lambda c: qkv[at, pl.ds(c, 128)], mask[m])
            d_pair = d_mix[at, pl.ds(pair * 128, 128)]
            grads = []
            for h, (q, k, v, probs) in enumerate(heads):
                d_out = d_pair[:, h * HEAD_SIZE : (h + 1) * HEAD_SIZE]
                d_probs = dot_nt(d_out, v)
                delta = jnp.sum(probs * d_probs, axis=-1, keepdims=True)
                d_scores = (probs * (d_probs - delta) * HEAD_SIZE ** (-0.5)).astype(BF16)
                grads.append((dot(d_scores, k), dot_tn(d_scores, q), dot_tn(probs.astype(BF16), d_out)))
            for j in range(3):
                both = jnp.concatenate([grads[0][j], grads[1][j]], axis=1).astype(BF16)
                d_qkv[at, pl.ds(j * QUARTER + pair * 128, 128)] = both
        return carry

    for m in range(micro):
        micro_back(m, 0)
        steps(group, cuts[1 + m], cuts[2 + m])
    for p in range(4):
        store_blocks(g_qkv, p, dot_tn(n1[:, pl.ds(p * QUARTER, QUARTER)], d_qkv[...]))
    pairs(0)
    steps((2,), 0, length)

    count = d_att.shape[0]
    chunk = 128
    chunks = count // chunk
    lane = lax.broadcasted_iota(jnp.int32, (chunk, 128), 1)
    beside_core = 1 - core
    sends = []
    for k in range(chunks):
        at = pl.ds(k * chunk, chunk)
        u, scale = row_norm(tok[at].astype(F32))
        unit[at] = u
        scales[at] = jnp.broadcast_to(scale, (chunk, 128))
        d_normed = dot_nt(d_qkv[at], w_qkv[...])
        part[at] = d_normed.astype(BF16)
        d_unit = d_normed * gain[...]
        sum_a = jnp.sum(d_unit, axis=-1, keepdims=True)
        sum_b = jnp.sum(d_unit * u, axis=-1, keepdims=True)
        both = jnp.where(lane == 0, sum_a, jnp.where(lane == 1, sum_b, 0.0))
        stats[:, at] = both.T[:8]
        for which, half in ((1, 1 - side), (0, side)):
            c = push(
                part.at[at, columns(2 * half + beside_core)],
                near_in.at[which, at],
                s1.at[which, k],
                r1.at[which, k],
                {"section": beside},
            )
            c.start()
            sends.append(c)
    st1 = push(stats, stats_in, st_s.at[0], st_r.at[0], {"section": beside})
    st1.start()
    crossing = []
    for k in range(chunks):
        at = pl.ds(k * chunk, chunk)
        sends[2 * k].wait()
        far[at] = (part[at, columns(2 * (1 - side) + core)].astype(F32) + near_in[1, at].astype(F32)).astype(BF16)
        c = push(far.at[at], far_in.at[at], s2.at[k], r2.at[k], {"section": across})
        c.start()
        crossing.append(c)
    st1.wait()
    stats_mid[...] = stats[...] + stats_in[...]
    st2 = push(stats_mid, stats_far, st_s.at[1], st_r.at[1], {"section": across})
    st2.start()
    steps(group, cuts[3], cuts[4])
    steps((0,), 0, length)
    st2.wait()
    stats[...] = (stats_mid[...] + stats_far[...]) * (1.0 / gain.shape[1])
    total = jnp.zeros((1, QUARTER), F32)
    gain_q = gain[:, columns(me)]
    for k in range(chunks):
        at = pl.ds(k * chunk, chunk)
        sends[2 * k + 1].wait()
        near = part[at, columns(me)].astype(F32) + near_in[0, at].astype(F32)
        crossing[k].wait()
        d_q = near + far_in[at].astype(F32)
        u = unit[at, columns(me)]
        sums = jnp.concatenate([stats[:, at], jnp.zeros((chunk - 8, chunk), F32)], axis=0).T
        norm = scales[at, pl.ds(0, 1)] * (d_q * gain_q - sums[:, 0:1] - u * sums[:, 1:2])
        o_tok[at] = d_att[at, columns(me)].astype(F32) + norm
        total = total + jnp.sum(d_q * u, axis=0, keepdims=True)
    row = lax.broadcasted_iota(jnp.int32, (8, QUARTER), 0)
    gains[...] = jnp.where(row == 0, total, jnp.where(row == 1, gain_d[...], 0.0))

    def gain_copy(to, frm):
        return push(gains, gains_in.at[frm], gn_s.at[to], gn_r.at[frm], {"wide": to})

    for j in range(1, wide):
        gain_copy(lax.rem(w + j, wide), w).start()
    for i in (3, 1, 2, 0):
        own_block(i)
    gathered = gains[...]
    for j in range(1, wide):
        frm = lax.rem(w + j, wide)
        gain_copy(frm, frm).wait_recv()
        gathered = gathered + gains_in[frm]
    o_gain[...] = gathered
    for i, out in ((3, o_back), (2, o_out)):
        finals[i].wait_recv()
        add_rows(out, acc[i].at[2 * a + b], pair_in[i].at[0])
    for c in finals.values():
        c.wait_send()
    for c in late:
        c.wait()
    for j in range(1, wide):
        to = lax.rem(w + j, wide)
        gain_copy(to, w).wait_send()
        res_copy(to, w).wait_send()
        res_copy(to, to).wait_recv()

    def finish(t, carry):
        for i in range(4):
            if pair_first[i]:
                pair_copy(i, t).wait_send()

            @pl.when(t != a)
            def _():
                for block, _ in slots(i, t):
                    line_copy(i, block, block, w).wait_send()

        return carry

    lax.fori_loop(0, length, finish, 0)


def tail_call(g_in, g_back, first, second, d_att, tok, n1, qkv, mixed, w_qkv, w_out, mask, gain, gain_d, res, collective_id):
    wide = g_back.shape[0]
    length = wide // 2
    small = g_in.shape[2]
    hid = first.shape[2]
    count, width = d_att.shape
    chunks = count // 128
    shapes = [(4, small, 3 * QUARTER), (4, small, hid), (small, width), g_back.shape[1:]]
    expert = ((first.shape[1], 4 * hid), BF16)
    outs = [
        ((small, 3 * width), BF16),
        ((small, 4 * hid), BF16),
        (shapes[2], F32),
        (shapes[3], F32),
        ((8, QUARTER), F32),
        expert,
        expert,
        ((count, QUARTER), F32),
        (res.shape, BF16),
    ]
    scratch = [pltpu.VMEM((4, wide, small, 3 * QUARTER), BF16), pltpu.VMEM((wide, small, width), BF16)]
    for counts in (
        [length, length, wide, wide],
        [length + 1, length + 1, wide + 2, wide + 2],
        [length, length, 1, 1],
    ):
        scratch += [pltpu.VMEM((n, *s), BF16) for n, s in zip(counts, shapes)]
    scratch += [
        pltpu.VMEM((count, QUARTER), BF16),
        pltpu.VMEM((count, 3 * QUARTER), BF16),
        pltpu.VMEM((count, width), BF16),
        pltpu.VMEM((count, width), F32),
        pltpu.VMEM((count, 128), F32),
        pltpu.VMEM((8, count), F32),
        pltpu.VMEM((8, count), F32),
        pltpu.VMEM((8, count), F32),
        pltpu.VMEM((8, count), F32),
        pltpu.VMEM((2, count, QUARTER), BF16),
        pltpu.VMEM((count, QUARTER), BF16),
        pltpu.VMEM((count, QUARTER), BF16),
        pltpu.VMEM((8, QUARTER), F32),
        pltpu.VMEM((wide, 8, QUARTER), F32),
        DMA((8,)),
        DMA((2, 3)),
        DMA((2, 3)),
        DMA((4, 3)),
        DMA((4, 3)),
        DMA((4, length)),
        DMA((4, length)),
        DMA((4, wide)),
        DMA((4, wide + 2)),
        DMA((2, chunks)),
        DMA((2, chunks)),
        DMA((chunks,)),
        DMA((chunks,)),
        DMA((2,)),
        DMA((2,)),
        DMA((wide,)),
        DMA((wide,)),
        DMA((wide,)),
        DMA((wide,)),
    ]
    return call(
        tail_kernel,
        tuple(jax.ShapeDtypeStruct(*o) for o in outs),
        [VM, VM, ANY, ANY] + [VM] * 11,
        (ANY, ANY, VM, VM, VM, ANY, ANY, VM, VM),
        scratch,
        collective_id,
        *(g_in, g_back, first, second, d_att, tok, n1, qkv, mixed, w_qkv, w_out, mask, gain, gain_d, res),
    )


def head_kernel(*refs):
    qkv, inn, vec, outw, backw, first, second, tok, mask, cot = refs[:10]
    o_qkv, o_in, o_vec, o_out, o_back, o_first, o_second, o_tok, o_n1, o_act, o_mixed, o_att, o_cot = refs[10:23]
    st_qkv, st_in, st_vec, gain, part, near_in, far, far_in = refs[23:31]
    loc, cut_s, cut_r, tok_s, tok_r, line_s, line_r, exp_s, exp_r, s1, r1, s2, r2, g_s, g_r, c_s, c_r = refs[31:]
    me, beside, across = section_places()
    core, side = lax.rem(me, 2), lax.div(me, 2)
    w, length, a, b = line_of_wide()
    other = 1 - b
    mate = 2 * a + other
    diagonal = beside + across - me
    peers = [beside, across, diagonal]
    greet_line(peers, True)
    hid = o_first.shape[2]
    width = 4 * QUARTER
    sent, local_cuts = [], []

    def part_of(src, start, count):
        return src.at[:, pl.ds(pl.multiple_of(start, 128), count)]

    def cuts_for(p):
        got = [
            (0, part_of(qkv, j * width + p * QUARTER, QUARTER), st_qkv.at[me, :, pl.ds(j * QUARTER, QUARTER)])
            for j in range(3)
        ]
        return got + [(1, part_of(inn, p * hid, hid), st_in.at[me]), (2, vec, st_vec.at[me])]

    for k, p in enumerate(peers):
        for n, (i, src, dst) in enumerate(cuts_for(p)):
            c = push(src, dst, cut_s.at[n, k], cut_r.at[n, k], {"section": p})
            c.start()
            sent.append((i, c))
    for n, (i, src, dst) in enumerate(cuts_for(me)):
        c = pltpu.make_async_copy(src, dst, loc.at[11 + n])
        c.start()
        local_cuts.append((i, c))
    tok_c = [
        push(tok, o_tok.at[:, columns(me)], tok_s.at[k], tok_r.at[k], {"section": p})
        for k, p in enumerate((across, beside))
    ]
    for c in tok_c:
        c.start()
    own_tok = pltpu.make_async_copy(tok, o_tok.at[:, columns(me)], loc.at[3])
    own_tok.start()
    late = []
    exp_c = []
    for i, (src, dst) in enumerate(((first, o_first), (second, o_second))):
        c = pltpu.make_async_copy(part_of(src, me * hid, hid), dst.at[me], loc.at[4 + i])
        c.start()
        late.append(c)
        for k, p in enumerate((across, diagonal, beside)):
            c = push(part_of(src, p * hid, hid), dst.at[me], exp_s.at[i, k], exp_r.at[i, k], {"section": p})
            c.start()
            exp_c.append(c)

    lines = (
        (st_qkv, o_qkv, True),
        (outw, o_out, False),
        (st_in, o_in, True),
        (backw, o_back, True),
        (st_vec, o_vec, False),
    )
    staged = {0: 0, 2: 1, 4: 2}
    up, down, pair = 0, 1, 2

    def place(i, which):
        dst = lines[i][1]
        return dst.at[:, which] if i in staged else dst.at[which]

    def item(i, which, kind, to, own=False):
        spot = place(i, which)
        return push(lines[i][0] if own else spot, spot, line_s.at[kind, i, which], line_r.at[i, which], {"wide": to})

    def along(i, which, kind, own, act):
        if kind == pair:
            act(item(i, which, pair, mate, own))
            return

        @pl.when((a < length - 1) if kind == up else (a > 0))
        def _():
            act(item(i, which, kind, w + 2 if kind == up else w - 2, own))

    def start(c):
        c.start()

    def done(c):
        c.wait_send()

    def arrived(i, which):
        item(i, which, pair, mate).wait_recv()

    def own_item(i):
        if i in staged:
            for j, c in sent:
                if j == staged[i]:
                    c.wait_recv()
            for j, c in local_cuts:
                if j == staged[i]:
                    c.wait()
        for kind in (up, down, pair):
            along(i, w, kind, True, start)
        c = pltpu.make_async_copy(lines[i][0], place(i, w), loc.at[6 + i])
        c.start()
        return c

    def mate_item(i):
        if not lines[i][2]:
            arrived(i, mate)
            for kind in (up, down):
                along(i, mate, kind, False, start)

    def both_ways(t, what):
        for kind, there, ok in ((up, a - t, a - t >= 0), (down, a + t, a + t < length)):

            @pl.when(ok)
            def _():
                what(kind, there)

    def steps(group, begin, end):
        def step(t, carry):
            for i in group:

                def pass_on(kind, there):
                    arrived(i, 2 * there + b)
                    along(i, 2 * there + b, kind, False, start)
                    if lines[i][2]:
                        along(i, 2 * there + b, pair, False, start)
                    else:
                        arrived(i, 2 * there + other)
                        along(i, 2 * there + other, kind, False, start)

                both_ways(t, pass_on)
            return carry

        lax.fori_loop(begin, end, step, 0)

    def pair_items(i):
        if lines[i][2]:
            lax.fori_loop(0, length, lambda there, carry: (arrived(i, 2 * there + other), carry)[1], 0)

    def all_sent(i):
        for kind in (up, down, pair):
            along(i, w, kind, True, done)
        if not lines[i][2]:
            for kind in (up, down):
                along(i, mate, kind, False, done)

        def finish(t, carry):
            def one(kind, there):
                along(i, 2 * there + b, kind, False, done)
                if lines[i][2]:
                    along(i, 2 * there + b, pair, False, done)
                else:
                    along(i, 2 * there + other, kind, False, done)

            both_ways(t, one)
            return carry

        lax.fori_loop(1, length, finish, 0)

    early, later = (4, 0, 1), (2, 3)
    soon = [own_item(i) for i in early]
    tok_c[0].wait_recv()
    spot = o_tok.at[:, columns(across)]
    tok_fwd = push(spot, spot, tok_s.at[2], tok_r.at[2], {"section": beside})
    tok_fwd.start()
    for i in early:
        mate_item(i)
    steps(early, 1, 2)
    late += [own_item(i) for i in later]
    steps(early, 2, length)

    def cot_place(which, block):
        return o_cot.at[block, :, columns(which)]

    def cot_wide(to, frm):
        return push(cot.at[to], cot_place(me, frm), c_s.at[0, to], c_r.at[0, frm], {"wide": to})

    def cot_spread(kind, block, to):
        here = cot_place(across if kind == 3 else me, block)
        return push(here, here, c_s.at[kind, block], c_r.at[kind, block], {"section": to})

    for j in range(1, 2 * length):
        cot_wide(lax.rem(w + j, 2 * length), w).start()
    o_cot[w, :, columns(me)] = cot[w]
    for i in later:
        mate_item(i)
    for i in early:
        pair_items(i)
    for c in soon:
        c.wait()
    own_tok.wait()
    tok_c[1].wait_recv()
    tok_fwd.wait_recv()

    wide = 2 * length
    small = qkv.shape[0]
    per = 128 // small
    for p in range(4):
        for g in range(wide // per):
            total = o_vec[p, g * per, 6:7]
            for j in range(1, per):
                total = total + o_vec[p, g * per + j, 6:7]
            gain[:, pl.ds((p * (wide // per) + g) * 128, 128)] = total
    micro, rows = mask.shape[:2]
    count = micro * rows
    chunk = 128
    chunks = count // chunk

    def project(k, carry):
        at = pl.ds(pl.multiple_of(k * chunk, chunk), chunk)
        unit, _ = row_norm(o_tok[at].astype(F32))
        o_n1[at] = (unit * gain[...]).astype(BF16)
        total = jnp.zeros((chunk, 3 * QUARTER), F32)
        for p in range(4):
            total = total + dot(o_n1[at, pl.ds(p * QUARTER, QUARTER)], o_qkv[p].reshape(QUARTER, 3 * QUARTER))
        o_act[at] = total.astype(BF16)
        return carry

    lax.fori_loop(0, chunks, project, 0)
    cuts = [1 + k * (length - 1) // 3 for k in range(4)]
    beside_core = 1 - core
    sends, crossing, spread = [], [], []
    for m in range(micro):
        at = pl.ds(m * rows, rows)
        for n in range(2):
            heads = attention_pair(n, lambda c: o_act[at, pl.ds(c, 128)], mask[m])
            got = [dot(probs.astype(BF16), v) for _, _, v, probs in heads]
            o_mixed[at, pl.ds(n * 128, 128)] = jnp.concatenate(got, axis=1).astype(BF16)
        for k in range(m * rows // chunk, (m + 1) * rows // chunk):
            at = pl.ds(k * chunk, chunk)
            part[at] = dot(o_mixed[at], o_out[...].reshape(QUARTER, width)).astype(BF16)
            for which, half in ((1, 1 - side), (0, side)):
                c = push(
                    part.at[at, columns(2 * half + beside_core)],
                    near_in.at[which, at],
                    s1.at[which, k],
                    r1.at[which, k],
                    {"section": beside},
                )
                c.start()
                sends.append(c)
        steps(later, cuts[m], cuts[m + 1])
    for k in range(chunks):
        at = pl.ds(k * chunk, chunk)
        sends[2 * k].wait()
        far[at] = (part[at, columns(2 * (1 - side) + core)].astype(F32) + near_in[1, at].astype(F32)).astype(BF16)
        c = push(far.at[at], far_in.at[at], s2.at[k], r2.at[k], {"section": across})
        c.start()
        crossing.append(c)
    for k in range(chunks):
        at = pl.ds(k * chunk, chunk)
        sends[2 * k + 1].wait()
        near = part[at, columns(me)].astype(F32) + near_in[0, at].astype(F32)
        crossing[k].wait()
        o_att[at, columns(me)] = (o_tok[at, columns(me)].astype(F32) + (near + far_in[at].astype(F32))).astype(BF16)
        here = o_att.at[at, columns(me)]
        for kind, to in ((0, across), (1, beside)):
            c = push(here, here, g_s.at[kind, k], g_r.at[kind, k], {"section": to})
            c.start()
            spread.append(c)
    steps(later, cuts[micro], cuts[3])
    for j in range(wide):
        block = lax.rem(w + j, wide)
        if j:
            cot_wide(block, block).wait_recv()
        cot_spread(1, block, across).start()
        cot_spread(2, block, beside).start()
    for k in range(chunks):
        spread[2 * k].wait()
        here = o_att.at[pl.ds(k * chunk, chunk), columns(across)]
        c = push(here, here, g_s.at[2, k], g_r.at[2, k], {"section": beside})
        c.start()
        spread.append(c)
    for j in range(wide):
        block = lax.rem(w + j, wide)
        cot_spread(1, block, across).wait_recv()
        cot_spread(3, block, beside).start()
    for i in later:
        pair_items(i)
    for j in range(wide):
        block = lax.rem(w + j, wide)
        cot_spread(1, block, across).wait_send()
        cot_spread(2, block, beside).wait()
        cot_spread(3, block, beside).wait()
        if j:
            cot_wide(block, w).wait_send()
    for k in range(chunks):
        spread[2 * k + 1].wait()
        spread[2 * chunks + k].wait()
    for i in early + later:
        all_sent(i)
    for _, c in sent:
        c.wait_send()
    for c in tok_c + [tok_fwd]:
        c.wait_send()
    for c in exp_c + late:
        c.wait()


def head_call(qkv, inn, vec, outw, backw, first, second, tok, mask, cot, collective_id):
    wide = cot.shape[0]
    small = qkv.shape[0]
    hid = inn.shape[1] // 4
    cut = 3 * QUARTER
    count = tok.shape[0]
    width = 4 * QUARTER
    chunks = count // 128
    outs = [
        ((4, wide, small, cut), BF16),
        ((4, wide, small, hid), BF16),
        ((4, wide, *vec.shape), F32),
        ((wide, *outw.shape), BF16),
        ((wide, *backw.shape), BF16),
        ((4, first.shape[0], hid), BF16),
        ((4, first.shape[0], hid), BF16),
        ((count, width), BF16),
        ((count, width), BF16),
        ((count, cut), BF16),
        ((count, QUARTER), BF16),
        ((count, width), BF16),
        ((*cot.shape[:2], width), BF16),
    ]
    return call(
        head_kernel,
        tuple(jax.ShapeDtypeStruct(*o) for o in outs),
        [ANY] * 8 + [VM, VM],
        (VM, ANY, VM, VM, ANY, ANY, ANY, VM, VM, VM, VM, VM, VM),
        [
            pltpu.VMEM((4, small, cut), BF16),
            pltpu.VMEM((4, small, hid), BF16),
            pltpu.VMEM((4, *vec.shape), F32),
            pltpu.VMEM((1, width), F32),
            pltpu.VMEM((count, width), BF16),
            pltpu.VMEM((2, count, QUARTER), BF16),
            pltpu.VMEM((count, QUARTER), BF16),
            pltpu.VMEM((count, QUARTER), BF16),
            DMA((16,)),
            DMA((5, 3)),
            DMA((5, 3)),
            DMA((3,)),
            DMA((3,)),
            DMA((3, 5, wide)),
            DMA((5, wide)),
            DMA((2, 3)),
            DMA((2, 3)),
            DMA((2, chunks)),
            DMA((2, chunks)),
            DMA((chunks,)),
            DMA((chunks,)),
            DMA((3, chunks)),
            DMA((3, chunks)),
            DMA((4, wide)),
            DMA((4, wide)),
        ],
        collective_id,
        *(qkv, inn, vec, outw, backw, first, second, tok, mask, cot),
    )


def dot(left, right):
    return jnp.dot(left, right, preferred_element_type=F32)


def dot_nt(left, right):
    return lax.dot_general(left, right, (((1,), (1,)), ((), ())), preferred_element_type=F32)


def dot_tn(left, right):
    return lax.dot_general(left, right, (((0,), (0,)), ((), ())), preferred_element_type=F32)


def gelu_value(v):
    return 0.5 * v * (1.0 + lax.erf(v * 0.7071067811865476))


def gelu_slope(v):
    return (
        0.5 * (1.0 + lax.erf(v * 0.7071067811865476))
        + v * jnp.exp(-0.5 * v * v) * 0.3989422804014327
    )


def unit_norm(v):
    centred = v - jnp.mean(v, axis=-1, keepdims=True)
    scale = lax.rsqrt(jnp.mean(centred * centred, axis=-1, keepdims=True) + 1e-05)
    return centred * scale, scale


IDS = {}


def id_of(*key):
    return IDS.setdefault(key, len(IDS))


def reduce_quarters(part, stats=None):
    return reduce_call(part.astype(BF16), stats, id_of("reduce", part.shape, stats is None))


def gather_quarters(quarter):
    return gather_call(quarter, id_of("gather", quarter.shape))


def wide_exchange(slots, spread):
    return exchange_call(slots, spread, id_of("exchange", spread))


def allowed_of(lengths, rows):
    pos = jnp.arange(rows, dtype=jnp.int32)
    group = pos[None] // lengths[:, None]
    return ((pos[:, None] >= pos[None, :])[None] & (group[:, :, None] == group[:, None, :])).astype(F32)


def body(
    tokens_in,
    cotangent,
    routes,
    seq_lengths,
    qkv_weight,
    out_weight,
    attn_gain,
    ffn_in,
    ffn_back,
    ffn_gain,
    centroids,
    first_gain,
    first_in,
    first_back,
    second_gain,
    second_in,
    second_back,
):
    sections = lax.axis_size("section")
    wide = lax.axis_size("wide")
    section_id = lax.axis_index("section")
    wide_id = lax.axis_index("wide")
    micro, rows, quarter = tokens_in.shape
    width = quarter * sections
    cap = 5 * rows // (4 * wide)
    tok_rows = micro * rows
    hid = first_back.shape[1]
    small = qkv_weight.shape[0]
    qkv_cols = qkv_weight.shape[1] // sections

    experts = jnp.arange(wide, dtype=jnp.int32)
    choose = (routes == experts).astype(jnp.int32)
    upto = (jnp.arange(rows)[:, None] >= jnp.arange(rows)[None, :]).astype(BF16)
    ranking = jnp.einsum("rk,mke->mre", upto, choose.astype(BF16), preferred_element_type=F32).astype(jnp.int32) - 1
    slot_of = routes[:, :, 0] * cap + jnp.sum(ranking * choose, axis=2)
    onehot = (jnp.arange(wide * cap, dtype=jnp.int32)[None, :, None] == slot_of[:, None, :]).astype(BF16)

    def to_slots(rows_q):
        packed = jnp.einsum("msr,mrd->msd", onehot, rows_q.reshape(micro, rows, quarter), preferred_element_type=F32)
        packed = packed.astype(BF16).reshape(micro, wide, cap, quarter).transpose(1, 0, 2, 3)
        return packed.reshape(wide, micro * cap, quarter)

    def to_experts(rows_q):
        return wide_exchange(to_slots(rows_q), True).reshape(wide * micro * cap, width)

    def from_slots(back):
        back = back.reshape(wide, micro, cap, quarter).transpose(1, 0, 2, 3).reshape(micro, wide * cap, quarter)
        got = jnp.einsum("msr,msd->mrd", onehot, back, preferred_element_type=F32)
        return got.astype(BF16).reshape(tok_rows, quarter)

    def to_tokens(slots_q):
        return from_slots(wide_exchange(slots_q.reshape(wide, micro * cap, quarter), False))

    per = 128 // small
    spread = lambda v: lax.dynamic_update_slice_in_dim(
        jnp.zeros((1, 128), F32), v.astype(F32)[None], lax.rem(wide_id, per) * small, 1
    )
    vectors = [v.astype(F32).reshape(2, 128) for v in (first_gain, second_gain, centroids)]
    vectors = jnp.concatenate(vectors + [spread(attn_gain), spread(ffn_gain)], axis=0)
    allowed = allowed_of(seq_lengths, rows)
    tokens_q = tokens_in.reshape(tok_rows, quarter)

    (qkv_w, in_w, vectors, out_w, back_w, first_w, second_w, tokens, normed_a, packed, mixed, attended, d_mixed) = head_call(
        qkv_weight,
        ffn_in,
        vectors,
        out_weight,
        ffn_back,
        first_in[0],
        second_in[0],
        tokens_q,
        allowed,
        to_slots(cotangent.reshape(tok_rows, quarter)),
        id_of("head"),
    )
    qkv_w = qkv_w.reshape(width, qkv_cols)
    in_w = in_w.reshape(width, hid)
    out_w = out_w.reshape(quarter, width)
    back_w = back_w.reshape(hid, width)
    first_w = first_w.reshape(width, hid)
    second_w = second_w.reshape(width, hid)
    own = lax.dynamic_index_in_dim(vectors, wide_id, axis=1, keepdims=False)
    gain_first, gain_second, centre = (own[:, 2 * j : 2 * j + 2].reshape(1, width) for j in range(3))
    gain_attn, gain_ffn = (
        jnp.sum(vectors[:, :, j].reshape(sections, wide // per, per, 128), axis=2).reshape(1, width) for j in (6, 7)
    )
    own_quarter = lambda v: lax.dynamic_slice_in_dim(v, section_id * quarter, quarter, axis=1)
    first_b = first_back[0]
    second_b = second_back[0]

    attended_q = own_quarter(attended)

    def branch(v, w_in, w_back, gain):
        unit, scale = unit_norm(v.astype(F32))
        normed = (unit * gain).astype(BF16)
        pre = dot(normed, w_in)
        hidden = gelu_value(pre).astype(BF16)
        return (normed, unit, scale, pre, hidden), dot(hidden, w_back)

    def branch_back(grad, saved, w_in, w_back, gain, more=None):
        normed, unit, scale, pre, hidden = saved
        d_back = dot_tn(hidden, grad)
        d_pre = (dot_nt(grad, w_back) * gelu_slope(pre)).astype(BF16)
        d_in = dot_tn(normed, d_pre)
        return d_in, d_back, norm_back(dot_nt(d_pre, w_in), unit, scale, gain, more)

    def norm_back(d_part, unit, scale, gain, more=None):
        d_unit = d_part * gain
        sums = jnp.stack([jnp.sum(d_unit, axis=1), jnp.sum(d_unit * unit, axis=1)])
        if more is not None:
            sums = jnp.concatenate([sums, more])
        d_q, sums = reduce_quarters(d_part, jnp.pad(sums, ((0, 8 - sums.shape[0]), (0, 0))))
        extra, sums = sums[2], sums / width
        unit_q = own_quarter(unit)
        d_rows = scale * (d_q * own_quarter(gain) - sums[0][:, None] - unit_q * sums[1][:, None])
        return d_rows, jnp.sum(d_q * unit_q, axis=0), extra

    saved_d, part = branch(attended, in_w, back_w, gain_ffn)
    fed_q = (attended_q.astype(F32) + reduce_quarters(part)).astype(BF16)
    routed = to_experts(fed_q)
    routed_q = own_quarter(routed)
    d_mixed = d_mixed.reshape(wide * micro * cap, width).astype(F32)
    d_mixed_q = own_quarter(d_mixed)
    saved_1, part = branch(routed, first_w, first_b, gain_first)
    first_q = (routed_q.astype(F32) + reduce_quarters(part)).astype(BF16)
    first = gather_quarters(first_q)
    saved_2, part = branch(first, second_w, second_b, gain_second)
    gate = jax.nn.sigmoid(jnp.sum(routed.astype(F32) * centre, axis=-1, keepdims=True))
    second_q = first_q.astype(F32) + reduce_quarters(part)
    mixed_q = routed_q.astype(F32) + gate * second_q

    d_second = gate * d_mixed
    d_second_q = gate * d_mixed_q
    d_second_in, d_second_back, (norm_q, second_gain_grad, d_logit) = branch_back(
        d_second.astype(BF16), saved_2, second_w, second_b, gain_second, jnp.sum(d_mixed_q * second_q, axis=-1)[None]
    )
    d_logit = d_logit[:, None] * gate * (1.0 - gate)
    centroids_grad = jnp.sum(d_logit * routed_q.astype(F32), axis=0)[None]
    d_gated_q = (d_mixed_q + d_logit * own_quarter(centre)).astype(BF16)
    d_first_q = (d_second_q + norm_q).astype(BF16)
    d_first_in, d_first_back, (norm_q, first_gain_grad, _) = branch_back(
        gather_quarters(d_first_q), saved_1, first_w, first_b, gain_first
    )
    d_routed_q = (d_first_q.astype(F32) + norm_q + d_gated_q.astype(F32)).astype(BF16)
    d_fed_q = to_tokens(d_routed_q)
    d_in, d_back, (norm_q, d_gain_ffn, _) = branch_back(gather_quarters(d_fed_q), saved_d, in_w, back_w, gain_ffn)
    d_attended_q = (d_fed_q.astype(F32) + norm_q).astype(BF16)
    d_attended = gather_quarters(d_attended_q)
    def by_row(grad):
        return grad.astype(BF16).reshape(sections, wide, small, grad.shape[1])

    qkv_grad, ffn_in_grad, out_grad, ffn_back_grad, d_gains, d_first_in, d_second_in, tokens_grad, result = tail_call(
        by_row(d_in),
        d_back.astype(BF16).reshape(wide, hid // wide, width),
        d_first_in.astype(BF16).reshape(sections, quarter, hid),
        d_second_in.astype(BF16).reshape(sections, quarter, hid),
        d_attended,
        tokens,
        normed_a,
        packed,
        mixed,
        qkv_w,
        out_w,
        allowed,
        gain_attn,
        d_gain_ffn[None],
        mixed_q.astype(BF16).reshape(wide, micro * cap, quarter),
        id_of("tail"),
    )
    block_out = from_slots(result).reshape(micro, rows, quarter)
    d_gains = lax.dynamic_slice_in_dim(d_gains, wide_id * small, small, axis=1)
    tokens_grad = tokens_grad.reshape(micro, rows, quarter)
    return (
        block_out,
        tokens_grad,
        qkv_grad.astype(F32),
        out_grad,
        d_gains[0],
        ffn_in_grad.astype(F32),
        ffn_back_grad,
        d_gains[1],
        centroids_grad,
        first_gain_grad[None],
        d_first_in[None].astype(F32),
        d_first_back[None],
        second_gain_grad[None],
        d_second_in[None].astype(F32),
        d_second_back[None],
    )


def solution(mesh):
    dense = P(("section", "wide"), None)
    dense_gain = P(("section", "wide"))
    tokens = P(None, "wide", "section")
    gain = P("wide", "section")
    expert = P("wide", "section", None)
    in_specs = (
        (tokens, tokens, P(None, "wide", None), P(), dense, dense, dense_gain, dense, dense, dense_gain)
        + (gain, gain, expert, expert, gain, expert, expert)
    )
    out_specs = (
        (tokens, tokens, dense, dense, dense_gain, dense, dense, dense_gain)
        + (gain, gain, expert, expert, gain, expert, expert)
    )
    return jax.shard_map(body, mesh=mesh, in_specs=in_specs, out_specs=out_specs, check_vma=False)
```
